16 devices in a mesh: dp: 2 (over y, z), ep: 8 (over x, core).
Axes of the slice: x: 4, y: 2, z: 1, core: 2. Of those that a mesh axis runs over, the one named last changes fastest.
The devices are a block of a 4x4x8 slice.
Arguments:
- x_in: bfloat16 [1024, 2880], P(('dp', 'ep')), parts along dimension 0
- expert_ids: int32 [1024, 4], P(('dp', 'ep')), parts along dimension 0
- norm_weight: bfloat16 [2880], replicated
- router_w: bfloat16 [2880, 32], replicated
- router_b: bfloat16 [32], replicated
- w_gate_up: bfloat16 [32, 2880, 5760], P('ep')
- b_gate_up: bfloat16 [32, 5760], P('ep')
- w_down: bfloat16 [32, 2880, 2880], P('ep')
- b_down: bfloat16 [32, 2880], P('ep')
Outputs:
- output: bfloat16 [1024, 2880], P(('dp', 'ep')), parts along dimension 0
There are 2 independent parts. The reference program is written for one: setup_inputs(seed, part) draws one part's arguments, and reference() takes and returns one part's arrays. A program takes and returns all parts, laid end to end along the dimension named above; an argument that names none is the same for every part.
All inputs are finite; a program needn't handle non-finite values.
Results may differ from the reference program's by a relative error of at most 0.00686295.
Values are sent between devices in bfloat16 or wider.
A program may use at most 768 MiB of HBM per device.

```python
import jax
import jax.numpy as jnp
from jax import lax

D_MODEL = 2880
D_FF = 2880
EXPERTS = 32
TOP_K = 4
TOK_DEV = 64
GROUP_SIZE = 8

TOKENS = TOK_DEV * GROUP_SIZE
CAPACITY = 4 * TOP_K * TOK_DEV // EXPERTS
HOT_COUNT = EXPERTS // 8
EPSILON = 1e-5
LIMIT = 7.0
ALPHA = 1.702


def draw_routes(key):
    key_hot, key_src = jax.random.split(key)
    expert_order = jax.random.permutation(key_hot, EXPERTS)
    cold_total = TOP_K * TOK_DEV - HOT_COUNT * CAPACITY
    cold_count = EXPERTS - HOT_COUNT
    position = jnp.arange(EXPERTS)
    extra = (position - HOT_COUNT < cold_total % cold_count).astype(jnp.int32)
    counts = jnp.where(position < HOT_COUNT, CAPACITY, cold_total // cold_count + extra)
    ends = jnp.cumsum(counts)
    slot_rank = jnp.sum(jnp.arange(TOP_K * TOK_DEV)[:, None] >= ends[None, :], axis=1)

    def one_source(src_key):
        key_cold, key_tok = jax.random.split(src_key)
        cold = jax.random.permutation(key_cold, expert_order[HOT_COUNT:])
        order = jnp.concatenate([expert_order[:HOT_COUNT], cold])
        table = order[slot_rank].reshape(TOP_K, TOK_DEV).T
        return table[jax.random.permutation(key_tok, TOK_DEV)]

    tables = jax.vmap(one_source)(jax.random.split(key_src, GROUP_SIZE))
    return tables.reshape(TOKENS, TOP_K).astype(jnp.int32)


def stacked_normal(key, shape, scale):
    def one_expert(expert_key):
        return (jax.random.normal(expert_key, shape, jnp.float32) * scale).astype(jnp.bfloat16)
    return lax.map(one_expert, jax.random.split(key, EXPERTS))


def setup_inputs(seed: int = 0, part: int = 0) -> dict:
    shared = jax.random.split(jax.random.key(seed), 7)
    own = jax.random.split(jax.random.fold_in(jax.random.key(seed + 1), part), 2)
    x_in = jax.random.normal(own[0], (TOKENS, D_MODEL), jnp.float32).astype(jnp.bfloat16)
    expert_ids = draw_routes(own[1])
    norm_weight = (1.0 + 0.3 * jax.random.normal(shared[0], (D_MODEL,), jnp.float32)).astype(jnp.bfloat16)
    router_w = (jax.random.normal(shared[1], (D_MODEL, EXPERTS), jnp.float32) * D_MODEL ** -0.5).astype(jnp.bfloat16)
    router_b = (0.7 * jax.random.normal(shared[2], (EXPERTS,), jnp.float32)).astype(jnp.bfloat16)
    w_gate_up = stacked_normal(shared[3], (D_MODEL, 2 * D_FF), 5.0 * D_MODEL ** -0.5)
    b_gate_up = jax.random.normal(shared[4], (EXPERTS, 2 * D_FF), jnp.float32).astype(jnp.bfloat16)
    w_down = stacked_normal(shared[5], (D_FF, D_MODEL), 0.125 * D_FF ** -0.5)
    b_down = (0.5 * jax.random.normal(shared[6], (EXPERTS, D_MODEL), jnp.float32)).astype(jnp.bfloat16)
    return dict(x_in=x_in, expert_ids=expert_ids, norm_weight=norm_weight, router_w=router_w, router_b=router_b, w_gate_up=w_gate_up, b_gate_up=b_gate_up, w_down=w_down, b_down=b_down)


def clamped_glu(gate_up):
    gate = jnp.minimum(gate_up[..., 0::2].astype(jnp.float32), LIMIT)
    linear = jnp.clip(gate_up[..., 1::2].astype(jnp.float32), -LIMIT, LIMIT)
    return (gate * jax.nn.sigmoid(ALPHA * gate) * (linear + 1.0)).astype(jnp.bfloat16)


def reference(x_in, expert_ids, norm_weight, router_w, router_b, w_gate_up, b_gate_up, w_down, b_down):
    x_float = x_in.astype(jnp.float32)
    inv_rms = lax.rsqrt(jnp.mean(x_float * x_float, axis=-1, keepdims=True) + EPSILON)
    hidden = (x_float * inv_rms * norm_weight.astype(jnp.float32)).astype(jnp.bfloat16)
    logits = jnp.dot(hidden, router_w, preferred_element_type=jnp.float32) + router_b.astype(jnp.float32)
    gates = jax.nn.softmax(jnp.take_along_axis(logits, expert_ids, axis=1), axis=-1)
    flat_ids = expert_ids.reshape(-1)
    flat_gates = gates.reshape(-1)
    max_rows = GROUP_SIZE * CAPACITY

    def one_expert(combined, weights):
        expert, gate_up_w, gate_up_b, down_w, down_b = weights
        chosen = flat_ids == expert
        picks = jnp.nonzero(chosen, size=max_rows, fill_value=0)[0]
        valid = jnp.arange(max_rows) < jnp.sum(chosen)
        row_token = picks // TOP_K
        rows = hidden[row_token]
        gate_up = (jnp.dot(rows, gate_up_w, preferred_element_type=jnp.float32) + gate_up_b.astype(jnp.float32)).astype(jnp.bfloat16)
        glu_out = clamped_glu(gate_up)
        expert_out = (jnp.dot(glu_out, down_w, preferred_element_type=jnp.float32) + down_b.astype(jnp.float32)).astype(jnp.bfloat16)
        scale = jnp.where(valid, flat_gates[picks], 0.0)
        combined = combined.at[row_token].add(scale[:, None] * expert_out.astype(jnp.float32))
        return combined, None

    start_sum = jnp.zeros((TOKENS, D_MODEL), jnp.float32)
    combined, _ = lax.scan(one_expert, start_sum, (jnp.arange(EXPERTS, dtype=jnp.int32), w_gate_up, b_gate_up, w_down, b_down))
    return (x_float + combined).astype(jnp.bfloat16)
```

```python
import functools

import jax
import jax.numpy as jnp
from jax import lax
from jax.experimental import pallas as pl
from jax.experimental.pallas import tpu as pltpu
from jax.sharding import PartitionSpec as P

EPSILON = 1e-5
LIMIT = 7.0
ALPHA = 1.702
F32 = jnp.float32
BF16 = jnp.bfloat16
VMEM_LIMIT = 63 * 1024 * 1024


def dot32(a, b):
    return jnp.dot(a, b, preferred_element_type=F32)


def dot_t(a, b):
    return lax.dot_general(a, b, (((0,), (0,)), ((), ())), preferred_element_type=F32)


def dispatch_kernel(n, local_exp, x_ref, ids_ref, g_ref, wr_ref, br_ref, hall, pos_ref, post_ref, p_ref,
                    mall, sa, ra, sb, rb, sc, rc, sd, rd, sm, rm):
    me = lax.axis_index('ep')
    chips = n // 2
    chip, core = me // 2, me % 2
    partner = chip * 2 + (1 - core)
    right_chip, left_chip = (chip + 1) % chips, (chip + chips - 1) % chips
    far_chip = (chip + 2) % chips
    right, left = right_chip * 2 + core, left_chip * 2 + core
    far = far_chip * 2 + core
    tok, _ = x_ref.shape
    top_k = ids_ref.shape[1]
    experts = wr_ref.shape[1]
    half = tok // 2

    barrier = pltpu.get_barrier_semaphore()
    for k in range(1, n):
        pl.semaphore_signal(barrier, inc=1, device_id={'ep': (me + k) % n}, device_id_type=pl.DeviceIdType.MESH)

    x = x_ref[...].astype(F32)
    inv = lax.rsqrt(jnp.mean(x * x, axis=-1, keepdims=True) + EPSILON)
    h = (x * inv * g_ref[...].astype(F32)).astype(BF16)
    hall[me] = h
    logits = dot32(h, wr_ref[...]) + br_ref[...].astype(F32)
    lane = lax.broadcasted_iota(jnp.int32, (tok, experts), 1)
    hot = [ids_ref[:, k:k + 1] == lane for k in range(top_k)]
    picked = [jnp.sum(jnp.where(hk, logits, 0.0), axis=1, keepdims=True) for hk in hot]
    top = functools.reduce(jnp.maximum, picked)
    ex = [jnp.exp(v - top) for v in picked]
    total = functools.reduce(jnp.add, ex)
    gates = jnp.zeros((tok, experts), F32)
    chosen = jnp.zeros((tok, experts), F32)
    for k in range(top_k):
        gates = gates + jnp.where(hot[k], ex[k] / total, 0.0)
        chosen = chosen + jnp.where(hot[k], 1.0, 0.0)
    mall[me, 0] = gates
    mall[me, 1] = chosen

    pl.semaphore_wait(barrier, n - 1)

    def copy(src, dst, ssem, rsem, dev):
        return pltpu.make_async_remote_copy(src_ref=src, dst_ref=dst, send_sem=ssem, recv_sem=rsem,
                                            device_id={'ep': dev}, device_id_type=pl.DeviceIdType.MESH)

    lo, hi = pl.ds(0, half), pl.ds(half, half)
    sends = []

    def start(c):
        c.start()
        sends.append(c)

    for i, (dev, parts) in enumerate(((right, (lo, hi)), (left, (hi, lo)))):
        for j, rows in enumerate(parts):
            start(copy(hall.at[me, rows], hall.at[me, rows], sb.at[i, j], rb.at[i, j], dev))
    start(copy(hall.at[me], hall.at[me], sa, ra, partner))
    metas = []
    for k in range(1, n):
        c = copy(mall.at[me], mall.at[me], sm.at[k - 1], rm.at[k - 1], (me + k) % n)
        c.start()
        metas.append(c)
    order = ((0, left, right, (lo, hi)), (1, right, left, (hi, lo)))
    for i, origin, onward, parts in order:
        slot = hall.at[origin, parts[0]]
        copy(slot, slot, sb.at[i, 0], rb.at[i, 0], origin).wait_recv()
        start(copy(slot, slot, sc.at[i], rc.at[i], onward))
        start(copy(slot, slot, sd.at[i, 0], rd.at[i, 0], partner))
    for i, origin, onward, parts in order:
        slot = hall.at[origin, parts[1]]
        copy(slot, slot, sb.at[i, 1], rb.at[i, 1], origin).wait_recv()
        start(copy(slot, slot, sd.at[i, 1], rd.at[i, 1], partner))
    for i, origin, onward, parts in order:
        slot = hall.at[far, parts[0]]
        copy(slot, slot, sc.at[i], rc.at[i], origin).wait_recv()
        start(copy(slot, slot, sd.at[i, 2], rd.at[i, 2], partner))

    for k in range(1, n):
        src = (me + n - k) % n
        copy(mall.at[src], mall.at[src], sm.at[k - 1], rm.at[k - 1], src).wait_recv()
    tokens = n * tok
    e0 = me * local_exp
    gates_all = mall[:, 0].reshape(tokens, experts)
    chosen_all = mall[:, 1].reshape(tokens, experts)
    lane_all = lax.broadcasted_iota(jnp.int32, (tokens, experts), 1)
    pick = (lax.broadcasted_iota(jnp.int32, (experts, 8), 0)
            == lax.broadcasted_iota(jnp.int32, (experts, 8), 1) + e0)
    pick = jnp.where(pick & (lax.broadcasted_iota(jnp.int32, (experts, 8), 1) < local_exp), 1.0, 0.0).astype(BF16)
    mine = dot32(chosen_all.astype(BF16), pick).astype(BF16)
    row = lax.broadcasted_iota(jnp.int32, (tokens, tokens), 0)
    col = lax.broadcasted_iota(jnp.int32, (tokens, tokens), 1)
    lower = jnp.where(col < row, 1.0, 0.0).astype(BF16)
    upper = jnp.where(row < col, 1.0, 0.0).astype(BF16)
    eye = jnp.where(row == col, 1.0, 0.0).astype(BF16)
    pos_ref[...] = jnp.where(mine.astype(F32) > 0.5, dot32(lower, mine), -1.0)
    post_ref[...] = jnp.where(dot_t(mine, eye) > 0.5, dot_t(mine, upper), -1.0)
    for e in range(local_exp):
        p_ref[:, e:e + 1] = jnp.sum(jnp.where(lane_all == e0 + e, gates_all, 0.0), axis=1, keepdims=True)

    copy(hall.at[partner], hall.at[partner], sa, ra, partner).wait_recv()
    for i, origin_chip, parts in ((0, left_chip, (lo, hi)), (1, right_chip, (hi, lo))):
        other = origin_chip * 2 + (1 - core)
        for j in range(2):
            slot = hall.at[other, parts[j]]
            copy(slot, slot, sd.at[i, j], rd.at[i, j], partner).wait_recv()
        slot = hall.at[far_chip * 2 + (1 - core), parts[0]]
        copy(slot, slot, sd.at[i, 2], rd.at[i, 2], partner).wait_recv()
    for c in sends:
        c.wait_send()
    for c in metas:
        c.wait_send()


def dispatch(x, ids, g, wr, br, n, local_exp):
    tok, d_model = x.shape
    tokens = n * tok
    vm = pl.BlockSpec(memory_space=pltpu.VMEM)
    dma = pltpu.SemaphoreType.DMA
    hall, pos, post, p = pl.pallas_call(
        functools.partial(dispatch_kernel, n, local_exp),
        out_shape=(jax.ShapeDtypeStruct((n, tok, d_model), BF16),
                   jax.ShapeDtypeStruct((tokens, 8), F32),
                   jax.ShapeDtypeStruct((8, tokens), F32),
                   jax.ShapeDtypeStruct((tokens, local_exp), F32)),
        in_specs=[vm] * 5,
        out_specs=(vm,) * 4,
        scratch_shapes=[pltpu.VMEM((n, 2, tok, wr.shape[1]), F32),
                        dma, dma, dma((2, 2)), dma((2, 2)), dma((2,)), dma((2,)), dma((2, 3)), dma((2, 3)),
                        dma((n - 1,)), dma((n - 1,))],
        compiler_params=pltpu.CompilerParams(collective_id=0, has_side_effects=True, vmem_limit_bytes=VMEM_LIMIT),
        name='dispatch',
    )(x, ids, g, wr, br)
    return hall.reshape(tokens, d_model), pos, post, p


def gate_up_kernel(blk, m_blk, slots, hall, post_ref, w_hbm, b_ref, z_ref, wbuf, xg, perm, sems):
    local_exp, d_model, width = w_hbm.shape
    full, rest = width // blk, width % blk
    per_exp = full + (1 if rest else 0)
    total = local_exp * per_exp
    tokens = hall.shape[0]
    depth = slots - 1

    src = lax.broadcasted_iota(jnp.int32, (256, 256), 0)
    dst = lax.broadcasted_iota(jnp.int32, (256, 256), 1)
    want = jnp.where(dst < 128, 2 * dst, 2 * (dst - 128) + 1)
    perm[...] = jnp.where(src == want, 1.0, 0.0).astype(BF16)

    def block_copy(q, is_rest):
        e, j = q // per_exp, q % per_exp
        slot = q % slots
        if is_rest:
            return pltpu.make_async_copy(w_hbm.at[e, :, pl.ds(full * blk, rest)],
                                         wbuf.at[slot, :, pl.ds(0, rest)], sems.at[slot])
        return pltpu.make_async_copy(w_hbm.at[e, :, pl.ds(pl.multiple_of(j * blk, 128), blk)], wbuf.at[slot], sems.at[slot])

    def start(q):
        if not rest:
            block_copy(q, False).start()
            return
        j = lax.rem(q, per_exp)

        @pl.when(j < full)
        def _():
            block_copy(q, False).start()

        @pl.when(j == full)
        def _():
            block_copy(q, True).start()

    for q in range(depth):
        start(jnp.int32(q))

    def one_expert(e, carry):
        where_row = post_ref[pl.ds(e, 1), :]
        count = jnp.sum(jnp.where(where_row >= 0.0, 1.0, 0.0)).astype(jnp.int32)
        chunks = (count + (m_blk - 1)) // m_blk

        def gather(m, c):
            at = lax.broadcasted_iota(jnp.int32, (m_blk, tokens), 0) + m * m_blk
            onehot = jnp.where(at.astype(F32) == where_row, 1.0, 0.0).astype(BF16)
            xg[pl.ds(pl.multiple_of(m * m_blk, m_blk), m_blk), :] = dot32(onehot, hall[...]).astype(BF16)
            return c

        lax.fori_loop(0, chunks, gather, 0)

        def block(j, cols):
            q = e * per_exp + j
            slot = lax.rem(q, slots)

            @pl.when(q + depth < total)
            def _():
                start(q + depth)

            block_copy(q, cols != blk).wait()
            off = pl.multiple_of(j * blk, 128)
            bias = b_ref[e, :, pl.ds(off, cols)].astype(F32)

            def rows(m, c):
                at = pl.ds(pl.multiple_of(m * m_blk, m_blk), m_blk)
                u = (dot32(xg[at, :], wbuf[slot, :, :cols]) + bias).astype(BF16)
                for t in range(0, cols, 256):
                    wide = min(256, cols - t)
                    if wide == 256:
                        pm = perm[...]
                    else:
                        pm = jnp.concatenate([perm[:128, :64], perm[:128, 128:192]], axis=1)
                    al = dot32(u[:, t:t + wide], pm)
                    gate = jnp.minimum(al[:, :wide // 2], LIMIT)
                    linear = jnp.clip(al[:, wide // 2:], -LIMIT, LIMIT)
                    z = gate * jax.nn.sigmoid(ALPHA * gate) * (linear + 1.0)
                    zoff = pl.multiple_of(j * (blk // 2), 128) + t // 2
                    z_ref[e, at, pl.ds(zoff, wide // 2)] = z.astype(BF16)
                return c

            lax.fori_loop(0, chunks, rows, 0)

        def body(j, c):
            block(j, blk)
            return c

        lax.fori_loop(0, full, body, 0)
        if rest:
            block(jnp.int32(full), rest)
        return carry

    lax.fori_loop(0, local_exp, one_expert, 0)


def gate_up(hall, post, w, b, max_rows, blk, m_blk, slots):
    local_exp, d_model, width = w.shape
    vm = pl.BlockSpec(memory_space=pltpu.VMEM)
    return pl.pallas_call(
        functools.partial(gate_up_kernel, blk, m_blk, slots),
        out_shape=jax.ShapeDtypeStruct((local_exp, max_rows, width // 2), BF16),
        in_specs=[vm, vm, pl.BlockSpec(memory_space=pl.ANY), vm],
        out_specs=vm,
        scratch_shapes=[pltpu.VMEM((slots, d_model, blk), BF16), pltpu.VMEM((max_rows, d_model), BF16),
                        pltpu.VMEM((256, 256), BF16), pltpu.SemaphoreType.DMA((slots,))],
        compiler_params=pltpu.CompilerParams(vmem_limit_bytes=VMEM_LIMIT),
        name='gate_up',
    )(hall, post, w, b.reshape(local_exp, 1, width))


def down_kernel(blk, slots, z_ref, pos_ref, p_ref, w_hbm, b_ref, out_ref, wbuf, wrest, scat, sems, rsems):
    local_exp, d_ff, width = w_hbm.shape
    tokens = pos_ref.shape[0]
    max_rows = z_ref.shape[1]
    chunks = [(c, min(blk, width - c)) for c in range(0, width, blk)]
    total = len(chunks) * local_exp
    depth = slots - 1

    def block_copy(q):
        off, cols = chunks[q // local_exp]
        src = w_hbm.at[q % local_exp, :, pl.ds(off, cols)]
        if cols == blk:
            return pltpu.make_async_copy(src, wbuf.at[q % slots], sems.at[q % slots])
        return pltpu.make_async_copy(src, wrest.at[q % local_exp], rsems.at[q % local_exp])

    for q in range(depth):
        block_copy(q).start()
    slot_ids = lax.broadcasted_iota(jnp.int32, (tokens, max_rows), 1).astype(F32)
    for e in range(local_exp):
        scat[e] = jnp.where(pos_ref[:, e:e + 1] == slot_ids, 1.0, 0.0).astype(BF16)
    row_ids = lax.broadcasted_iota(jnp.int32, (max_rows, 1), 0).astype(F32)
    for c, (off, cols) in enumerate(chunks):
        for e in range(local_exp):
            q = c * local_exp + e
            if q + depth < total:
                block_copy(q + depth).start()
            block_copy(q).wait()
            count = jnp.max(pos_ref[:, e:e + 1]) + 1.0
            wv = wbuf[q % slots] if cols == blk else wrest[e]
            y = dot32(z_ref[e], wv) + b_ref[e, :, off:off + cols].astype(F32)
            y = jnp.where(row_ids < count, y, 0.0).astype(BF16)
            part = p_ref[:, e:e + 1] * dot32(scat[e], y)
            if e == 0:
                out_ref[:, off:off + cols] = part
            else:
                out_ref[:, off:off + cols] += part


def down(z, pos, p, w, b, blk, slots):
    local_exp, d_ff, width = w.shape
    tokens = pos.shape[0]
    vm = pl.BlockSpec(memory_space=pltpu.VMEM)
    return pl.pallas_call(
        functools.partial(down_kernel, blk, slots),
        out_shape=jax.ShapeDtypeStruct((tokens, width), F32),
        in_specs=[vm, vm, vm, pl.BlockSpec(memory_space=pl.ANY), vm],
        out_specs=vm,
        scratch_shapes=[pltpu.VMEM((slots, d_ff, blk), BF16), pltpu.VMEM((local_exp, d_ff, width % blk), BF16),
                        pltpu.VMEM((local_exp, tokens, z.shape[1]), BF16),
                        pltpu.SemaphoreType.DMA((slots,)), pltpu.SemaphoreType.DMA((local_exp,))],
        compiler_params=pltpu.CompilerParams(vmem_limit_bytes=VMEM_LIMIT),
        name='down',
    )(z, pos, p, w, b.reshape(local_exp, 1, width))


def solution(mesh):
    n = mesh.shape['ep']
    rows_spec = P(('dp', 'ep'), None)

    def local_block(x_in, expert_ids, norm_weight, router_w, router_b, w_gate_up, b_gate_up, w_down, b_down):
        tok, d_model = x_in.shape
        top_k = expert_ids.shape[1]
        local_exp = w_gate_up.shape[0]
        experts = local_exp * n
        max_rows = n * (4 * top_k * tok // experts)
        blk = 768 if w_gate_up.shape[2] >= 2048 else 256
        hall, pos, post, p = dispatch(x_in, expert_ids, norm_weight.reshape(1, -1), router_w, router_b.reshape(1, -1), n, local_exp)
        z = gate_up(hall, post, w_gate_up, b_gate_up, max_rows, blk, min(128, max_rows), 4)
        part = down(z, pos, p, w_down, b_down, blk, 4)
        mixed = lax.psum_scatter(part, 'ep', scatter_dimension=0, tiled=True)
        return (x_in.astype(F32) + mixed).astype(BF16)

    return jax.shard_map(local_block, mesh=mesh, in_specs=(rows_spec, rows_spec, P(), P(), P(), P('ep', None, None), P('ep', None), P('ep', None, None), P('ep', None)), out_specs=rows_spec, check_vma=False)
```

```python
import functools

import jax
import jax.numpy as jnp
from jax import lax
from jax.experimental import pallas as pl
from jax.experimental.pallas import tpu as pltpu
from jax.sharding import PartitionSpec as P

EPSILON = 1e-5
LIMIT = 7.0
ALPHA = 1.702
F32 = jnp.float32
BF16 = jnp.bfloat16
VMEM_LIMIT = 63 * 1024 * 1024


def dot32(a, b):
    return jnp.dot(a, b, preferred_element_type=F32)


def dot_t(a, b):
    return lax.dot_general(a, b, (((0,), (0,)), ((), ())), preferred_element_type=F32)


def dispatch_kernel(n, local_exp, x_ref, ids_ref, g_ref, wr_ref, br_ref, hall, pos_ref, post_ref, p_ref,
                    mall, sa, ra, sb, rb, sc, rc, sd, rd, sm, rm):
    me = lax.axis_index('ep')
    chips = n // 2
    chip, core = me // 2, me % 2
    partner = chip * 2 + (1 - core)
    right_chip, left_chip = (chip + 1) % chips, (chip + chips - 1) % chips
    far_chip = (chip + 2) % chips
    right, left = right_chip * 2 + core, left_chip * 2 + core
    far = far_chip * 2 + core
    tok, _ = x_ref.shape
    top_k = ids_ref.shape[0]
    experts = wr_ref.shape[0]

    def at(dev):
        return (dev % 2) * chips + dev // 2

    half = tok // 2

    barrier = pltpu.get_barrier_semaphore()
    for k in range(1, n):
        pl.semaphore_signal(barrier, inc=1, device_id={'ep': (me + k) % n}, device_id_type=pl.DeviceIdType.MESH)

    x = x_ref[...].astype(F32)
    inv = lax.rsqrt(jnp.mean(x * x, axis=-1, keepdims=True) + EPSILON)
    h = (x * inv * g_ref[...].astype(F32)[None, :]).astype(BF16)
    hall[at(me)] = h
    logits = lax.dot_general(h, wr_ref[...], (((1,), (1,)), ((), ())), preferred_element_type=F32) + br_ref[...].astype(F32)[None, :]
    ids = ids_ref[...]
    expert = lax.broadcasted_iota(jnp.int32, (experts, tok), 0)
    turn = jnp.where(lax.broadcasted_iota(jnp.int32, (experts, experts), 0)
                     == lax.broadcasted_iota(jnp.int32, (experts, experts), 1), 1.0, 0.0).astype(BF16)
    hot = [dot_t(jnp.where(ids[k:k + 1, :] == expert, 1.0, 0.0).astype(BF16), turn) > 0.5 for k in range(top_k)]
    picked = [jnp.sum(jnp.where(hk, logits, 0.0), axis=1, keepdims=True) for hk in hot]
    top = functools.reduce(jnp.maximum, picked)
    ex = [jnp.exp(v - top) for v in picked]
    total = functools.reduce(jnp.add, ex)
    gates = jnp.zeros((tok, experts), F32)
    chosen = jnp.zeros((tok, experts), F32)
    for k in range(top_k):
        gates = gates + jnp.where(hot[k], ex[k] / total, 0.0)
        chosen = chosen + jnp.where(hot[k], 1.0, 0.0)
    mall[at(me), 0] = gates
    mall[at(me), 1] = chosen

    pl.semaphore_wait(barrier, n - 1)

    def copy(src, dst, ssem, rsem, dev):
        return pltpu.make_async_remote_copy(src_ref=src, dst_ref=dst, send_sem=ssem, recv_sem=rsem,
                                            device_id={'ep': dev}, device_id_type=pl.DeviceIdType.MESH)

    lo, hi = pl.ds(0, half), pl.ds(half, half)
    sends = []

    def start(c):
        c.start()
        sends.append(c)

    for i, (dev, parts) in enumerate(((right, (lo, hi)), (left, (hi, lo)))):
        for j, rows in enumerate(parts):
            start(copy(hall.at[at(me), rows], hall.at[at(me), rows], sb.at[i, j], rb.at[i, j], dev))
    start(copy(hall.at[at(me)], hall.at[at(me)], sa, ra, partner))
    metas = []
    for k in range(1, n):
        c = copy(mall.at[at(me)], mall.at[at(me)], sm.at[k - 1], rm.at[k - 1], (me + k) % n)
        c.start()
        metas.append(c)
    order = ((0, left, right, (lo, hi)), (1, right, left, (hi, lo)))
    for i, origin, onward, parts in order:
        slot = hall.at[at(origin), parts[0]]
        copy(slot, slot, sb.at[i, 0], rb.at[i, 0], origin).wait_recv()
        start(copy(slot, slot, sc.at[i], rc.at[i], onward))
        start(copy(slot, slot, sd.at[i, 0], rd.at[i, 0], partner))
    for i, origin, onward, parts in order:
        slot = hall.at[at(origin), parts[1]]
        copy(slot, slot, sb.at[i, 1], rb.at[i, 1], origin).wait_recv()
        start(copy(slot, slot, sd.at[i, 1], rd.at[i, 1], partner))
    for i, origin, onward, parts in order:
        slot = hall.at[at(far), parts[0]]
        copy(slot, slot, sc.at[i], rc.at[i], origin).wait_recv()
        start(copy(slot, slot, sd.at[i, 2], rd.at[i, 2], partner))

    for k in range(1, n):
        src = (me + n - k) % n
        copy(mall.at[at(src)], mall.at[at(src)], sm.at[k - 1], rm.at[k - 1], src).wait_recv()
    tokens = n * tok
    e0 = me * local_exp
    gates_all = mall[:, 0].reshape(tokens, experts)
    chosen_all = mall[:, 1].reshape(tokens, experts)
    lane_all = lax.broadcasted_iota(jnp.int32, (tokens, experts), 1)
    pick = (lax.broadcasted_iota(jnp.int32, (experts, 8), 0)
            == lax.broadcasted_iota(jnp.int32, (experts, 8), 1) + e0)
    pick = jnp.where(pick & (lax.broadcasted_iota(jnp.int32, (experts, 8), 1) < local_exp), 1.0, 0.0).astype(BF16)
    mine = dot32(chosen_all.astype(BF16), pick).astype(BF16)
    row = lax.broadcasted_iota(jnp.int32, (tokens, tokens), 0)
    col = lax.broadcasted_iota(jnp.int32, (tokens, tokens), 1)
    lower = jnp.where(col < row, 1.0, 0.0).astype(BF16)
    upper = jnp.where(row < col, 1.0, 0.0).astype(BF16)
    eye = jnp.where(row == col, 1.0, 0.0).astype(BF16)
    pos_ref[...] = jnp.where(mine.astype(F32) > 0.5, dot32(lower, mine), -1.0)
    post_ref[...] = jnp.where(dot_t(mine, eye) > 0.5, dot_t(mine, upper), -1.0)
    for e in range(local_exp):
        p_ref[:, e:e + 1] = jnp.sum(jnp.where(lane_all == e0 + e, gates_all, 0.0), axis=1, keepdims=True)

    copy(hall.at[at(partner)], hall.at[at(partner)], sa, ra, partner).wait_recv()
    for i, origin_chip, parts in ((0, left_chip, (lo, hi)), (1, right_chip, (hi, lo))):
        other = origin_chip * 2 + (1 - core)
        for j in range(2):
            slot = hall.at[at(other), parts[j]]
            copy(slot, slot, sd.at[i, j], rd.at[i, j], partner).wait_recv()
        slot = hall.at[at(far_chip * 2 + (1 - core)), parts[0]]
        copy(slot, slot, sd.at[i, 2], rd.at[i, 2], partner).wait_recv()
    for c in sends:
        c.wait_send()
    for c in metas:
        c.wait_send()


def dispatch(x, ids, g, wr, br, n, local_exp):
    tok, d_model = x.shape
    tokens = n * tok
    vm = pl.BlockSpec(memory_space=pltpu.VMEM)
    dma = pltpu.SemaphoreType.DMA
    hall, pos, post, p = pl.pallas_call(
        functools.partial(dispatch_kernel, n, local_exp),
        out_shape=(jax.ShapeDtypeStruct((n, tok, d_model), BF16),
                   jax.ShapeDtypeStruct((tokens, 8), F32),
                   jax.ShapeDtypeStruct((8, tokens), F32),
                   jax.ShapeDtypeStruct((tokens, local_exp), F32)),
        in_specs=[vm] * 5,
        out_specs=(vm,) * 4,
        scratch_shapes=[pltpu.VMEM((n, 2, tok, wr.shape[0]), F32),
                        dma, dma, dma((2, 2)), dma((2, 2)), dma((2,)), dma((2,)), dma((2, 3)), dma((2, 3)),
                        dma((n - 1,)), dma((n - 1,))],
        compiler_params=pltpu.CompilerParams(collective_id=0, has_side_effects=True, vmem_limit_bytes=VMEM_LIMIT),
        name='dispatch',
    )(x, ids, g, wr, br)
    return hall.reshape(tokens, d_model), pos, post, p


def gate_up_kernel(blk, m_blk, slots, hall, post_ref, w_hbm, b_ref, z_ref, wbuf, xg, perm, bias_ref, sems):
    local_exp, d_model, width = w_hbm.shape
    full, rest = width // blk, width % blk
    per_exp = full + (1 if rest else 0)
    total = local_exp * per_exp
    tokens = hall.shape[0]
    depth = slots - 1

    bias_ref[...] = b_ref[...].astype(F32)
    src = lax.broadcasted_iota(jnp.int32, (256, 256), 0)
    dst = lax.broadcasted_iota(jnp.int32, (256, 256), 1)
    want = jnp.where(dst < 128, 2 * dst, 2 * (dst - 128) + 1)
    perm[...] = jnp.where(src == want, 1.0, 0.0).astype(BF16)

    def block_copy(q, is_rest):
        e, j = q // per_exp, q % per_exp
        slot = q % slots
        if is_rest:
            return pltpu.make_async_copy(w_hbm.at[e, :, pl.ds(full * blk, rest)],
                                         wbuf.at[slot, :, pl.ds(0, rest)], sems.at[slot])
        return pltpu.make_async_copy(w_hbm.at[e, :, pl.ds(pl.multiple_of(j * blk, 128), blk)], wbuf.at[slot], sems.at[slot])

    def start(q):
        if not rest:
            block_copy(q, False).start()
            return
        j = lax.rem(q, per_exp)

        @pl.when(j < full)
        def _():
            block_copy(q, False).start()

        @pl.when(j == full)
        def _():
            block_copy(q, True).start()

    for q in range(depth):
        start(jnp.int32(q))

    def one_expert(e, carry):
        where_row = post_ref[pl.ds(e, 1), :]
        count = jnp.sum(jnp.where(where_row >= 0.0, 1.0, 0.0)).astype(jnp.int32)
        chunks = (count + (m_blk - 1)) // m_blk

        def gather(m, c):
            at = lax.broadcasted_iota(jnp.int32, (m_blk, tokens), 0) + m * m_blk
            onehot = jnp.where(at.astype(F32) == where_row, 1.0, 0.0).astype(BF16)
            xg[pl.ds(pl.multiple_of(m * m_blk, m_blk), m_blk), :] = dot32(onehot, hall[...]).astype(BF16)
            return c

        lax.fori_loop(0, chunks, gather, 0)

        def block(j, cols):
            q = e * per_exp + j
            slot = lax.rem(q, slots)

            @pl.when(q + depth < total)
            def _():
                start(q + depth)

            block_copy(q, cols != blk).wait()
            off = pl.multiple_of(j * blk, 128)
            bias = bias_ref[pl.ds(e, 1), pl.ds(off, cols)]

            def rows(m, c):
                at = pl.ds(pl.multiple_of(m * m_blk, m_blk), m_blk)
                u = (dot32(xg[at, :], wbuf[slot, :, :cols]) + bias).astype(BF16)
                for t in range(0, cols, 256):
                    wide = min(256, cols - t)
                    if wide == 256:
                        pm = perm[...]
                    else:
                        pm = jnp.concatenate([perm[:128, :64], perm[:128, 128:192]], axis=1)
                    al = dot32(u[:, t:t + wide], pm)
                    gate = jnp.minimum(al[:, :wide // 2], LIMIT)
                    linear = jnp.clip(al[:, wide // 2:], -LIMIT, LIMIT)
                    z = gate * jax.nn.sigmoid(ALPHA * gate) * (linear + 1.0)
                    zoff = pl.multiple_of(j * (blk // 2), 128) + t // 2
                    z_ref[e, at, pl.ds(zoff, wide // 2)] = z.astype(BF16)
                return c

            lax.fori_loop(0, chunks, rows, 0)

        def body(j, c):
            block(j, blk)
            return c

        lax.fori_loop(0, full, body, 0)
        if rest:
            block(jnp.int32(full), rest)
        return carry

    lax.fori_loop(0, local_exp, one_expert, 0)


def gate_up(hall, post, w, b, max_rows, blk, m_blk, slots):
    local_exp, d_model, width = w.shape
    vm = pl.BlockSpec(memory_space=pltpu.VMEM)
    return pl.pallas_call(
        functools.partial(gate_up_kernel, blk, m_blk, slots),
        out_shape=jax.ShapeDtypeStruct((local_exp, max_rows, width // 2), BF16),
        in_specs=[vm, vm, pl.BlockSpec(memory_space=pl.ANY), vm],
        out_specs=vm,
        scratch_shapes=[pltpu.VMEM((slots, d_model, blk), BF16), pltpu.VMEM((max_rows, d_model), BF16),
                        pltpu.VMEM((256, 256), BF16), pltpu.VMEM((local_exp, width), F32), pltpu.SemaphoreType.DMA((slots,))],
        compiler_params=pltpu.CompilerParams(vmem_limit_bytes=VMEM_LIMIT),
        name='gate_up',
    )(hall, post, w, b)


def down_kernel(n, chunks, slots, z_ref, pos_ref, p_ref, x_ref, b_ref, w_hbm, out_ref,
                wbuf, wrest, scat, part, part_r, near, near_r, ring, ring_r,
                wsem, rsem, ns, nr, fs, fr, hs, hr):
    local_exp, d_ff, width = w_hbm.shape
    tokens = pos_ref.shape[0]
    max_rows = z_ref.shape[1]
    tok = tokens // n
    half = tok // 2
    nchip = n // 2
    blk = chunks[0][1]
    total = len(chunks) * local_exp
    depth = slots - 1
    me = lax.axis_index('ep')
    chip, core = me // 2, me % 2
    partner = chip * 2 + (1 - core)
    right_chip, left_chip, far_chip = (chip + 1) % nchip, (chip + nchip - 1) % nchip, (chip + 2) % nchip
    right, left = right_chip * 2 + core, left_chip * 2 + core
    sides = ((right, right_chip, 0), (left, left_chip, 1))

    barrier = pltpu.get_barrier_semaphore()
    for dev in (partner, right, left):
        pl.semaphore_signal(barrier, inc=1, device_id={'ep': dev}, device_id_type=pl.DeviceIdType.MESH)

    def block_copy(q):
        off, cols = chunks[q // local_exp]
        src = w_hbm.at[q % local_exp, :, pl.ds(off, cols)]
        if cols == blk:
            return pltpu.make_async_copy(src, wbuf.at[q % slots], wsem.at[q % slots])
        return pltpu.make_async_copy(src, wrest.at[q % local_exp], rsem.at[q % local_exp])

    for q in range(depth):
        block_copy(q).start()

    def copy(src, dst, ssem, rsem_, dev):
        return pltpu.make_async_remote_copy(src_ref=src, dst_ref=dst, send_sem=ssem, recv_sem=rsem_,
                                            device_id={'ep': dev}, device_id_type=pl.DeviceIdType.MESH)

    def bufs(c):
        if chunks[c][1] == blk:
            return part.at[c], near.at[c], ring.at[c]
        return part_r, near_r, ring_r

    def near_copy(c):
        pb, nb, _ = bufs(c)
        return copy(pb.at[1 - core], nb, ns.at[c], nr.at[c], partner)

    def far_copy(c, side):
        dev, _, i = side
        pb, _, rb = bufs(c)
        rows = pl.ds(i * half, half)
        return copy(pb.at[core, far_chip, rows], rb.at[i, 0], fs.at[c, i, 0], fr.at[c, i, 0], dev)

    def early_copy(c, side):
        dev, dchip, i = side
        pb, _, rb = bufs(c)
        rows = pl.ds((1 - i) * half, half)
        return copy(pb.at[core, dchip, rows], rb.at[i, 1], fs.at[c, i, 1], fr.at[c, i, 1], dev)

    def late_copy(c, side):
        dev, dchip, i = side
        pb, _, rb = bufs(c)
        rows = pl.ds(i * half, half)
        return copy(pb.at[core, dchip, rows], rb.at[i, 2], hs.at[c, i], hr.at[c, i], dev)

    def stage_near(c):
        near_copy(c).start()

    def stage_far(c):
        near_copy(c).wait()
        pb, nb, _ = bufs(c)
        pb[core] += nb[...]
        for side in sides:
            far_copy(c, side).start()
            early_copy(c, side).start()

    def stage_late(c):
        pb, _, rb = bufs(c)
        for side in sides:
            _, dchip, i = side
            far_copy(c, side).wait_recv()
            pb[core, dchip, i * half:(i + 1) * half] += rb[i, 0]
            late_copy(c, side).start()

    def stage_out(c):
        off, cols = chunks[c]
        pb, _, rb = bufs(c)
        for side in sides:
            early_copy(c, side).wait_recv()
            late_copy(c, side).wait_recv()
        for r in range(2):
            rows = slice(r * half, (r + 1) * half)
            total_ = pb[core, chip, rows] + rb[0, 2 if r == 0 else 1] + rb[1, 1 if r == 0 else 2]
            out_ref[rows, off:off + cols] = (x_ref[rows, off:off + cols].astype(F32) + total_).astype(BF16)

    slot_ids = lax.broadcasted_iota(jnp.int32, (tokens, max_rows), 1).astype(F32)
    for e in range(local_exp):
        scat[e] = jnp.where(pos_ref[:, e:e + 1] == slot_ids, 1.0, 0.0).astype(BF16)
    row_ids = lax.broadcasted_iota(jnp.int32, (max_rows, 1), 0).astype(F32)
    counts = [jnp.max(pos_ref[:, e:e + 1]) + 1.0 for e in range(local_exp)]
    bias = b_ref[...].astype(F32)
    pl.semaphore_wait(barrier, 3)

    last = len(chunks)
    for c, (off, cols) in enumerate(chunks):
        pb = bufs(c)[0]
        for e in range(local_exp):
            q = c * local_exp + e
            if q + depth < total:
                block_copy(q + depth).start()
            block_copy(q).wait()
            wv = wbuf[q % slots] if cols == blk else wrest[e]
            y = dot32(z_ref[e], wv) + bias[e:e + 1, off:off + cols]
            y = jnp.where(row_ids < counts[e], y, 0.0).astype(BF16)
            add = (p_ref[:, e:e + 1] * dot32(scat[e], y)).reshape(2, nchip, tok, cols)
            if e == 0:
                pb[...] = add
            else:
                pb[...] += add
            if e == 0 and c >= 2:
                stage_out(c - 2)
            if e == 1 and c >= 1:
                stage_far(c - 1)
            if e == 3 and c >= 1:
                stage_late(c - 1)
        stage_near(c)
    stage_far(last - 1)
    stage_out(last - 2)
    stage_late(last - 1)
    stage_out(last - 1)
    for c in range(last):
        for side in sides:
            far_copy(c, side).wait_send()
            early_copy(c, side).wait_send()
            late_copy(c, side).wait_send()


def down(z, pos, p, x, w, b, n, blk, slots):
    local_exp, d_ff, width = w.shape
    tokens = pos.shape[0]
    tok = tokens // n
    chunks = [(c, min(blk, width - c)) for c in range(0, width, blk)]
    full, rest, last = width // blk, width % blk, len(chunks)
    vm = pl.BlockSpec(memory_space=pltpu.VMEM)
    dma = pltpu.SemaphoreType.DMA
    return pl.pallas_call(
        functools.partial(down_kernel, n, chunks, slots),
        out_shape=jax.ShapeDtypeStruct((tok, width), BF16),
        in_specs=[vm, vm, vm, vm, vm, pl.BlockSpec(memory_space=pl.ANY)],
        out_specs=vm,
        scratch_shapes=[pltpu.VMEM((slots, d_ff, blk), BF16), pltpu.VMEM((local_exp, d_ff, rest), BF16),
                        pltpu.VMEM((local_exp, tokens, z.shape[1]), BF16),
                        pltpu.VMEM((full, 2, n // 2, tok, blk), F32), pltpu.VMEM((2, n // 2, tok, rest), F32),
                        pltpu.VMEM((full, n // 2, tok, blk), F32), pltpu.VMEM((n // 2, tok, rest), F32),
                        pltpu.VMEM((full, 2, 3, tok // 2, blk), F32), pltpu.VMEM((2, 3, tok // 2, rest), F32),
                        dma((slots,)), dma((local_exp,)),
                        dma((last,)), dma((last,)), dma((last, 2, 2)), dma((last, 2, 2)), dma((last, 2)), dma((last, 2))],
        compiler_params=pltpu.CompilerParams(collective_id=1, has_side_effects=True, vmem_limit_bytes=VMEM_LIMIT),
        name='down',
    )(z, pos, p, x, b, w)


def solution(mesh):
    n = mesh.shape['ep']
    rows_spec = P(('dp', 'ep'), None)

    def local_block(x_in, expert_ids, norm_weight, router_w, router_b, w_gate_up, b_gate_up, w_down, b_down):
        tok, d_model = x_in.shape
        top_k = expert_ids.shape[1]
        local_exp = w_gate_up.shape[0]
        experts = local_exp * n
        max_rows = n * (4 * top_k * tok // experts)
        blk = 768 if w_gate_up.shape[2] >= 2048 else 256
        hall, pos, post, p = dispatch(x_in, expert_ids.T, norm_weight, router_w.T, router_b, n, local_exp)
        z = gate_up(hall, post, w_gate_up, b_gate_up, max_rows, blk, min(128, max_rows), 4)
        return down(z, pos, p, x_in, w_down, b_down, n, 512 if blk == 768 else 128, 4)

    return jax.shard_map(local_block, mesh=mesh, in_specs=(rows_spec, rows_spec, P(), P(), P(), P('ep', None, None), P('ep', None), P('ep', None, None), P('ep', None)), out_specs=rows_spec, check_vma=False)
```

```python
import functools

import jax
import jax.numpy as jnp
from jax import lax
from jax.experimental import pallas as pl
from jax.experimental.pallas import tpu as pltpu
from jax.sharding import PartitionSpec as P

EPSILON = 1e-5
LIMIT = 7.0
ALPHA = 1.702
F32 = jnp.float32
BF16 = jnp.bfloat16
DISPATCH_VMEM = 10 * 1024 * 1024
GATE_UP_VMEM = 20 * 1024 * 1024
DOWN_VMEM = 48 * 1024 * 1024


def dot32(a, b):
    return jnp.dot(a, b, preferred_element_type=F32)


def in_vmem(a):
    return pltpu.with_memory_space_constraint(a, pltpu.VMEM)


def dot_t(a, b):
    return lax.dot_general(a, b, (((0,), (0,)), ((), ())), preferred_element_type=F32)


def dispatch_kernel(n, local_exp, x_ref, ids_ref, g_ref, wr_ref, br_ref, w_hbm, hall, pos_ref, post_ref, p_ref, pre,
                    mall, psem, sa, ra, sb, rb, sc, rc, sd, rd, sm, rm):
    me = lax.axis_index('ep')
    chips = n // 2
    chip, core = me // 2, me % 2
    partner = chip * 2 + (1 - core)
    right_chip, left_chip = (chip + 1) % chips, (chip + chips - 1) % chips
    far_chip = (chip + 2) % chips
    right, left = right_chip * 2 + core, left_chip * 2 + core
    far = far_chip * 2 + core
    tok, _ = x_ref.shape
    top_k = ids_ref.shape[0]
    experts = wr_ref.shape[0]

    def at(dev):
        return (dev % 2) * chips + dev // 2

    half = tok // 2

    barrier = pltpu.get_barrier_semaphore()
    for k in range(1, n):
        pl.semaphore_signal(barrier, inc=1, device_id={'ep': (me + k) % n}, device_id_type=pl.DeviceIdType.MESH)
    blk = pre.shape[2]
    ahead = [pltpu.make_async_copy(w_hbm.at[0, :, pl.ds(j * blk, blk)], pre.at[j], psem.at[j]) for j in range(pre.shape[0])]
    for c in ahead:
        c.start()

    x = x_ref[...].astype(F32)
    inv = lax.rsqrt(jnp.mean(x * x, axis=-1, keepdims=True) + EPSILON)
    h = (x * inv * g_ref[...].astype(F32)[None, :]).astype(BF16)
    hall[at(me)] = h
    logits = lax.dot_general(h, wr_ref[...], (((1,), (1,)), ((), ())), preferred_element_type=F32) + br_ref[...].astype(F32)[None, :]
    ids = ids_ref[...]
    expert = lax.broadcasted_iota(jnp.int32, (experts, tok), 0)
    turn = jnp.where(lax.broadcasted_iota(jnp.int32, (experts, experts), 0)
                     == lax.broadcasted_iota(jnp.int32, (experts, experts), 1), 1.0, 0.0).astype(BF16)
    hot = [dot_t(jnp.where(ids[k:k + 1, :] == expert, 1.0, 0.0).astype(BF16), turn) > 0.5 for k in range(top_k)]
    picked = [jnp.sum(jnp.where(hk, logits, 0.0), axis=1, keepdims=True) for hk in hot]
    top = functools.reduce(jnp.maximum, picked)
    ex = [jnp.exp(v - top) for v in picked]
    total = functools.reduce(jnp.add, ex)
    gates = jnp.zeros((tok, experts), F32)
    chosen = jnp.zeros((tok, experts), F32)
    for k in range(top_k):
        gates = gates + jnp.where(hot[k], ex[k] / total, 0.0)
        chosen = chosen + jnp.where(hot[k], 1.0, 0.0)
    mall[at(me), 0] = gates
    mall[at(me), 1] = chosen

    pl.semaphore_wait(barrier, n - 1)

    def copy(src, dst, ssem, rsem, dev):
        return pltpu.make_async_remote_copy(src_ref=src, dst_ref=dst, send_sem=ssem, recv_sem=rsem,
                                            device_id={'ep': dev}, device_id_type=pl.DeviceIdType.MESH)

    lo, hi = pl.ds(0, half), pl.ds(half, half)
    sends = []

    def start(c):
        c.start()
        sends.append(c)

    for i, (dev, parts) in enumerate(((right, (lo, hi)), (left, (hi, lo)))):
        for j, rows in enumerate(parts):
            start(copy(hall.at[at(me), rows], hall.at[at(me), rows], sb.at[i, j], rb.at[i, j], dev))
    start(copy(hall.at[at(me)], hall.at[at(me)], sa, ra, partner))
    metas = []
    for k in range(1, n):
        c = copy(mall.at[at(me)], mall.at[at(me)], sm.at[k - 1], rm.at[k - 1], (me + k) % n)
        c.start()
        metas.append(c)
    order = ((0, left, right, (lo, hi)), (1, right, left, (hi, lo)))
    for i, origin, onward, parts in order:
        slot = hall.at[at(origin), parts[0]]
        copy(slot, slot, sb.at[i, 0], rb.at[i, 0], origin).wait_recv()
        start(copy(slot, slot, sc.at[i], rc.at[i], onward))
        start(copy(slot, slot, sd.at[i, 0], rd.at[i, 0], partner))
    for i, origin, onward, parts in order:
        slot = hall.at[at(origin), parts[1]]
        copy(slot, slot, sb.at[i, 1], rb.at[i, 1], origin).wait_recv()
        start(copy(slot, slot, sd.at[i, 1], rd.at[i, 1], partner))
    for i, origin, onward, parts in order:
        slot = hall.at[at(far), parts[0]]
        copy(slot, slot, sc.at[i], rc.at[i], origin).wait_recv()
        start(copy(slot, slot, sd.at[i, 2], rd.at[i, 2], partner))

    for k in range(1, n):
        src = (me + n - k) % n
        copy(mall.at[at(src)], mall.at[at(src)], sm.at[k - 1], rm.at[k - 1], src).wait_recv()
    tokens = n * tok
    e0 = me * local_exp
    gates_all = mall[:, 0].reshape(tokens, experts)
    chosen_all = mall[:, 1].reshape(tokens, experts)
    lane_all = lax.broadcasted_iota(jnp.int32, (tokens, experts), 1)
    pick = (lax.broadcasted_iota(jnp.int32, (experts, 8), 0)
            == lax.broadcasted_iota(jnp.int32, (experts, 8), 1) + e0)
    pick = jnp.where(pick & (lax.broadcasted_iota(jnp.int32, (experts, 8), 1) < local_exp), 1.0, 0.0).astype(BF16)
    mine = dot32(chosen_all.astype(BF16), pick).astype(BF16)
    row = lax.broadcasted_iota(jnp.int32, (tokens, tokens), 0)
    col = lax.broadcasted_iota(jnp.int32, (tokens, tokens), 1)
    lower = jnp.where(col < row, 1.0, 0.0).astype(BF16)
    upper = jnp.where(row < col, 1.0, 0.0).astype(BF16)
    eye = jnp.where(row == col, 1.0, 0.0).astype(BF16)
    pos_ref[...] = jnp.where(mine.astype(F32) > 0.5, dot32(lower, mine), -1.0)
    post_ref[...] = jnp.where(dot_t(mine, eye) > 0.5, dot_t(mine, upper), -1.0)
    for e in range(local_exp):
        p_ref[:, e:e + 1] = jnp.sum(jnp.where(lane_all == e0 + e, gates_all, 0.0), axis=1, keepdims=True)

    copy(hall.at[at(partner)], hall.at[at(partner)], sa, ra, partner).wait_recv()
    for i, origin_chip, parts in ((0, left_chip, (lo, hi)), (1, right_chip, (hi, lo))):
        other = origin_chip * 2 + (1 - core)
        for j in range(2):
            slot = hall.at[at(other), parts[j]]
            copy(slot, slot, sd.at[i, j], rd.at[i, j], partner).wait_recv()
        slot = hall.at[at(far_chip * 2 + (1 - core)), parts[0]]
        copy(slot, slot, sd.at[i, 2], rd.at[i, 2], partner).wait_recv()
    for c in sends:
        c.wait_send()
    for c in metas:
        c.wait_send()
    for c in ahead:
        c.wait()


def dispatch(x, ids, g, wr, br, w, n, local_exp, blk, npre):
    tok, d_model = x.shape
    tokens = n * tok
    vm = pl.BlockSpec(memory_space=pltpu.VMEM)
    dma = pltpu.SemaphoreType.DMA
    hall, pos, post, p, pre = pl.pallas_call(
        functools.partial(dispatch_kernel, n, local_exp),
        out_shape=(pltpu.VMEM((n, tok, d_model), BF16), pltpu.VMEM((tokens, 8), F32), pltpu.VMEM((8, tokens), F32),
                   pltpu.VMEM((tokens, local_exp), F32), pltpu.VMEM((npre, d_model, blk), BF16)),
        in_specs=[vm] * 5 + [pl.BlockSpec(memory_space=pl.ANY)],
        out_specs=(vm,) * 5,
        scratch_shapes=[pltpu.VMEM((n, 2, tok, wr.shape[0]), F32), dma((npre,)),
                        dma, dma, dma((2, 2)), dma((2, 2)), dma((2,)), dma((2,)), dma((2, 3)), dma((2, 3)),
                        dma((n - 1,)), dma((n - 1,))],
        compiler_params=pltpu.CompilerParams(collective_id=0, has_side_effects=True, vmem_limit_bytes=DISPATCH_VMEM),
        name='dispatch',
    )(x, ids, g, wr, br, w)
    return hall, pos, post, p, pre


def gate_up_kernel(m_blk, slots, hall, post_ref, pre, b_ref, w_hbm, z_ref, wbuf, xg, perm, bias_ref, sems):
    local_exp, d_model, width = w_hbm.shape
    npre, _, blk = pre.shape
    full, rest = width // blk, width % blk
    per_exp = full + (1 if rest else 0)
    total = local_exp * per_exp
    tokens = hall.shape[0] * hall.shape[1]
    depth = slots - 1

    def block_copy(q, is_rest):
        e, j = q // per_exp, q % per_exp
        slot = q % slots
        if is_rest:
            return pltpu.make_async_copy(w_hbm.at[e, :, pl.ds(full * blk, rest)],
                                         wbuf.at[slot, :, pl.ds(0, rest)], sems.at[slot])
        return pltpu.make_async_copy(w_hbm.at[e, :, pl.ds(pl.multiple_of(j * blk, 128), blk)], wbuf.at[slot], sems.at[slot])

    def start(q):
        j = q % per_exp

        @pl.when(j < full)
        def _():
            block_copy(q, False).start()

        if rest:
            @pl.when(j == full)
            def _():
                block_copy(q, True).start()

    for q in range(npre, npre + depth):
        start(q)

    bias_ref[...] = b_ref[...].astype(F32)
    src = lax.broadcasted_iota(jnp.int32, (256, 256), 0)
    dst = lax.broadcasted_iota(jnp.int32, (256, 256), 1)
    want = jnp.where(dst < 128, 2 * dst, 2 * (dst - 128) + 1)
    perm[...] = jnp.where(src == want, 1.0, 0.0).astype(BF16)

    def gather(e):
        where_row = post_ref[pl.ds(e, 1), :]
        count = jnp.sum(jnp.where(where_row >= 0.0, 1.0, 0.0)).astype(jnp.int32)
        chunks = (count + (m_blk - 1)) // m_blk

        def body(m, c):
            at = lax.broadcasted_iota(jnp.int32, (m_blk, tokens), 0) + m * m_blk
            onehot = jnp.where(at.astype(F32) == where_row, 1.0, 0.0).astype(BF16)
            xg[pl.ds(pl.multiple_of(m * m_blk, m_blk), m_blk), :] = dot32(onehot, hall[...].reshape(tokens, d_model)).astype(BF16)
            return c

        lax.fori_loop(0, chunks, body, 0)
        return chunks

    def compute(e, j, cols, chunks, weights):
        off = pl.multiple_of(j * blk, 128)
        bias = bias_ref[pl.ds(e, 1), pl.ds(off, cols)]

        def rows(m, c):
            at = pl.ds(pl.multiple_of(m * m_blk, m_blk), m_blk)
            u = (dot32(xg[at, :], weights()) + bias).astype(BF16)
            for t in range(0, cols, 256):
                wide = min(256, cols - t)
                if wide == 256:
                    pm = perm[...]
                else:
                    pm = jnp.concatenate([perm[:128, :64], perm[:128, 128:192]], axis=1)
                al = dot32(u[:, t:t + wide], pm)
                gate = jnp.minimum(al[:, :wide // 2], LIMIT)
                linear = jnp.clip(al[:, wide // 2:], -LIMIT, LIMIT)
                z = gate * jax.nn.sigmoid(ALPHA * gate) * (linear + 1.0)
                zoff = pl.multiple_of(j * (blk // 2), 128) + t // 2
                z_ref[e, at, pl.ds(zoff, wide // 2)] = z.astype(BF16)
            return c

        lax.fori_loop(0, chunks, rows, 0)

    def streamed(e, j, cols, chunks):
        q = e * per_exp + j
        slot = q % slots

        @pl.when(q + depth < total)
        def _():
            start(q + depth)

        block_copy(q, cols != blk).wait()
        compute(e, j, cols, chunks, lambda: wbuf[slot, :, :cols])

    def expert(e, first):
        chunks = gather(e)

        def from_pre(j, c):
            compute(e, j, blk, chunks, lambda: pre[j])
            return c

        def body(j, c):
            streamed(e, j, blk, chunks)
            return c

        if first:
            lax.fori_loop(0, npre, from_pre, 0)
        lax.fori_loop(npre if first else 0, full, body, 0)
        if rest:
            streamed(e, jnp.int32(full), rest, chunks)

    expert(0, True)

    def others(e, c):
        expert(e, False)
        return c

    lax.fori_loop(1, local_exp, others, 0)


def gate_up(hall, post, pre, w, b, max_rows, m_blk, slots):
    local_exp, d_model, width = w.shape
    blk = pre.shape[2]
    vm = pl.BlockSpec(memory_space=pltpu.VMEM)
    return pl.pallas_call(
        functools.partial(gate_up_kernel, m_blk, slots),
        out_shape=pltpu.VMEM((local_exp, max_rows, width // 2), BF16),
        in_specs=[vm, vm, vm, vm, pl.BlockSpec(memory_space=pl.ANY)],
        out_specs=vm,
        scratch_shapes=[pltpu.VMEM((slots, d_model, blk), BF16), pltpu.VMEM((max_rows, d_model), BF16),
                        pltpu.VMEM((256, 256), BF16), pltpu.VMEM((local_exp, width), F32), pltpu.SemaphoreType.DMA((slots,))],
        compiler_params=pltpu.CompilerParams(vmem_limit_bytes=GATE_UP_VMEM),
        name='gate_up',
    )(in_vmem(hall), in_vmem(post), in_vmem(pre), b, w)


def down_kernel(n, chunks, slots, z_ref, pos_ref, p_ref, x_ref, b_ref, w_hbm, out_ref,
                wbuf, wrest, scat, part, part_r, near, near_r, ring, ring_r,
                wsem, rsem, ns, nr, fs, fr, hs, hr):
    local_exp, d_ff, width = w_hbm.shape
    tokens = pos_ref.shape[0]
    max_rows = z_ref.shape[1]
    tok = tokens // n
    half = tok // 2
    nchip = n // 2
    blk = chunks[0][1]
    total = len(chunks) * local_exp
    depth = slots - 1
    me = lax.axis_index('ep')
    chip, core = me // 2, me % 2
    partner = chip * 2 + (1 - core)
    right_chip, left_chip, far_chip = (chip + 1) % nchip, (chip + nchip - 1) % nchip, (chip + 2) % nchip
    right, left = right_chip * 2 + core, left_chip * 2 + core
    sides = ((right, right_chip, 0), (left, left_chip, 1))

    barrier = pltpu.get_barrier_semaphore()
    for dev in (partner, right, left):
        pl.semaphore_signal(barrier, inc=1, device_id={'ep': dev}, device_id_type=pl.DeviceIdType.MESH)

    def block_copy(q):
        off, cols = chunks[q // local_exp]
        src = w_hbm.at[q % local_exp, :, pl.ds(off, cols)]
        if cols == blk:
            return pltpu.make_async_copy(src, wbuf.at[q % slots], wsem.at[q % slots])
        return pltpu.make_async_copy(src, wrest.at[q % local_exp], rsem.at[q % local_exp])

    for q in range(depth):
        block_copy(q).start()

    def copy(src, dst, ssem, rsem_, dev):
        return pltpu.make_async_remote_copy(src_ref=src, dst_ref=dst, send_sem=ssem, recv_sem=rsem_,
                                            device_id={'ep': dev}, device_id_type=pl.DeviceIdType.MESH)

    def bufs(c):
        if chunks[c][1] == blk:
            return part.at[c], near.at[c], ring.at[c]
        return part_r, near_r, ring_r

    def near_copy(c):
        pb, nb, _ = bufs(c)
        return copy(pb.at[1 - core], nb, ns.at[c], nr.at[c], partner)

    def far_copy(c, side):
        dev, _, i = side
        pb, _, rb = bufs(c)
        rows = pl.ds(i * half, half)
        return copy(pb.at[core, far_chip, rows], rb.at[i, 0], fs.at[c, i, 0], fr.at[c, i, 0], dev)

    def early_copy(c, side):
        dev, dchip, i = side
        pb, _, rb = bufs(c)
        rows = pl.ds((1 - i) * half, half)
        return copy(pb.at[core, dchip, rows], rb.at[i, 1], fs.at[c, i, 1], fr.at[c, i, 1], dev)

    def late_copy(c, side):
        dev, dchip, i = side
        pb, _, rb = bufs(c)
        rows = pl.ds(i * half, half)
        return copy(pb.at[core, dchip, rows], rb.at[i, 2], hs.at[c, i], hr.at[c, i], dev)

    def stage_near(c):
        near_copy(c).start()

    def stage_far(c):
        near_copy(c).wait()
        pb, nb, _ = bufs(c)
        pb[core] += nb[...]
        for side in sides:
            far_copy(c, side).start()
            early_copy(c, side).start()

    def stage_late(c):
        pb, _, rb = bufs(c)
        for side in sides:
            _, dchip, i = side
            far_copy(c, side).wait_recv()
            pb[core, dchip, i * half:(i + 1) * half] += rb[i, 0]
            late_copy(c, side).start()

    def stage_out(c):
        off, cols = chunks[c]
        pb, _, rb = bufs(c)
        for side in sides:
            early_copy(c, side).wait_recv()
            late_copy(c, side).wait_recv()
        for r in range(2):
            rows = slice(r * half, (r + 1) * half)
            total_ = pb[core, chip, rows] + rb[0, 2 if r == 0 else 1] + rb[1, 1 if r == 0 else 2]
            out_ref[rows, off:off + cols] = (x_ref[rows, off:off + cols].astype(F32) + total_).astype(BF16)

    slot_ids = lax.broadcasted_iota(jnp.int32, (tokens, max_rows), 1).astype(F32)
    for e in range(local_exp):
        scat[e] = jnp.where(pos_ref[:, e:e + 1] == slot_ids, 1.0, 0.0).astype(BF16)
    row_ids = lax.broadcasted_iota(jnp.int32, (max_rows, 1), 0).astype(F32)
    counts = [jnp.max(pos_ref[:, e:e + 1]) + 1.0 for e in range(local_exp)]
    bias = b_ref[...].astype(F32)
    pl.semaphore_wait(barrier, 3)

    last = len(chunks)
    for c, (off, cols) in enumerate(chunks):
        pb = bufs(c)[0]
        for e in range(local_exp):
            q = c * local_exp + e
            if q + depth < total:
                block_copy(q + depth).start()
            block_copy(q).wait()
            wv = wbuf[q % slots] if cols == blk else wrest[e]
            y = dot32(z_ref[e], wv) + bias[e:e + 1, off:off + cols]
            y = jnp.where(row_ids < counts[e], y, 0.0).astype(BF16)
            add = (p_ref[:, e:e + 1] * dot32(scat[e], y)).reshape(2, nchip, tok, cols)
            if e == 0:
                pb[...] = add
            else:
                pb[...] += add
            if e == 1:
                if c >= 1:
                    stage_far(c - 1)
                if c >= 2:
                    stage_late(c - 2)
                if c >= 3:
                    stage_out(c - 3)
        stage_near(c)
    stage_late(last - 2)
    stage_far(last - 1)
    stage_out(last - 3)
    stage_out(last - 2)
    stage_late(last - 1)
    stage_out(last - 1)
    for c in range(last):
        for side in sides:
            far_copy(c, side).wait_send()
            early_copy(c, side).wait_send()
            late_copy(c, side).wait_send()


def down(z, pos, p, x, w, b, n, blk, slots):
    local_exp, d_ff, width = w.shape
    tokens = pos.shape[0]
    tok = tokens // n
    chunks = [(c, min(blk, width - c)) for c in range(0, width, blk)]
    full, rest, last = width // blk, width % blk, len(chunks)
    vm = pl.BlockSpec(memory_space=pltpu.VMEM)
    dma = pltpu.SemaphoreType.DMA
    return pl.pallas_call(
        functools.partial(down_kernel, n, chunks, slots),
        out_shape=jax.ShapeDtypeStruct((tok, width), BF16),
        in_specs=[vm, vm, vm, vm, vm, pl.BlockSpec(memory_space=pl.ANY)],
        out_specs=vm,
        scratch_shapes=[pltpu.VMEM((slots, d_ff, blk), BF16), pltpu.VMEM((local_exp, d_ff, rest), BF16),
                        pltpu.VMEM((local_exp, tokens, z.shape[1]), BF16),
                        pltpu.VMEM((full, 2, n // 2, tok, blk), F32), pltpu.VMEM((2, n // 2, tok, rest), F32),
                        pltpu.VMEM((full, n // 2, tok, blk), F32), pltpu.VMEM((n // 2, tok, rest), F32),
                        pltpu.VMEM((full, 2, 3, tok // 2, blk), F32), pltpu.VMEM((2, 3, tok // 2, rest), F32),
                        dma((slots,)), dma((local_exp,)),
                        dma((last,)), dma((last,)), dma((last, 2, 2)), dma((last, 2, 2)), dma((last, 2)), dma((last, 2))],
        compiler_params=pltpu.CompilerParams(collective_id=1, has_side_effects=True, vmem_limit_bytes=DOWN_VMEM),
        name='down',
    )(in_vmem(z), in_vmem(pos), in_vmem(p), x, b, w)


def solution(mesh):
    n = mesh.shape['ep']
    rows_spec = P(('dp', 'ep'), None)

    def local_block(x_in, expert_ids, norm_weight, router_w, router_b, w_gate_up, b_gate_up, w_down, b_down):
        tok, d_model = x_in.shape
        top_k = expert_ids.shape[1]
        local_exp = w_gate_up.shape[0]
        experts = local_exp * n
        max_rows = n * (4 * top_k * tok // experts)
        blk = 768 if w_gate_up.shape[2] >= 2048 else 256
        npre = min(7, w_gate_up.shape[2] // blk)
        hall, pos, post, p, pre = dispatch(x_in, expert_ids.T, norm_weight, router_w.T, router_b, w_gate_up, n, local_exp, blk, npre)
        z = gate_up(hall, post, pre, w_gate_up, b_gate_up, max_rows, min(128, max_rows), 3)
        return down(z, pos, p, x_in, w_down, b_down, n, 512 if blk == 768 else 128, 4)

    return jax.shard_map(local_block, mesh=mesh, in_specs=(rows_spec, rows_spec, P(), P(), P(), P('ep', None, None), P('ep', None), P('ep', None, None), P('ep', None)), out_specs=rows_spec, check_vma=False)
```

```python
import functools

import jax
import jax.numpy as jnp
from jax import lax
from jax.experimental import pallas as pl
from jax.experimental.pallas import tpu as pltpu
from jax.sharding import PartitionSpec as P

EPSILON = 1e-5
LIMIT = 7.0
ALPHA = 1.702
F32 = jnp.float32
BF16 = jnp.bfloat16
DISPATCH_VMEM = 10 * 1024 * 1024
GATE_UP_VMEM = 22 * 1024 * 1024
DOWN_VMEM = 48 * 1024 * 1024


def dot32(a, b):
    return jnp.dot(a, b, preferred_element_type=F32)


def in_vmem(a):
    return pltpu.with_memory_space_constraint(a, pltpu.VMEM)


def vmem_out(shape, dtype):
    return pltpu.VMEM(shape, dtype)


def in_hbm(a):
    return pltpu.with_memory_space_constraint(a, pltpu.HBM)


def dot_t(a, b):
    return lax.dot_general(a, b, (((0,), (0,)), ((), ())), preferred_element_type=F32)


def dispatch_kernel(n, local_exp, x_hbm, ids_hbm, g_hbm, wr_hbm, br_hbm, w_hbm, hall, pos_ref, post_ref, p_ref, pre,
                    x_ref, ids_ref, g_ref, wr_ref, br_ref, isem, mall, psem, sa, ra, sb, rb, sc, rc, sd, rd, sm, rm):
    me = lax.axis_index('ep')
    chips = n // 2
    chip, core = me // 2, me % 2
    partner = chip * 2 + (1 - core)
    right_chip, left_chip = (chip + 1) % chips, (chip + chips - 1) % chips
    far_chip = (chip + 2) % chips
    right, left = right_chip * 2 + core, left_chip * 2 + core
    far = far_chip * 2 + core
    tok, _ = x_ref.shape
    top_k = ids_ref.shape[0]
    experts = wr_ref.shape[0]

    def at(dev):
        return (dev % 2) * chips + dev // 2

    half = tok // 2

    loads = [pltpu.make_async_copy(src, dst, isem.at[i]) for i, (src, dst) in enumerate(
        ((x_hbm, x_ref), (g_hbm, g_ref), (wr_hbm, wr_ref), (br_hbm, br_ref), (ids_hbm, ids_ref)))]
    for c in loads:
        c.start()
    barrier = pltpu.get_barrier_semaphore()
    for k in range(1, n):
        pl.semaphore_signal(barrier, inc=1, device_id={'ep': (me + k) % n}, device_id_type=pl.DeviceIdType.MESH)
    blk = pre.shape[2]
    ahead = [pltpu.make_async_copy(w_hbm.at[0, :, pl.ds(j * blk, blk)], pre.at[j], psem.at[j]) for j in range(pre.shape[0])]
    for c in loads:
        c.wait()
    for c in ahead:
        c.start()

    x = x_ref[...].astype(F32)
    inv = lax.rsqrt(jnp.mean(x * x, axis=-1, keepdims=True) + EPSILON)
    h = (x * inv * g_ref[...].astype(F32)[None, :]).astype(BF16)
    hall[at(me)] = h
    logits = lax.dot_general(h, wr_ref[...], (((1,), (1,)), ((), ())), preferred_element_type=F32) + br_ref[...].astype(F32)[None, :]
    ids = ids_ref[...]
    expert = lax.broadcasted_iota(jnp.int32, (experts, tok), 0)
    turn = jnp.where(lax.broadcasted_iota(jnp.int32, (experts, experts), 0)
                     == lax.broadcasted_iota(jnp.int32, (experts, experts), 1), 1.0, 0.0).astype(BF16)
    hot = [dot_t(jnp.where(ids[k:k + 1, :] == expert, 1.0, 0.0).astype(BF16), turn) > 0.5 for k in range(top_k)]
    picked = [jnp.sum(jnp.where(hk, logits, 0.0), axis=1, keepdims=True) for hk in hot]
    top = functools.reduce(jnp.maximum, picked)
    ex = [jnp.exp(v - top) for v in picked]
    total = functools.reduce(jnp.add, ex)
    gates = jnp.zeros((tok, experts), F32)
    chosen = jnp.zeros((tok, experts), F32)
    for k in range(top_k):
        gates = gates + jnp.where(hot[k], ex[k] / total, 0.0)
        chosen = chosen + jnp.where(hot[k], 1.0, 0.0)
    mall[at(me), 0] = gates
    mall[at(me), 1] = chosen

    pl.semaphore_wait(barrier, n - 1)

    def copy(src, dst, ssem, rsem, dev):
        return pltpu.make_async_remote_copy(src_ref=src, dst_ref=dst, send_sem=ssem, recv_sem=rsem,
                                            device_id={'ep': dev}, device_id_type=pl.DeviceIdType.MESH)

    lo, hi = pl.ds(0, half), pl.ds(half, half)
    sends = []

    def start(c):
        c.start()
        sends.append(c)

    for i, (dev, parts) in enumerate(((right, (lo, hi)), (left, (hi, lo)))):
        for j, rows in enumerate(parts):
            start(copy(hall.at[at(me), rows], hall.at[at(me), rows], sb.at[i, j], rb.at[i, j], dev))
    start(copy(hall.at[at(me)], hall.at[at(me)], sa, ra, partner))
    metas = []
    for k in range(1, n):
        c = copy(mall.at[at(me)], mall.at[at(me)], sm.at[k - 1], rm.at[k - 1], (me + k) % n)
        c.start()
        metas.append(c)
    order = ((0, left, right, (lo, hi)), (1, right, left, (hi, lo)))
    for i, origin, onward, parts in order:
        slot = hall.at[at(origin), parts[0]]
        copy(slot, slot, sb.at[i, 0], rb.at[i, 0], origin).wait_recv()
        start(copy(slot, slot, sc.at[i], rc.at[i], onward))
        start(copy(slot, slot, sd.at[i, 0], rd.at[i, 0], partner))
    for i, origin, onward, parts in order:
        slot = hall.at[at(origin), parts[1]]
        copy(slot, slot, sb.at[i, 1], rb.at[i, 1], origin).wait_recv()
        start(copy(slot, slot, sd.at[i, 1], rd.at[i, 1], partner))
    for i, origin, onward, parts in order:
        slot = hall.at[at(far), parts[0]]
        copy(slot, slot, sc.at[i], rc.at[i], origin).wait_recv()
        start(copy(slot, slot, sd.at[i, 2], rd.at[i, 2], partner))

    for k in range(1, n):
        src = (me + n - k) % n
        copy(mall.at[at(src)], mall.at[at(src)], sm.at[k - 1], rm.at[k - 1], src).wait_recv()
    tokens = n * tok
    e0 = me * local_exp
    gates_all = mall[:, 0].reshape(tokens, experts)
    chosen_all = mall[:, 1].reshape(tokens, experts)
    lane_all = lax.broadcasted_iota(jnp.int32, (tokens, experts), 1)
    pick = (lax.broadcasted_iota(jnp.int32, (experts, 8), 0)
            == lax.broadcasted_iota(jnp.int32, (experts, 8), 1) + e0)
    pick = jnp.where(pick & (lax.broadcasted_iota(jnp.int32, (experts, 8), 1) < local_exp), 1.0, 0.0).astype(BF16)
    mine = dot32(chosen_all.astype(BF16), pick).astype(BF16)
    row = lax.broadcasted_iota(jnp.int32, (tokens, tokens), 0)
    col = lax.broadcasted_iota(jnp.int32, (tokens, tokens), 1)
    lower = jnp.where(col < row, 1.0, 0.0).astype(BF16)
    upper = jnp.where(row < col, 1.0, 0.0).astype(BF16)
    eye = jnp.where(row == col, 1.0, 0.0).astype(BF16)
    pos_ref[...] = jnp.where(mine.astype(F32) > 0.5, dot32(lower, mine), -1.0)
    post_ref[...] = jnp.where(dot_t(mine, eye) > 0.5, dot_t(mine, upper), -1.0)
    for e in range(local_exp):
        p_ref[:, e:e + 1] = jnp.sum(jnp.where(lane_all == e0 + e, gates_all, 0.0), axis=1, keepdims=True)

    copy(hall.at[at(partner)], hall.at[at(partner)], sa, ra, partner).wait_recv()
    for i, origin_chip, parts in ((0, left_chip, (lo, hi)), (1, right_chip, (hi, lo))):
        other = origin_chip * 2 + (1 - core)
        for j in range(2):
            slot = hall.at[at(other), parts[j]]
            copy(slot, slot, sd.at[i, j], rd.at[i, j], partner).wait_recv()
        slot = hall.at[at(far_chip * 2 + (1 - core)), parts[0]]
        copy(slot, slot, sd.at[i, 2], rd.at[i, 2], partner).wait_recv()
    for c in sends:
        c.wait_send()
    for c in metas:
        c.wait_send()
    for c in ahead:
        c.wait()


def dispatch(x, ids, g, wr, br, w, n, local_exp, blk, npre):
    tok, d_model = x.shape
    tokens = n * tok
    vm = pl.BlockSpec(memory_space=pltpu.VMEM)
    hbm = pl.BlockSpec(memory_space=pltpu.HBM)
    dma = pltpu.SemaphoreType.DMA
    hall, pos, post, p, pre = pl.pallas_call(
        functools.partial(dispatch_kernel, n, local_exp),
        out_shape=(vmem_out((n, tok, d_model), BF16), vmem_out((tokens, 8), F32), vmem_out((8, tokens), F32),
                   vmem_out((tokens, local_exp), F32), vmem_out((npre, d_model, blk), BF16)),
        in_specs=[hbm] * 6,
        out_specs=(vm,) * 5,
        scratch_shapes=[pltpu.VMEM(x.shape, x.dtype), pltpu.VMEM(ids.shape, ids.dtype), pltpu.VMEM(g.shape, g.dtype),
                        pltpu.VMEM(wr.shape, wr.dtype), pltpu.VMEM(br.shape, br.dtype), dma((5,)),
                        pltpu.VMEM((n, 2, tok, wr.shape[0]), F32), dma((npre,)),
                        dma, dma, dma((2, 2)), dma((2, 2)), dma((2,)), dma((2,)), dma((2, 3)), dma((2, 3)),
                        dma((n - 1,)), dma((n - 1,))],
        compiler_params=pltpu.CompilerParams(collective_id=0, has_side_effects=True, vmem_limit_bytes=DISPATCH_VMEM),
        name='dispatch',
    )(in_hbm(x), in_hbm(ids), in_hbm(g), in_hbm(wr), in_hbm(br), w)
    return hall, pos, post, p, pre


def gate_up_kernel(m_blk, slots, hall, post_ref, pre, b_ref, w_hbm, z_ref,
                   wbuf, xg, ubuf, perm, bias_ref, sems):
    local_exp, d_model, width = w_hbm.shape
    npre, _, blk = pre.shape
    full, rest = width // blk, width % blk
    per_exp = full + (1 if rest else 0)
    total = local_exp * per_exp
    tokens = hall.shape[0] * hall.shape[1]
    depth = slots - 1

    def block_copy(q, is_rest):
        e, j = q // per_exp, q % per_exp
        slot = q % slots
        if is_rest:
            return pltpu.make_async_copy(w_hbm.at[e, :, pl.ds(full * blk, rest)],
                                         wbuf.at[slot, :, pl.ds(0, rest)], sems.at[slot])
        return pltpu.make_async_copy(w_hbm.at[e, :, pl.ds(pl.multiple_of(j * blk, 128), blk)], wbuf.at[slot], sems.at[slot])

    def start(q):
        j = q % per_exp

        @pl.when(j < full)
        def _():
            block_copy(q, False).start()

        if rest:
            @pl.when(j == full)
            def _():
                block_copy(q, True).start()

    for q in range(npre, npre + depth):
        start(q)

    bias_ref[...] = b_ref[...].astype(F32)
    src = lax.broadcasted_iota(jnp.int32, (256, 256), 0)
    dst = lax.broadcasted_iota(jnp.int32, (256, 256), 1)
    want = jnp.where(dst < 128, 2 * dst, 2 * (dst - 128) + 1)
    perm[...] = jnp.where(src == want, 1.0, 0.0).astype(BF16)

    def gather(e):
        where_row = post_ref[pl.ds(e, 1), :]
        count = jnp.sum(jnp.where(where_row >= 0.0, 1.0, 0.0)).astype(jnp.int32)
        chunks = (count + (m_blk - 1)) // m_blk

        def body(m, c):
            at = lax.broadcasted_iota(jnp.int32, (m_blk, tokens), 0) + m * m_blk
            onehot = jnp.where(at.astype(F32) == where_row, 1.0, 0.0).astype(BF16)
            xg[pl.ds(pl.multiple_of(m * m_blk, m_blk), m_blk), :] = dot32(onehot, hall[...].reshape(tokens, d_model)).astype(BF16)
            return c

        lax.fori_loop(0, chunks, body, 0)
        return chunks

    def glu(e, j, m, cols):
        at = pl.ds(pl.multiple_of(m * m_blk, m_blk), m_blk)
        for t in range(0, cols, 256):
            wide = min(256, cols - t)
            if wide == 256:
                pm = perm[...]
            else:
                pm = jnp.concatenate([perm[:128, :64], perm[:128, 128:192]], axis=1)
            al = dot32(ubuf[m, :, t:t + wide], pm)
            gate = jnp.minimum(al[:, :wide // 2], LIMIT)
            linear = jnp.clip(al[:, wide // 2:], -LIMIT, LIMIT)
            z = gate * jax.nn.sigmoid(ALPHA * gate) * (linear + 1.0)
            zoff = pl.multiple_of(j * (blk // 2), 128) + t // 2
            z_ref[e, at, pl.ds(zoff, wide // 2)] = z.astype(BF16)

    def compute(e, j, cols, chunks, weights):
        off = pl.multiple_of(j * blk, 128)
        bias = bias_ref[pl.ds(e, 1), pl.ds(off, cols)]
        before = j - 1 if isinstance(j, int) else jnp.maximum(j - 1, 0)

        def rows(m, c):
            at = pl.ds(pl.multiple_of(m * m_blk, m_blk), m_blk)
            glu(e, before, m, blk)
            ubuf[m, :, :cols] = (dot32(xg[at, :], weights()) + bias).astype(BF16)
            return c

        lax.fori_loop(0, chunks, rows, 0)

    def streamed(e, j, cols, chunks):
        q = e * per_exp + j
        slot = q % slots

        @pl.when(q + depth < total)
        def _():
            start(q + depth)

        block_copy(q, cols != blk).wait()
        compute(e, j, cols, chunks, lambda: wbuf[slot, :, :cols])

    def expert(e, first):
        chunks = gather(e)

        def from_pre(j, c):
            compute(e, j, blk, chunks, lambda: pre[j])
            return c

        def body(j, c):
            streamed(e, j, blk, chunks)
            return c

        if first:
            lax.fori_loop(0, npre, from_pre, 0)
        lax.fori_loop(npre if first else 0, full, body, 0)
        streamed(e, full, rest, chunks)

        def end(m, c):
            glu(e, full, m, rest)
            return c

        lax.fori_loop(0, chunks, end, 0)

    expert(0, True)

    def others(e, c):
        expert(e, False)
        return c

    lax.fori_loop(1, local_exp, others, 0)


def gate_up(hall, post, pre, w, b, max_rows, m_blk, slots):
    local_exp, d_model, width = w.shape
    blk = pre.shape[2]
    vm = pl.BlockSpec(memory_space=pltpu.VMEM)
    hbm = pl.BlockSpec(memory_space=pl.ANY)
    return pl.pallas_call(
        functools.partial(gate_up_kernel, m_blk, slots),
        out_shape=vmem_out((local_exp, max_rows, width // 2), BF16),
        in_specs=[vm, vm, vm, vm, hbm],
        out_specs=vm,
        scratch_shapes=[pltpu.VMEM((slots, d_model, blk), BF16), pltpu.VMEM((max_rows, d_model), BF16),
                        pltpu.VMEM((max_rows // m_blk, m_blk, blk), BF16),
                        pltpu.VMEM((256, 256), BF16), pltpu.VMEM((local_exp, width), F32), pltpu.SemaphoreType.DMA((slots,))],
        compiler_params=pltpu.CompilerParams(vmem_limit_bytes=GATE_UP_VMEM),
        name='gate_up',
    )(in_vmem(hall), in_vmem(post), in_vmem(pre), b, w)


def down_kernel(n, chunks, slots, z_ref, pos_ref, p_ref, x_ref, b_ref, w_hbm, out_ref,
                wbuf, wrest, scat, part, part_r, near, near_r, ring, ring_r,
                wsem, rsem, ns, nr, fs, fr, hs, hr):
    local_exp, d_ff, width = w_hbm.shape
    tokens = pos_ref.shape[0]
    max_rows = z_ref.shape[1]
    tok = tokens // n
    half = tok // 2
    nchip = n // 2
    blk = chunks[0][1]
    total = len(chunks) * local_exp
    depth = slots - 1
    me = lax.axis_index('ep')
    chip, core = me // 2, me % 2
    partner = chip * 2 + (1 - core)
    right_chip, left_chip, far_chip = (chip + 1) % nchip, (chip + nchip - 1) % nchip, (chip + 2) % nchip
    right, left = right_chip * 2 + core, left_chip * 2 + core
    sides = ((right, right_chip, 0), (left, left_chip, 1))

    barrier = pltpu.get_barrier_semaphore()
    for dev in (partner, right, left):
        pl.semaphore_signal(barrier, inc=1, device_id={'ep': dev}, device_id_type=pl.DeviceIdType.MESH)

    def block_copy(q):
        off, cols = chunks[q // local_exp]
        src = w_hbm.at[q % local_exp, :, pl.ds(off, cols)]
        if cols == blk:
            return pltpu.make_async_copy(src, wbuf.at[q % slots], wsem.at[q % slots])
        return pltpu.make_async_copy(src, wrest.at[q % slots], rsem.at[q % slots])

    def weights(q, cols):
        return wbuf[q % slots] if cols == blk else wrest[q % slots]

    for q in range(depth):
        block_copy(q).start()

    def copy(src, dst, ssem, rsem_, dev):
        return pltpu.make_async_remote_copy(src_ref=src, dst_ref=dst, send_sem=ssem, recv_sem=rsem_,
                                            device_id={'ep': dev}, device_id_type=pl.DeviceIdType.MESH)

    def bufs(c):
        if chunks[c][1] == blk:
            return part.at[c], near.at[c], ring.at[c]
        return part_r, near_r, ring_r

    def near_copy(c):
        pb, nb, _ = bufs(c)
        return copy(pb.at[1 - core], nb, ns.at[c], nr.at[c], partner)

    def far_copy(c, side):
        dev, _, i = side
        pb, _, rb = bufs(c)
        rows = pl.ds(i * half, half)
        return copy(pb.at[core, far_chip, rows], rb.at[i, 0], fs.at[c, i, 0], fr.at[c, i, 0], dev)

    def early_copy(c, side):
        dev, dchip, i = side
        pb, _, rb = bufs(c)
        rows = pl.ds((1 - i) * half, half)
        return copy(pb.at[core, dchip, rows], rb.at[i, 1], fs.at[c, i, 1], fr.at[c, i, 1], dev)

    def late_copy(c, side):
        dev, dchip, i = side
        pb, _, rb = bufs(c)
        rows = pl.ds(i * half, half)
        return copy(pb.at[core, dchip, rows], rb.at[i, 2], hs.at[c, i], hr.at[c, i], dev)

    def stage_near(c):
        near_copy(c).start()

    def stage_far(c):
        near_copy(c).wait()
        pb, nb, _ = bufs(c)
        pb[core] += nb[...]
        for side in sides:
            far_copy(c, side).start()
            early_copy(c, side).start()

    def stage_late(c):
        pb, _, rb = bufs(c)
        for side in sides:
            _, dchip, i = side
            far_copy(c, side).wait_recv()
            pb[core, dchip, i * half:(i + 1) * half] += rb[i, 0]
            late_copy(c, side).start()

    def stage_out(c):
        off, cols = chunks[c]
        pb, _, rb = bufs(c)
        for side in sides:
            early_copy(c, side).wait_recv()
            late_copy(c, side).wait_recv()
        for r in range(2):
            rows = slice(r * half, (r + 1) * half)
            total_ = pb[core, chip, rows] + rb[0, 2 if r == 0 else 1] + rb[1, 1 if r == 0 else 2]
            out_ref[rows, off:off + cols] = (x_ref[rows, off:off + cols].astype(F32) + total_).astype(BF16)

    slot_ids = lax.broadcasted_iota(jnp.int32, (tokens, max_rows), 1).astype(F32)
    for e in range(local_exp):
        scat[e] = jnp.where(pos_ref[:, e:e + 1] == slot_ids, 1.0, 0.0).astype(BF16)
    row_ids = lax.broadcasted_iota(jnp.int32, (max_rows, 1), 0).astype(F32)
    counts = [jnp.max(pos_ref[:, e:e + 1]) + 1.0 for e in range(local_exp)]
    bias = b_ref[...].astype(F32)
    pl.semaphore_wait(barrier, 3)

    last = len(chunks)
    for c, (off, cols) in enumerate(chunks):
        pb = bufs(c)[0]
        for e in range(local_exp):
            q = c * local_exp + e
            if q + depth < total:
                block_copy(q + depth).start()
            block_copy(q).wait()
            y = dot32(z_ref[e], weights(q, cols)) + bias[e:e + 1, off:off + cols]
            y = jnp.where(row_ids < counts[e], y, 0.0).astype(BF16)
            add = (p_ref[:, e:e + 1] * dot32(scat[e], y)).reshape(2, nchip, tok, cols)
            if e == 0:
                pb[...] = add
            else:
                pb[...] += add
            if e == 1:
                if c >= 1:
                    stage_far(c - 1)
            if e == 2:
                if c >= 2:
                    stage_late(c - 2)
                if c >= 3:
                    stage_out(c - 3)
        stage_near(c)
    stage_late(last - 2)
    stage_far(last - 1)
    stage_out(last - 3)
    stage_out(last - 2)
    stage_late(last - 1)
    stage_out(last - 1)
    for c in range(last):
        for side in sides:
            far_copy(c, side).wait_send()
            early_copy(c, side).wait_send()
            late_copy(c, side).wait_send()


def down(z, pos, p, x, w, b, n, blk, slots):
    local_exp, d_ff, width = w.shape
    tokens = pos.shape[0]
    tok = tokens // n
    chunks = [(c, min(blk, width - c)) for c in range(0, width, blk)]
    full, rest, last = width // blk, width % blk, len(chunks)
    vm = pl.BlockSpec(memory_space=pltpu.VMEM)
    dma = pltpu.SemaphoreType.DMA
    return pl.pallas_call(
        functools.partial(down_kernel, n, chunks, slots),
        out_shape=jax.ShapeDtypeStruct((tok, width), BF16),
        in_specs=[vm, vm, vm, vm, vm, pl.BlockSpec(memory_space=pl.ANY)],
        out_specs=vm,
        scratch_shapes=[pltpu.VMEM((slots, d_ff, blk), BF16), pltpu.VMEM((slots, d_ff, rest), BF16),
                        pltpu.VMEM((local_exp, tokens, z.shape[1]), BF16),
                        pltpu.VMEM((full, 2, n // 2, tok, blk), F32), pltpu.VMEM((2, n // 2, tok, rest), F32),
                        pltpu.VMEM((full, n // 2, tok, blk), F32), pltpu.VMEM((n // 2, tok, rest), F32),
                        pltpu.VMEM((full, 2, 3, tok // 2, blk), F32), pltpu.VMEM((2, 3, tok // 2, rest), F32),
                        dma((slots,)), dma((slots,)),
                        dma((last,)), dma((last,)), dma((last, 2, 2)), dma((last, 2, 2)), dma((last, 2)), dma((last, 2))],
        compiler_params=pltpu.CompilerParams(collective_id=1, has_side_effects=True, vmem_limit_bytes=DOWN_VMEM),
        name='down',
    )(in_vmem(z), in_vmem(pos), in_vmem(p), x, b, w)


def solution(mesh):
    n = mesh.shape['ep']
    rows_spec = P(('dp', 'ep'), None)

    def local_block(x_in, expert_ids, norm_weight, router_w, router_b, w_gate_up, b_gate_up, w_down, b_down):
        tok, d_model = x_in.shape
        top_k = expert_ids.shape[1]
        local_exp = w_gate_up.shape[0]
        experts = local_exp * n
        max_rows = n * (4 * top_k * tok // experts)
        wide = w_gate_up.shape[2] >= 2048
        blk, dcol = (1024, 512) if wide else (256, 128)
        npre = w_gate_up.shape[2] // blk
        hall, pos, post, p, pre = dispatch(x_in, expert_ids.T, norm_weight, router_w.T, router_b, w_gate_up, n, local_exp, blk, npre)
        z = gate_up(hall, post, pre, w_gate_up, b_gate_up, max_rows, min(128, max_rows), 3)
        return down(z, pos, p, x_in, w_down, b_down, n, dcol, 4)

    return jax.shard_map(local_block, mesh=mesh, in_specs=(rows_spec, rows_spec, P(), P(), P(), P('ep', None, None), P('ep', None), P('ep', None, None), P('ep', None)), out_specs=rows_spec, check_vma=False)
```

```python
import functools

import jax
import jax.numpy as jnp
from jax import lax
from jax.experimental import pallas as pl
from jax.experimental.pallas import tpu as pltpu
from jax.sharding import PartitionSpec as P

EPSILON = 1e-5
LIMIT = 7.0
ALPHA = 1.702
F32 = jnp.float32
BF16 = jnp.bfloat16
DISPATCH_VMEM = 10 * 1024 * 1024
GATE_UP_VMEM = 23 * 1024 * 1024
DOWN_VMEM = 30 * 1024 * 1024


def dot32(a, b):
    return jnp.dot(a, b, preferred_element_type=F32)


def in_vmem(a):
    return pltpu.with_memory_space_constraint(a, pltpu.VMEM)


def vmem_out(shape, dtype):
    return pltpu.VMEM(shape, dtype)


def in_hbm(a):
    return pltpu.with_memory_space_constraint(a, pltpu.HBM)


def dot_t(a, b):
    return lax.dot_general(a, b, (((0,), (0,)), ((), ())), preferred_element_type=F32)


def dispatch_kernel(n, local_exp, x_hbm, ids_hbm, g_hbm, wr_hbm, br_hbm, w_hbm, hall, pos_ref, post_ref, p_ref, pre,
                    x_ref, ids_ref, g_ref, wr_ref, br_ref, isem, mall, psem, sa, ra, sb, rb, sc, rc, sd, rd, sm, rm):
    me = lax.axis_index('ep')
    chips = n // 2
    chip, core = me // 2, me % 2
    partner = chip * 2 + (1 - core)
    right_chip, left_chip = (chip + 1) % chips, (chip + chips - 1) % chips
    far_chip = (chip + 2) % chips
    right, left = right_chip * 2 + core, left_chip * 2 + core
    far = far_chip * 2 + core
    tok, _ = x_ref.shape
    top_k = ids_ref.shape[0]
    experts = wr_ref.shape[0]

    def at(dev):
        return (dev % 2) * chips + dev // 2

    half = tok // 2

    loads = [pltpu.make_async_copy(src, dst, isem.at[i]) for i, (src, dst) in enumerate(
        ((x_hbm, x_ref), (g_hbm, g_ref), (wr_hbm, wr_ref), (br_hbm, br_ref), (ids_hbm, ids_ref)))]
    for c in loads:
        c.start()
    barrier = pltpu.get_barrier_semaphore()
    for k in range(1, n):
        pl.semaphore_signal(barrier, inc=1, device_id={'ep': (me + k) % n}, device_id_type=pl.DeviceIdType.MESH)
    blk = pre.shape[2]
    ahead = [pltpu.make_async_copy(w_hbm.at[0, :, pl.ds(j * blk, blk)], pre.at[j], psem.at[j]) for j in range(pre.shape[0])]
    for c in loads:
        c.wait()
    for c in ahead:
        c.start()

    x = x_ref[...].astype(F32)
    inv = lax.rsqrt(jnp.mean(x * x, axis=-1, keepdims=True) + EPSILON)
    h = (x * inv * g_ref[...].astype(F32)[None, :]).astype(BF16)
    hall[at(me)] = h

    pl.semaphore_wait(barrier, n - 1)

    def copy(src, dst, ssem, rsem, dev):
        return pltpu.make_async_remote_copy(src_ref=src, dst_ref=dst, send_sem=ssem, recv_sem=rsem,
                                            device_id={'ep': dev}, device_id_type=pl.DeviceIdType.MESH)

    lo, hi = pl.ds(0, half), pl.ds(half, half)
    sends = []

    def start(c):
        c.start()
        sends.append(c)

    for i, (dev, parts) in enumerate(((right, (lo, hi)), (left, (hi, lo)))):
        for j, rows in enumerate(parts):
            start(copy(hall.at[at(me), rows], hall.at[at(me), rows], sb.at[i, j], rb.at[i, j], dev))
    start(copy(hall.at[at(me)], hall.at[at(me)], sa, ra, partner))
    logits = lax.dot_general(h, wr_ref[...], (((1,), (1,)), ((), ())), preferred_element_type=F32) + br_ref[...].astype(F32)[None, :]
    ids = ids_ref[...]
    expert = lax.broadcasted_iota(jnp.int32, (experts, tok), 0)
    turn = jnp.where(lax.broadcasted_iota(jnp.int32, (experts, experts), 0)
                     == lax.broadcasted_iota(jnp.int32, (experts, experts), 1), 1.0, 0.0).astype(BF16)
    hot = [dot_t(jnp.where(ids[k:k + 1, :] == expert, 1.0, 0.0).astype(BF16), turn) > 0.5 for k in range(top_k)]
    picked = [jnp.sum(jnp.where(hk, logits, 0.0), axis=1, keepdims=True) for hk in hot]
    top = functools.reduce(jnp.maximum, picked)
    ex = [jnp.exp(v - top) for v in picked]
    total = functools.reduce(jnp.add, ex)
    gates = jnp.zeros((tok, experts), F32)
    chosen = jnp.zeros((tok, experts), F32)
    for k in range(top_k):
        gates = gates + jnp.where(hot[k], ex[k] / total, 0.0)
        chosen = chosen + jnp.where(hot[k], 1.0, 0.0)
    mall[at(me), 0] = gates
    mall[at(me), 1] = chosen
    metas = []
    for k in range(1, n):
        c = copy(mall.at[at(me)], mall.at[at(me)], sm.at[k - 1], rm.at[k - 1], (me + k) % n)
        c.start()
        metas.append(c)
    order = ((0, left, right, (lo, hi)), (1, right, left, (hi, lo)))
    for i, origin, onward, parts in order:
        slot = hall.at[at(origin), parts[0]]
        copy(slot, slot, sb.at[i, 0], rb.at[i, 0], origin).wait_recv()
        start(copy(slot, slot, sc.at[i], rc.at[i], onward))
        start(copy(slot, slot, sd.at[i, 0], rd.at[i, 0], partner))
    for k in range(1, n):
        src = (me + n - k) % n
        copy(mall.at[at(src)], mall.at[at(src)], sm.at[k - 1], rm.at[k - 1], src).wait_recv()
    tokens = n * tok
    e0 = me * local_exp
    gates_all = mall[:, 0].reshape(tokens, experts)
    chosen_all = mall[:, 1].reshape(tokens, experts)
    lane_all = lax.broadcasted_iota(jnp.int32, (tokens, experts), 1)
    pick = (lax.broadcasted_iota(jnp.int32, (experts, 8), 0)
            == lax.broadcasted_iota(jnp.int32, (experts, 8), 1) + e0)
    pick = jnp.where(pick & (lax.broadcasted_iota(jnp.int32, (experts, 8), 1) < local_exp), 1.0, 0.0).astype(BF16)
    mine = dot32(chosen_all.astype(BF16), pick).astype(BF16)
    row = lax.broadcasted_iota(jnp.int32, (tokens, tokens), 0)
    col = lax.broadcasted_iota(jnp.int32, (tokens, tokens), 1)
    lower = jnp.where(col < row, 1.0, 0.0).astype(BF16)
    upper = jnp.where(row < col, 1.0, 0.0).astype(BF16)
    eye = jnp.where(row == col, 1.0, 0.0).astype(BF16)
    pos_ref[...] = jnp.where(mine.astype(F32) > 0.5, dot32(lower, mine), -1.0)
    post_ref[...] = jnp.where(dot_t(mine, eye) > 0.5, dot_t(mine, upper), -1.0)
    for e in range(local_exp):
        p_ref[:, e:e + 1] = jnp.sum(jnp.where(lane_all == e0 + e, gates_all, 0.0), axis=1, keepdims=True)
    for i, origin, onward, parts in order:
        slot = hall.at[at(origin), parts[1]]
        copy(slot, slot, sb.at[i, 1], rb.at[i, 1], origin).wait_recv()
        start(copy(slot, slot, sd.at[i, 1], rd.at[i, 1], partner))
    for i, origin, onward, parts in order:
        slot = hall.at[at(far), parts[0]]
        copy(slot, slot, sc.at[i], rc.at[i], origin).wait_recv()
        start(copy(slot, slot, sd.at[i, 2], rd.at[i, 2], partner))

    copy(hall.at[at(partner)], hall.at[at(partner)], sa, ra, partner).wait_recv()
    for i, origin_chip, parts in ((0, left_chip, (lo, hi)), (1, right_chip, (hi, lo))):
        other = origin_chip * 2 + (1 - core)
        for j in range(2):
            slot = hall.at[at(other), parts[j]]
            copy(slot, slot, sd.at[i, j], rd.at[i, j], partner).wait_recv()
        slot = hall.at[at(far_chip * 2 + (1 - core)), parts[0]]
        copy(slot, slot, sd.at[i, 2], rd.at[i, 2], partner).wait_recv()
    for c in sends:
        c.wait_send()
    for c in metas:
        c.wait_send()
    for c in ahead:
        c.wait()


def dispatch(x, ids, g, wr, br, w, n, local_exp, blk, npre):
    tok, d_model = x.shape
    tokens = n * tok
    vm = pl.BlockSpec(memory_space=pltpu.VMEM)
    hbm = pl.BlockSpec(memory_space=pltpu.HBM)
    dma = pltpu.SemaphoreType.DMA
    hall, pos, post, p, pre = pl.pallas_call(
        functools.partial(dispatch_kernel, n, local_exp),
        out_shape=(vmem_out((n, tok, d_model), BF16), vmem_out((tokens, 8), F32), vmem_out((8, tokens), F32),
                   vmem_out((tokens, local_exp), F32), vmem_out((npre, d_model, blk), BF16)),
        in_specs=[hbm] * 6,
        out_specs=(vm,) * 5,
        scratch_shapes=[pltpu.VMEM(x.shape, x.dtype), pltpu.VMEM(ids.shape, ids.dtype), pltpu.VMEM(g.shape, g.dtype),
                        pltpu.VMEM(wr.shape, wr.dtype), pltpu.VMEM(br.shape, br.dtype), dma((5,)),
                        pltpu.VMEM((n, 2, tok, wr.shape[0]), F32), dma((npre,)),
                        dma, dma, dma((2, 2)), dma((2, 2)), dma((2,)), dma((2,)), dma((2, 3)), dma((2, 3)),
                        dma((n - 1,)), dma((n - 1,))],
        compiler_params=pltpu.CompilerParams(collective_id=0, has_side_effects=True, vmem_limit_bytes=DISPATCH_VMEM),
        name='dispatch',
    )(in_hbm(x), in_hbm(ids), in_hbm(g), in_hbm(wr), in_hbm(br), w)
    return hall, pos, post, p, pre


def gate_up_kernel(m_blk, slots, hall, post_ref, pos_ref, p_ref, pre, b_ref, bd_ref, w_hbm, wd_hbm, z_ref, part_ref,
                   wbuf, xg, ubuf, ybuf, perm, bias_ref, biasd_ref, sems):
    local_exp, d_model, width = w_hbm.shape
    npre, _, blk = pre.shape
    full, rest = width // blk, width % blk
    per_exp = full + 2
    total = local_exp * per_exp
    tokens = hall.shape[0] * hall.shape[1]
    max_rows = z_ref.shape[1]
    dcol = part_ref.shape[3]

    def block_copy(e, j):
        slot = (e * per_exp + j) % slots
        if isinstance(j, int) and j == full + 1:
            return pltpu.make_async_copy(wd_hbm.at[e, :, pl.ds(0, dcol)], wbuf.at[slot, :, pl.ds(0, dcol)], sems.at[slot])
        if isinstance(j, int) and j == full:
            return pltpu.make_async_copy(w_hbm.at[e, :, pl.ds(full * blk, rest)],
                                         wbuf.at[slot, :, pl.ds(0, rest)], sems.at[slot])
        return pltpu.make_async_copy(w_hbm.at[e, :, pl.ds(pl.multiple_of(j * blk, 128), blk)], wbuf.at[slot], sems.at[slot])

    def start(q):
        e, j = q // per_exp, q % per_exp

        @pl.when(j < full)
        def _():
            block_copy(e, j).start()

        for last in (full, full + 1):
            @pl.when(j == last)
            def _(last=last):
                block_copy(e, last).start()

    for q in range(npre, npre + slots):
        start(q)

    bias_ref[...] = b_ref[...].astype(F32)
    biasd_ref[...] = bd_ref[:, :dcol].astype(F32)
    src = lax.broadcasted_iota(jnp.int32, (256, 256), 0)
    dst = lax.broadcasted_iota(jnp.int32, (256, 256), 1)
    want = jnp.where(dst < 128, 2 * dst, 2 * (dst - 128) + 1)
    perm[...] = jnp.where(src == want, 1.0, 0.0).astype(BF16)

    def gather(e):
        where_row = post_ref[pl.ds(e, 1), :]
        count = jnp.sum(jnp.where(where_row >= 0.0, 1.0, 0.0)).astype(jnp.int32)
        chunks = (count + (m_blk - 1)) // m_blk

        def body(m, c):
            at = lax.broadcasted_iota(jnp.int32, (m_blk, tokens), 0) + m * m_blk
            onehot = jnp.where(at.astype(F32) == where_row, 1.0, 0.0).astype(BF16)
            xg[pl.ds(pl.multiple_of(m * m_blk, m_blk), m_blk), :] = dot32(onehot, hall[...].reshape(tokens, d_model)).astype(BF16)
            return c

        lax.fori_loop(0, chunks, body, 0)
        return chunks

    def glu(e, j, m, cols):
        at = pl.ds(pl.multiple_of(m * m_blk, m_blk), m_blk)
        for t in range(0, cols, 256):
            wide = min(256, cols - t)
            if wide == 256:
                pm = perm[...]
            else:
                pm = jnp.concatenate([perm[:128, :64], perm[:128, 128:192]], axis=1)
            al = dot32(ubuf[m, :, t:t + wide], pm)
            gate = jnp.minimum(al[:, :wide // 2], LIMIT)
            linear = jnp.clip(al[:, wide // 2:], -LIMIT, LIMIT)
            z = gate * jax.nn.sigmoid(ALPHA * gate) * (linear + 1.0)
            zoff = pl.multiple_of(j * (blk // 2), 128) + t // 2
            z_ref[e, at, pl.ds(zoff, wide // 2)] = z.astype(BF16)

    def compute(e, j, cols, chunks, weights):
        off = pl.multiple_of(j * blk, 128)
        bias = bias_ref[pl.ds(e, 1), pl.ds(off, cols)]
        before = j - 1 if isinstance(j, int) else jnp.maximum(j - 1, 0)

        def rows(m, c):
            at = pl.ds(pl.multiple_of(m * m_blk, m_blk), m_blk)
            glu(e, before, m, blk)
            ubuf[m, :, :cols] = (dot32(xg[at, :], weights()) + bias).astype(BF16)
            return c

        lax.fori_loop(0, chunks, rows, 0)

    def refill(q):
        @pl.when(q + slots < total)
        def _():
            start(q + slots)

    def streamed(e, j, cols, chunks):
        q = e * per_exp + j
        slot = q % slots
        block_copy(e, j).wait()
        compute(e, j, cols, chunks, lambda: wbuf[slot, :, :cols])
        refill(q)

    def down_start(e, chunks, first):
        q = e * per_exp + full + 1
        slot = q % slots
        where = pos_ref[:, e:e + 1] if first else jnp.sum(
            jnp.where(lax.broadcasted_iota(jnp.int32, pos_ref.shape, 1) == e, pos_ref[...], 0.0), axis=1, keepdims=True)
        gate = p_ref[:, e:e + 1] if first else jnp.sum(
            jnp.where(lax.broadcasted_iota(jnp.int32, p_ref.shape, 1) == e, p_ref[...], 0.0), axis=1, keepdims=True)
        count = jnp.max(where) + 1.0
        ybuf[...] = jnp.zeros_like(ybuf)
        block_copy(e, full + 1).wait()

        def rows(m, c):
            at = pl.ds(pl.multiple_of(m * m_blk, m_blk), m_blk)
            y = dot32(z_ref[e, at, :], wbuf[slot, :, :dcol]) + biasd_ref[pl.ds(e, 1), :]
            row_ids = (lax.broadcasted_iota(jnp.int32, (m_blk, 1), 0) + m * m_blk).astype(F32)
            ybuf[at, :] = jnp.where(row_ids < count, y, 0.0).astype(BF16)
            return c

        lax.fori_loop(0, chunks, rows, 0)
        refill(q)
        slot_ids = lax.broadcasted_iota(jnp.int32, (tokens, max_rows), 1).astype(F32)
        scat = jnp.where(where == slot_ids, 1.0, 0.0).astype(BF16)
        add = (gate * dot32(scat, ybuf[...])).reshape(part_ref.shape)
        if first:
            part_ref[...] = add
        else:
            part_ref[...] += add

    def expert(e, first):
        chunks = gather(e)

        def from_pre(j, c):
            compute(e, j, blk, chunks, lambda: pre[j])
            return c

        def body(j, c):
            streamed(e, j, blk, chunks)
            return c

        if first:
            lax.fori_loop(0, npre, from_pre, 0)
        lax.fori_loop(npre if first else 0, full, body, 0)
        streamed(e, full, rest, chunks)

        def end(m, c):
            glu(e, full, m, rest)
            return c

        lax.fori_loop(0, chunks, end, 0)
        down_start(e, chunks, first)

    expert(0, True)

    def others(e, c):
        expert(e, False)
        return c

    lax.fori_loop(1, local_exp, others, 0)


def gate_up(hall, post, pos, p, pre, w, b, wd, bd, n, max_rows, m_blk, slots, dcol):
    local_exp, d_model, width = w.shape
    blk = pre.shape[2]
    tok = hall.shape[1]
    vm = pl.BlockSpec(memory_space=pltpu.VMEM)
    hbm = pl.BlockSpec(memory_space=pl.ANY)
    return pl.pallas_call(
        functools.partial(gate_up_kernel, m_blk, slots),
        out_shape=(vmem_out((local_exp, max_rows, width // 2), BF16), vmem_out((2, n // 2, tok, dcol), F32)),
        in_specs=[vm] * 7 + [hbm] * 2,
        out_specs=(vm, vm),
        scratch_shapes=[pltpu.VMEM((slots, d_model, blk), BF16), pltpu.VMEM((max_rows, d_model), BF16),
                        pltpu.VMEM((max_rows // m_blk, m_blk, blk), BF16), pltpu.VMEM((max_rows, dcol), BF16),
                        pltpu.VMEM((256, 256), BF16), pltpu.VMEM((local_exp, width), F32), pltpu.VMEM((local_exp, dcol), F32),
                        pltpu.SemaphoreType.DMA((slots,))],
        compiler_params=pltpu.CompilerParams(vmem_limit_bytes=GATE_UP_VMEM),
        name='gate_up',
    )(in_vmem(hall), in_vmem(post), in_vmem(pos), in_vmem(p), in_vmem(pre), b, bd, w, wd)


def down_kernel(n, chunks, slots, z_ref, pos_ref, p_ref, part_in, x_ref, b_ref, w_hbm, out_ref,
                wbuf, wrest, scat, part, part_r, near, near_r, ring, ring_r,
                wsem, rsem, ns, nr, fs, fr, hs, hr):
    local_exp, d_ff, width = w_hbm.shape
    tokens = pos_ref.shape[0]
    max_rows = z_ref.shape[1]
    tok = tokens // n
    half = tok // 2
    nchip = n // 2
    blk = chunks[0][1]
    total = len(chunks) * local_exp
    depth = slots - 1
    me = lax.axis_index('ep')
    chip, core = me // 2, me % 2
    partner = chip * 2 + (1 - core)
    right_chip, left_chip, far_chip = (chip + 1) % nchip, (chip + nchip - 1) % nchip, (chip + 2) % nchip
    right, left = right_chip * 2 + core, left_chip * 2 + core
    sides = ((right, right_chip, 0), (left, left_chip, 1))

    barrier = pltpu.get_barrier_semaphore()
    for dev in (partner, right, left):
        pl.semaphore_signal(barrier, inc=1, device_id={'ep': dev}, device_id_type=pl.DeviceIdType.MESH)

    def block_copy(q):
        off, cols = chunks[q // local_exp]
        src = w_hbm.at[q % local_exp, :, pl.ds(off, cols)]
        if cols == blk:
            return pltpu.make_async_copy(src, wbuf.at[q % slots], wsem.at[q % slots])
        return pltpu.make_async_copy(src, wrest.at[q % slots], rsem.at[q % slots])

    def weights(q, cols):
        return wbuf[q % slots] if cols == blk else wrest[q % slots]

    for q in range(local_exp, local_exp + depth):
        block_copy(q).start()

    def copy(src, dst, ssem, rsem_, dev):
        return pltpu.make_async_remote_copy(src_ref=src, dst_ref=dst, send_sem=ssem, recv_sem=rsem_,
                                            device_id={'ep': dev}, device_id_type=pl.DeviceIdType.MESH)

    def bufs(c):
        if chunks[c][1] == blk:
            return part.at[c], near.at[c], ring.at[c]
        return part_r, near_r, ring_r

    def near_copy(c):
        pb, nb, _ = bufs(c)
        pb = part_in if c == 0 else pb
        return copy(pb.at[1 - core], nb, ns.at[c], nr.at[c], partner)

    def far_copy(c, side):
        dev, _, i = side
        pb, _, rb = bufs(c)
        rows = pl.ds(i * half, half)
        return copy(pb.at[core, far_chip, rows], rb.at[i, 0], fs.at[c, i, 0], fr.at[c, i, 0], dev)

    def early_copy(c, side):
        dev, dchip, i = side
        pb, _, rb = bufs(c)
        rows = pl.ds((1 - i) * half, half)
        return copy(pb.at[core, dchip, rows], rb.at[i, 1], fs.at[c, i, 1], fr.at[c, i, 1], dev)

    def late_copy(c, side):
        dev, dchip, i = side
        pb, _, rb = bufs(c)
        rows = pl.ds(i * half, half)
        return copy(pb.at[core, dchip, rows], rb.at[i, 2], hs.at[c, i], hr.at[c, i], dev)

    def stage_near(c):
        near_copy(c).start()

    def stage_far(c):
        near_copy(c).wait()
        pb, nb, _ = bufs(c)
        pb[core] = (part_in if c == 0 else pb)[core] + nb[...]
        for side in sides:
            far_copy(c, side).start()
            early_copy(c, side).start()

    def stage_late(c):
        pb, _, rb = bufs(c)
        for side in sides:
            _, dchip, i = side
            far_copy(c, side).wait_recv()
            pb[core, dchip, i * half:(i + 1) * half] += rb[i, 0]
            late_copy(c, side).start()

    def stage_out(c):
        off, cols = chunks[c]
        pb, _, rb = bufs(c)
        for side in sides:
            early_copy(c, side).wait_recv()
            late_copy(c, side).wait_recv()
        for r in range(2):
            rows = slice(r * half, (r + 1) * half)
            total_ = pb[core, chip, rows] + rb[0, 2 if r == 0 else 1] + rb[1, 1 if r == 0 else 2]
            out_ref[rows, off:off + cols] = (x_ref[rows, off:off + cols].astype(F32) + total_).astype(BF16)

    pl.semaphore_wait(barrier, 3)
    stage_near(0)
    slot_ids = lax.broadcasted_iota(jnp.int32, (tokens, max_rows), 1).astype(F32)
    for e in range(local_exp):
        scat[e] = jnp.where(pos_ref[:, e:e + 1] == slot_ids, 1.0, 0.0).astype(BF16)
    row_ids = lax.broadcasted_iota(jnp.int32, (max_rows, 1), 0).astype(F32)
    counts = [jnp.max(pos_ref[:, e:e + 1]) + 1.0 for e in range(local_exp)]
    bias = b_ref[...].astype(F32)

    last = len(chunks)
    for c, (off, cols) in enumerate(chunks):
        if c == 0:
            continue
        pb = bufs(c)[0]
        for e in range(local_exp):
            q = c * local_exp + e
            if q + depth < total:
                block_copy(q + depth).start()
            block_copy(q).wait()
            y = dot32(z_ref[e], weights(q, cols)) + bias[e:e + 1, off:off + cols]
            y = jnp.where(row_ids < counts[e], y, 0.0).astype(BF16)
            add = (p_ref[:, e:e + 1] * dot32(scat[e], y)).reshape(2, nchip, tok, cols)
            if e == 0:
                pb[...] = add
            else:
                pb[...] += add
            if e == 1:
                if c >= 1:
                    stage_far(c - 1)
            if e == 2:
                if c >= 2:
                    stage_late(c - 2)
                if c >= 3:
                    stage_out(c - 3)
        stage_near(c)
    stage_late(last - 2)
    stage_far(last - 1)
    stage_out(last - 3)
    stage_out(last - 2)
    stage_late(last - 1)
    stage_out(last - 1)
    for c in range(last):
        for side in sides:
            far_copy(c, side).wait_send()
            early_copy(c, side).wait_send()
            late_copy(c, side).wait_send()


def down(z, pos, p, part, x, w, b, n, blk, slots):
    local_exp, d_ff, width = w.shape
    tokens = pos.shape[0]
    tok = tokens // n
    chunks = [(c, min(blk, width - c)) for c in range(0, width, blk)]
    full, rest, last = width // blk, width % blk, len(chunks)
    vm = pl.BlockSpec(memory_space=pltpu.VMEM)
    dma = pltpu.SemaphoreType.DMA
    return pl.pallas_call(
        functools.partial(down_kernel, n, chunks, slots),
        out_shape=vmem_out((tok, width), BF16),
        in_specs=[vm, vm, vm, vm, vm, vm, pl.BlockSpec(memory_space=pl.ANY)],
        out_specs=vm,
        scratch_shapes=[pltpu.VMEM((slots, d_ff, blk), BF16), pltpu.VMEM((slots, d_ff, rest), BF16),
                        pltpu.VMEM((local_exp, tokens, z.shape[1]), BF16),
                        pltpu.VMEM((full, 2, n // 2, tok, blk), F32), pltpu.VMEM((2, n // 2, tok, rest), F32),
                        pltpu.VMEM((full, n // 2, tok, blk), F32), pltpu.VMEM((n // 2, tok, rest), F32),
                        pltpu.VMEM((full, 2, 3, tok // 2, blk), F32), pltpu.VMEM((2, 3, tok // 2, rest), F32),
                        dma((slots,)), dma((slots,)),
                        dma((last,)), dma((last,)), dma((last, 2, 2)), dma((last, 2, 2)), dma((last, 2)), dma((last, 2))],
        compiler_params=pltpu.CompilerParams(collective_id=1, has_side_effects=True, vmem_limit_bytes=DOWN_VMEM),
        name='down',
    )(in_vmem(z), in_vmem(pos), in_vmem(p), in_vmem(part), x, b, w)


def solution(mesh):
    n = mesh.shape['ep']
    rows_spec = P(('dp', 'ep'), None)

    def local_block(x_in, expert_ids, norm_weight, router_w, router_b, w_gate_up, b_gate_up, w_down, b_down):
        tok, d_model = x_in.shape
        top_k = expert_ids.shape[1]
        local_exp = w_gate_up.shape[0]
        experts = local_exp * n
        max_rows = n * (4 * top_k * tok // experts)
        wide = w_gate_up.shape[2] >= 2048
        blk, dcol = (1024, 512) if wide else (256, 128)
        npre = w_gate_up.shape[2] // blk
        hall, pos, post, p, pre = dispatch(x_in, expert_ids.T, norm_weight, router_w.T, router_b, w_gate_up, n, local_exp, blk, npre)
        z, part = gate_up(hall, post, pos, p, pre, w_gate_up, b_gate_up, w_down, b_down, n, max_rows, min(128, max_rows), 3, dcol)
        return down(z, pos, p, part, x_in, w_down, b_down, n, dcol, 3)

    return jax.shard_map(local_block, mesh=mesh, in_specs=(rows_spec, rows_spec, P(), P(), P(), P('ep', None, None), P('ep', None), P('ep', None, None), P('ep', None)), out_specs=rows_spec, check_vma=False)
```

```python
import functools

import jax
import jax.numpy as jnp
from jax import lax
from jax.experimental import pallas as pl
from jax.experimental.pallas import tpu as pltpu
from jax.sharding import PartitionSpec as P

EPSILON = 1e-5
LIMIT = 7.0
ALPHA = 1.702
F32 = jnp.float32
BF16 = jnp.bfloat16
DISPATCH_VMEM = 10 * 1024 * 1024
GATE_UP_VMEM = 10 * 1024 * 1024
DOWN_VMEM = 30 * 1024 * 1024


def dot32(a, b):
    return jnp.dot(a, b, preferred_element_type=F32)


def in_vmem(a):
    return pltpu.with_memory_space_constraint(a, pltpu.VMEM)


def vmem_out(shape, dtype):
    return pltpu.VMEM(shape, dtype)


def in_hbm(a):
    return pltpu.with_memory_space_constraint(a, pltpu.HBM)


def dot_t(a, b):
    return lax.dot_general(a, b, (((0,), (0,)), ((), ())), preferred_element_type=F32)


def blocks_per_expert(w_hbm, ring):
    return w_hbm.shape[2] // ring.shape[2] + 2


def weight_block(w_hbm, wd_hbm, ring, sems, dcol, e, j):
    slots, _, blk = ring.shape
    full, rest = w_hbm.shape[2] // blk, w_hbm.shape[2] % blk
    slot = (e * (full + 2) + j) % slots
    if isinstance(j, int) and j == full + 1:
        return pltpu.make_async_copy(wd_hbm.at[e, :, pl.ds(0, dcol)], ring.at[slot, :, pl.ds(0, dcol)], sems.at[slot])
    if isinstance(j, int) and j == full:
        return pltpu.make_async_copy(w_hbm.at[e, :, pl.ds(full * blk, rest)], ring.at[slot, :, pl.ds(0, rest)], sems.at[slot])
    off = j * blk if isinstance(j, int) else pl.multiple_of(j * blk, 128)
    return pltpu.make_async_copy(w_hbm.at[e, :, pl.ds(off, blk)], ring.at[slot], sems.at[slot])


def dispatch_kernel(n, local_exp, dcol, x_hbm, ids_hbm, g_hbm, wr_hbm, br_hbm, w_hbm, wd_hbm, hall, pos_ref, post_ref, p_ref, pre,
                    x_ref, ids_ref, g_ref, wr_ref, br_ref, isem, mall, psem, sa, ra, sb, rb, sc, rc, sd, rd, sm, rm):
    me = lax.axis_index('ep')
    chips = n // 2
    chip, core = me // 2, me % 2
    partner = chip * 2 + (1 - core)
    right_chip, left_chip = (chip + 1) % chips, (chip + chips - 1) % chips
    far_chip = (chip + 2) % chips
    right, left = right_chip * 2 + core, left_chip * 2 + core
    far = far_chip * 2 + core
    tok, _ = x_ref.shape
    top_k = ids_ref.shape[0]
    experts = wr_ref.shape[0]

    def at(dev):
        return (dev % 2) * chips + dev // 2

    half = tok // 2

    loads = [pltpu.make_async_copy(src, dst, isem.at[i]) for i, (src, dst) in enumerate(
        ((x_hbm, x_ref), (g_hbm, g_ref), (wr_hbm, wr_ref), (br_hbm, br_ref), (ids_hbm, ids_ref)))]
    for c in loads:
        c.start()
    barrier = pltpu.get_barrier_semaphore()
    for k in range(1, n):
        pl.semaphore_signal(barrier, inc=1, device_id={'ep': (me + k) % n}, device_id_type=pl.DeviceIdType.MESH)
    per_exp = blocks_per_expert(w_hbm, pre)
    ahead = [weight_block(w_hbm, wd_hbm, pre, psem, dcol, q // per_exp, q % per_exp) for q in range(pre.shape[0])]
    for c in loads:
        c.wait()
    for c in ahead:
        c.start()

    x = x_ref[...].astype(F32)
    inv = lax.rsqrt(jnp.mean(x * x, axis=-1, keepdims=True) + EPSILON)
    h = (x * inv * g_ref[...].astype(F32)[None, :]).astype(BF16)
    hall[at(me)] = h

    pl.semaphore_wait(barrier, n - 1)

    def copy(src, dst, ssem, rsem, dev):
        return pltpu.make_async_remote_copy(src_ref=src, dst_ref=dst, send_sem=ssem, recv_sem=rsem,
                                            device_id={'ep': dev}, device_id_type=pl.DeviceIdType.MESH)

    lo, hi = pl.ds(0, half), pl.ds(half, half)
    sends = []

    def start(c):
        c.start()
        sends.append(c)

    for i, (dev, parts) in enumerate(((right, (lo, hi)), (left, (hi, lo)))):
        for j, rows in enumerate(parts):
            start(copy(hall.at[at(me), rows], hall.at[at(me), rows], sb.at[i, j], rb.at[i, j], dev))
    start(copy(hall.at[at(me)], hall.at[at(me)], sa, ra, partner))
    logits = lax.dot_general(h, wr_ref[...], (((1,), (1,)), ((), ())), preferred_element_type=F32) + br_ref[...].astype(F32)[None, :]
    ids = ids_ref[...]
    expert = lax.broadcasted_iota(jnp.int32, (experts, tok), 0)
    turn = jnp.where(lax.broadcasted_iota(jnp.int32, (experts, experts), 0)
                     == lax.broadcasted_iota(jnp.int32, (experts, experts), 1), 1.0, 0.0).astype(BF16)
    hot = [dot_t(jnp.where(ids[k:k + 1, :] == expert, 1.0, 0.0).astype(BF16), turn) > 0.5 for k in range(top_k)]
    picked = [jnp.sum(jnp.where(hk, logits, 0.0), axis=1, keepdims=True) for hk in hot]
    top = functools.reduce(jnp.maximum, picked)
    ex = [jnp.exp(v - top) for v in picked]
    total = functools.reduce(jnp.add, ex)
    gates = jnp.zeros((tok, experts), F32)
    chosen = jnp.zeros((tok, experts), F32)
    for k in range(top_k):
        gates = gates + jnp.where(hot[k], ex[k] / total, 0.0)
        chosen = chosen + jnp.where(hot[k], 1.0, 0.0)
    mall[at(me), 0] = gates
    mall[at(me), 1] = chosen
    metas = []
    for k in range(1, n):
        c = copy(mall.at[at(me)], mall.at[at(me)], sm.at[k - 1], rm.at[k - 1], (me + k) % n)
        c.start()
        metas.append(c)
    order = ((0, left, right, (lo, hi)), (1, right, left, (hi, lo)))
    for i, origin, onward, parts in order:
        slot = hall.at[at(origin), parts[0]]
        copy(slot, slot, sb.at[i, 0], rb.at[i, 0], origin).wait_recv()
        start(copy(slot, slot, sc.at[i], rc.at[i], onward))
        start(copy(slot, slot, sd.at[i, 0], rd.at[i, 0], partner))
    for k in range(1, n):
        src = (me + n - k) % n
        copy(mall.at[at(src)], mall.at[at(src)], sm.at[k - 1], rm.at[k - 1], src).wait_recv()
    tokens = n * tok
    e0 = me * local_exp
    gates_all = mall[:, 0].reshape(tokens, experts)
    chosen_all = mall[:, 1].reshape(tokens, experts)
    lane_all = lax.broadcasted_iota(jnp.int32, (tokens, experts), 1)
    pick = (lax.broadcasted_iota(jnp.int32, (experts, 8), 0)
            == lax.broadcasted_iota(jnp.int32, (experts, 8), 1) + e0)
    pick = jnp.where(pick & (lax.broadcasted_iota(jnp.int32, (experts, 8), 1) < local_exp), 1.0, 0.0).astype(BF16)
    mine = dot32(chosen_all.astype(BF16), pick).astype(BF16)
    row = lax.broadcasted_iota(jnp.int32, (tokens, tokens), 0)
    col = lax.broadcasted_iota(jnp.int32, (tokens, tokens), 1)
    lower = jnp.where(col < row, 1.0, 0.0).astype(BF16)
    upper = jnp.where(row < col, 1.0, 0.0).astype(BF16)
    eye = jnp.where(row == col, 1.0, 0.0).astype(BF16)
    pos_ref[...] = jnp.where(mine.astype(F32) > 0.5, dot32(lower, mine), -1.0)
    post_ref[...] = jnp.where(dot_t(mine, eye) > 0.5, dot_t(mine, upper), -1.0)
    for e in range(local_exp):
        p_ref[:, e:e + 1] = jnp.sum(jnp.where(lane_all == e0 + e, gates_all, 0.0), axis=1, keepdims=True)
    for i, origin, onward, parts in order:
        slot = hall.at[at(origin), parts[1]]
        copy(slot, slot, sb.at[i, 1], rb.at[i, 1], origin).wait_recv()
        start(copy(slot, slot, sd.at[i, 1], rd.at[i, 1], partner))
    for i, origin, onward, parts in order:
        slot = hall.at[at(far), parts[0]]
        copy(slot, slot, sc.at[i], rc.at[i], origin).wait_recv()
        start(copy(slot, slot, sd.at[i, 2], rd.at[i, 2], partner))

    copy(hall.at[at(partner)], hall.at[at(partner)], sa, ra, partner).wait_recv()
    for i, origin_chip, parts in ((0, left_chip, (lo, hi)), (1, right_chip, (hi, lo))):
        other = origin_chip * 2 + (1 - core)
        for j in range(2):
            slot = hall.at[at(other), parts[j]]
            copy(slot, slot, sd.at[i, j], rd.at[i, j], partner).wait_recv()
        slot = hall.at[at(far_chip * 2 + (1 - core)), parts[0]]
        copy(slot, slot, sd.at[i, 2], rd.at[i, 2], partner).wait_recv()
    for c in sends:
        c.wait_send()
    for c in metas:
        c.wait_send()
    for c in ahead:
        c.wait()


def dispatch(x, ids, g, wr, br, w, wd, n, local_exp, blk, npre, dcol):
    tok, d_model = x.shape
    tokens = n * tok
    vm = pl.BlockSpec(memory_space=pltpu.VMEM)
    hbm = pl.BlockSpec(memory_space=pltpu.HBM)
    dma = pltpu.SemaphoreType.DMA
    hall, pos, post, p, pre = pl.pallas_call(
        functools.partial(dispatch_kernel, n, local_exp, dcol),
        out_shape=(vmem_out((n, tok, d_model), BF16), vmem_out((tokens, 8), F32), vmem_out((8, tokens), F32),
                   vmem_out((tokens, local_exp), F32), vmem_out((npre, d_model, blk), BF16)),
        in_specs=[hbm] * 7,
        out_specs=(vm,) * 5,
        scratch_shapes=[pltpu.VMEM(x.shape, x.dtype), pltpu.VMEM(ids.shape, ids.dtype), pltpu.VMEM(g.shape, g.dtype),
                        pltpu.VMEM(wr.shape, wr.dtype), pltpu.VMEM(br.shape, br.dtype), dma((5,)),
                        pltpu.VMEM((n, 2, tok, wr.shape[0]), F32), dma((npre,)),
                        dma, dma, dma((2, 2)), dma((2, 2)), dma((2,)), dma((2,)), dma((2, 3)), dma((2, 3)),
                        dma((n - 1,)), dma((n - 1,))],
        compiler_params=pltpu.CompilerParams(collective_id=0, has_side_effects=True, vmem_limit_bytes=DISPATCH_VMEM),
        name='dispatch',
    )(in_hbm(x), in_hbm(ids), in_hbm(g), in_hbm(wr), in_hbm(br), w, wd)
    return hall, pos, post, p, pre


def gate_up_kernel(m_blk, hall, post_ref, pos_ref, p_ref, pre, b_ref, bd_ref, w_hbm, wd_hbm, z_ref, part_ref, ring,
                   xg, ubuf, ybuf, perm, bias_ref, biasd_ref, sems):
    local_exp, d_model, width = w_hbm.shape
    slots, _, blk = ring.shape
    full, rest = width // blk, width % blk
    per_exp = full + 2
    total = local_exp * per_exp
    tokens = hall.shape[0] * hall.shape[1]
    max_rows = z_ref.shape[1]
    dcol = part_ref.shape[3]

    def block_copy(e, j):
        return weight_block(w_hbm, wd_hbm, ring, sems, dcol, e, j)

    def block_wait(e, j):
        @pl.when(e * per_exp + j >= slots)
        def _():
            block_copy(e, j).wait()

    def start(q):
        e, j = q // per_exp, q % per_exp

        @pl.when(j < full)
        def _():
            block_copy(e, j).start()

        for last in (full, full + 1):
            @pl.when(j == last)
            def _(last=last):
                block_copy(e, last).start()

    bias_ref[...] = b_ref[...].astype(F32)
    biasd_ref[...] = bd_ref[:, :dcol].astype(F32)
    src = lax.broadcasted_iota(jnp.int32, (256, 256), 0)
    dst = lax.broadcasted_iota(jnp.int32, (256, 256), 1)
    want = jnp.where(dst < 128, 2 * dst, 2 * (dst - 128) + 1)
    perm[...] = jnp.where(src == want, 1.0, 0.0).astype(BF16)

    def gather(e):
        where_row = post_ref[pl.ds(e, 1), :]
        count = jnp.sum(jnp.where(where_row >= 0.0, 1.0, 0.0)).astype(jnp.int32)
        chunks = (count + (m_blk - 1)) // m_blk

        def body(m, c):
            at = lax.broadcasted_iota(jnp.int32, (m_blk, tokens), 0) + m * m_blk
            onehot = jnp.where(at.astype(F32) == where_row, 1.0, 0.0).astype(BF16)
            xg[pl.ds(pl.multiple_of(m * m_blk, m_blk), m_blk), :] = dot32(onehot, hall[...].reshape(tokens, d_model)).astype(BF16)
            return c

        lax.fori_loop(0, chunks, body, 0)
        return chunks

    def glu(e, j, m, cols):
        at = pl.ds(pl.multiple_of(m * m_blk, m_blk), m_blk)
        for t in range(0, cols, 256):
            wide = min(256, cols - t)
            if wide == 256:
                pm = perm[...]
            else:
                pm = jnp.concatenate([perm[:128, :64], perm[:128, 128:192]], axis=1)
            al = dot32(ubuf[m, :, t:t + wide], pm)
            gate = jnp.minimum(al[:, :wide // 2], LIMIT)
            linear = jnp.clip(al[:, wide // 2:], -LIMIT, LIMIT)
            z = gate * jax.nn.sigmoid(ALPHA * gate) * (linear + 1.0)
            zoff = pl.multiple_of(j * (blk // 2), 128) + t // 2
            z_ref[e, at, pl.ds(zoff, wide // 2)] = z.astype(BF16)

    def compute(e, j, cols, chunks, weights):
        off = pl.multiple_of(j * blk, 128)
        bias = bias_ref[pl.ds(e, 1), pl.ds(off, cols)]
        before = j - 1 if isinstance(j, int) else jnp.maximum(j - 1, 0)

        def rows(m, c):
            at = pl.ds(pl.multiple_of(m * m_blk, m_blk), m_blk)
            glu(e, before, m, blk)
            ubuf[m, :, :cols] = (dot32(xg[at, :], weights()) + bias).astype(BF16)
            return c

        lax.fori_loop(0, chunks, rows, 0)

    def refill(q):
        @pl.when(q + slots < total)
        def _():
            start(q + slots)

    def streamed(e, j, cols, chunks):
        q = e * per_exp + j
        slot = q % slots
        block_wait(e, j)
        compute(e, j, cols, chunks, lambda: ring[slot, :, :cols])
        refill(q)

    def down_start(e, chunks, first):
        q = e * per_exp + full + 1
        slot = q % slots
        where = pos_ref[:, e:e + 1] if first else jnp.sum(
            jnp.where(lax.broadcasted_iota(jnp.int32, pos_ref.shape, 1) == e, pos_ref[...], 0.0), axis=1, keepdims=True)
        gate = p_ref[:, e:e + 1] if first else jnp.sum(
            jnp.where(lax.broadcasted_iota(jnp.int32, p_ref.shape, 1) == e, p_ref[...], 0.0), axis=1, keepdims=True)
        count = jnp.max(where) + 1.0
        ybuf[...] = jnp.zeros_like(ybuf)
        block_wait(e, full + 1)

        def rows(m, c):
            at = pl.ds(pl.multiple_of(m * m_blk, m_blk), m_blk)
            y = dot32(z_ref[e, at, :], ring[slot, :, :dcol]) + biasd_ref[pl.ds(e, 1), :]
            row_ids = (lax.broadcasted_iota(jnp.int32, (m_blk, 1), 0) + m * m_blk).astype(F32)
            ybuf[at, :] = jnp.where(row_ids < count, y, 0.0).astype(BF16)
            return c

        lax.fori_loop(0, chunks, rows, 0)
        refill(q)
        slot_ids = lax.broadcasted_iota(jnp.int32, (tokens, max_rows), 1).astype(F32)
        scat = jnp.where(where == slot_ids, 1.0, 0.0).astype(BF16)
        add = (gate * dot32(scat, ybuf[...])).reshape(part_ref.shape)
        if first:
            part_ref[...] = add
        else:
            part_ref[...] += add

    def expert(e, first):
        chunks = gather(e)

        def body(j, c):
            streamed(e, j, blk, chunks)
            return c

        lax.fori_loop(0, full, body, 0)
        streamed(e, full, rest, chunks)

        def end(m, c):
            glu(e, full, m, rest)
            return c

        lax.fori_loop(0, chunks, end, 0)
        down_start(e, chunks, first)

    expert(0, True)

    def others(e, c):
        expert(e, False)
        return c

    lax.fori_loop(1, local_exp, others, 0)


def gate_up(hall, post, pos, p, pre, w, b, wd, bd, n, max_rows, m_blk, dcol):
    local_exp, d_model, width = w.shape
    blk = pre.shape[2]
    tok = hall.shape[1]
    vm = pl.BlockSpec(memory_space=pltpu.VMEM)
    hbm = pl.BlockSpec(memory_space=pl.ANY)
    return pl.pallas_call(
        functools.partial(gate_up_kernel, m_blk),
        out_shape=(vmem_out((local_exp, max_rows, width // 2), BF16), vmem_out((2, n // 2, tok, dcol), F32),
                   vmem_out(pre.shape, pre.dtype)),
        in_specs=[vm] * 7 + [hbm] * 2,
        out_specs=(vm, vm, vm),
        input_output_aliases={4: 2},
        scratch_shapes=[pltpu.VMEM((max_rows, d_model), BF16),
                        pltpu.VMEM((max_rows // m_blk, m_blk, blk), BF16), pltpu.VMEM((max_rows, dcol), BF16),
                        pltpu.VMEM((256, 256), BF16), pltpu.VMEM((local_exp, width), F32), pltpu.VMEM((local_exp, dcol), F32),
                        pltpu.SemaphoreType.DMA((pre.shape[0],))],
        compiler_params=pltpu.CompilerParams(vmem_limit_bytes=GATE_UP_VMEM),
        name='gate_up',
    )(in_vmem(hall), in_vmem(post), in_vmem(pos), in_vmem(p), in_vmem(pre), b, bd, w, wd)[:2]


def down_kernel(n, chunks, slots, z_ref, pos_ref, p_ref, part_in, x_ref, b_ref, w_hbm, out_ref,
                wbuf, wrest, scat, part, part_r, near, near_r, ring, ring_r,
                wsem, rsem, ns, nr, fs, fr, hs, hr):
    local_exp, d_ff, width = w_hbm.shape
    tokens = pos_ref.shape[0]
    max_rows = z_ref.shape[1]
    tok = tokens // n
    half = tok // 2
    nchip = n // 2
    blk = chunks[0][1]
    total = len(chunks) * local_exp
    depth = slots - 1
    me = lax.axis_index('ep')
    chip, core = me // 2, me % 2
    partner = chip * 2 + (1 - core)
    right_chip, left_chip, far_chip = (chip + 1) % nchip, (chip + nchip - 1) % nchip, (chip + 2) % nchip
    right, left = right_chip * 2 + core, left_chip * 2 + core
    sides = ((right, right_chip, 0), (left, left_chip, 1))

    barrier = pltpu.get_barrier_semaphore()
    for dev in (partner, right, left):
        pl.semaphore_signal(barrier, inc=1, device_id={'ep': dev}, device_id_type=pl.DeviceIdType.MESH)

    def block_copy(q):
        off, cols = chunks[q // local_exp]
        src = w_hbm.at[q % local_exp, :, pl.ds(off, cols)]
        if cols == blk:
            return pltpu.make_async_copy(src, wbuf.at[q % slots], wsem.at[q % slots])
        return pltpu.make_async_copy(src, wrest.at[q % slots], rsem.at[q % slots])

    def weights(q, cols):
        return wbuf[q % slots] if cols == blk else wrest[q % slots]

    for q in range(local_exp, local_exp + depth):
        block_copy(q).start()

    def copy(src, dst, ssem, rsem_, dev):
        return pltpu.make_async_remote_copy(src_ref=src, dst_ref=dst, send_sem=ssem, recv_sem=rsem_,
                                            device_id={'ep': dev}, device_id_type=pl.DeviceIdType.MESH)

    def bufs(c):
        if chunks[c][1] == blk:
            return part.at[c], near.at[c], ring.at[c]
        return part_r, near_r, ring_r

    def near_copy(c):
        pb, nb, _ = bufs(c)
        pb = part_in if c == 0 else pb
        return copy(pb.at[1 - core], nb, ns.at[c], nr.at[c], partner)

    def far_copy(c, side):
        dev, _, i = side
        pb, _, rb = bufs(c)
        rows = pl.ds(i * half, half)
        return copy(pb.at[core, far_chip, rows], rb.at[i, 0], fs.at[c, i, 0], fr.at[c, i, 0], dev)

    def early_copy(c, side):
        dev, dchip, i = side
        pb, _, rb = bufs(c)
        rows = pl.ds((1 - i) * half, half)
        return copy(pb.at[core, dchip, rows], rb.at[i, 1], fs.at[c, i, 1], fr.at[c, i, 1], dev)

    def late_copy(c, side):
        dev, dchip, i = side
        pb, _, rb = bufs(c)
        rows = pl.ds(i * half, half)
        return copy(pb.at[core, dchip, rows], rb.at[i, 2], hs.at[c, i], hr.at[c, i], dev)

    def stage_near(c):
        near_copy(c).start()

    def stage_far(c):
        near_copy(c).wait()
        pb, nb, _ = bufs(c)
        pb[core] = (part_in if c == 0 else pb)[core] + nb[...]
        for side in sides:
            far_copy(c, side).start()
            early_copy(c, side).start()

    def stage_late(c):
        pb, _, rb = bufs(c)
        for side in sides:
            _, dchip, i = side
            far_copy(c, side).wait_recv()
            pb[core, dchip, i * half:(i + 1) * half] += rb[i, 0]
            late_copy(c, side).start()

    def stage_out(c):
        off, cols = chunks[c]
        pb, _, rb = bufs(c)
        for side in sides:
            early_copy(c, side).wait_recv()
            late_copy(c, side).wait_recv()
        for r in range(2):
            rows = slice(r * half, (r + 1) * half)
            total_ = pb[core, chip, rows] + rb[0, 2 if r == 0 else 1] + rb[1, 1 if r == 0 else 2]
            out_ref[rows, off:off + cols] = (x_ref[rows, off:off + cols].astype(F32) + total_).astype(BF16)

    pl.semaphore_wait(barrier, 3)
    stage_near(0)
    slot_ids = lax.broadcasted_iota(jnp.int32, (tokens, max_rows), 1).astype(F32)
    for e in range(local_exp):
        scat[e] = jnp.where(pos_ref[:, e:e + 1] == slot_ids, 1.0, 0.0).astype(BF16)
    row_ids = lax.broadcasted_iota(jnp.int32, (max_rows, 1), 0).astype(F32)
    counts = [jnp.max(pos_ref[:, e:e + 1]) + 1.0 for e in range(local_exp)]
    bias = b_ref[...].astype(F32)

    last = len(chunks)
    for c, (off, cols) in enumerate(chunks):
        if c == 0:
            continue
        pb = bufs(c)[0]
        for e in range(local_exp):
            q = c * local_exp + e
            if q + depth < total:
                block_copy(q + depth).start()
            block_copy(q).wait()
            y = dot32(z_ref[e], weights(q, cols)) + bias[e:e + 1, off:off + cols]
            y = jnp.where(row_ids < counts[e], y, 0.0).astype(BF16)
            add = (p_ref[:, e:e + 1] * dot32(scat[e], y)).reshape(2, nchip, tok, cols)
            if e == 0:
                pb[...] = add
            else:
                pb[...] += add
            if e == 1:
                if c >= 1:
                    stage_far(c - 1)
            if e == 2:
                if c >= 2:
                    stage_late(c - 2)
                if c >= 3:
                    stage_out(c - 3)
        stage_near(c)
    stage_late(last - 2)
    stage_far(last - 1)
    stage_out(last - 3)
    stage_out(last - 2)
    stage_late(last - 1)
    stage_out(last - 1)
    for c in range(last):
        for side in sides:
            far_copy(c, side).wait_send()
            early_copy(c, side).wait_send()
            late_copy(c, side).wait_send()


def down(z, pos, p, part, x, w, b, n, blk, slots):
    local_exp, d_ff, width = w.shape
    tokens = pos.shape[0]
    tok = tokens // n
    chunks = [(c, min(blk, width - c)) for c in range(0, width, blk)]
    full, rest, last = width // blk, width % blk, len(chunks)
    vm = pl.BlockSpec(memory_space=pltpu.VMEM)
    dma = pltpu.SemaphoreType.DMA
    return pl.pallas_call(
        functools.partial(down_kernel, n, chunks, slots),
        out_shape=vmem_out((tok, width), BF16),
        in_specs=[vm, vm, vm, vm, vm, vm, pl.BlockSpec(memory_space=pl.ANY)],
        out_specs=vm,
        scratch_shapes=[pltpu.VMEM((slots, d_ff, blk), BF16), pltpu.VMEM((slots, d_ff, rest), BF16),
                        pltpu.VMEM((local_exp, tokens, z.shape[1]), BF16),
                        pltpu.VMEM((full, 2, n // 2, tok, blk), F32), pltpu.VMEM((2, n // 2, tok, rest), F32),
                        pltpu.VMEM((full, n // 2, tok, blk), F32), pltpu.VMEM((n // 2, tok, rest), F32),
                        pltpu.VMEM((full, 2, 3, tok // 2, blk), F32), pltpu.VMEM((2, 3, tok // 2, rest), F32),
                        dma((slots,)), dma((slots,)),
                        dma((last,)), dma((last,)), dma((last, 2, 2)), dma((last, 2, 2)), dma((last, 2)), dma((last, 2))],
        compiler_params=pltpu.CompilerParams(collective_id=1, has_side_effects=True, vmem_limit_bytes=DOWN_VMEM),
        name='down',
    )(in_vmem(z), in_vmem(pos), in_vmem(p), in_vmem(part), x, b, w)


def solution(mesh):
    n = mesh.shape['ep']
    rows_spec = P(('dp', 'ep'), None)

    def local_block(x_in, expert_ids, norm_weight, router_w, router_b, w_gate_up, b_gate_up, w_down, b_down):
        tok, d_model = x_in.shape
        top_k = expert_ids.shape[1]
        local_exp = w_gate_up.shape[0]
        experts = local_exp * n
        max_rows = n * (4 * top_k * tok // experts)
        wide = w_gate_up.shape[2] >= 2048
        blk, dcol = (1024, 512) if wide else (256, 128)
        npre = 7
        hall, pos, post, p, pre = dispatch(x_in, expert_ids.T, norm_weight, router_w.T, router_b, w_gate_up, w_down, n, local_exp, blk, npre, dcol)
        z, part = gate_up(hall, post, pos, p, pre, w_gate_up, b_gate_up, w_down, b_down, n, max_rows, min(128, max_rows), dcol)
        return down(z, pos, p, part, x_in, w_down, b_down, n, dcol, 3)

    return jax.shard_map(local_block, mesh=mesh, in_specs=(rows_spec, rows_spec, P(), P(), P(), P('ep', None, None), P('ep', None), P('ep', None, None), P('ep', None)), out_specs=rows_spec, check_vma=False)
```

```python
import functools

import jax
import jax.numpy as jnp
from jax import lax
from jax.experimental import pallas as pl
from jax.experimental.pallas import tpu as pltpu
from jax.sharding import PartitionSpec as P

EPSILON = 1e-5
LIMIT = 7.0
ALPHA = 1.702
F32 = jnp.float32
BF16 = jnp.bfloat16
DISPATCH_VMEM = 10 * 1024 * 1024
GATE_UP_VMEM = 10 * 1024 * 1024
DOWN_VMEM = 30 * 1024 * 1024


def dot32(a, b):
    return jnp.dot(a, b, preferred_element_type=F32)


def in_vmem(a):
    return pltpu.with_memory_space_constraint(a, pltpu.VMEM)


def vmem_out(shape, dtype):
    return pltpu.VMEM(shape, dtype)


def in_hbm(a):
    return pltpu.with_memory_space_constraint(a, pltpu.HBM)


def dot_t(a, b):
    return lax.dot_general(a, b, (((0,), (0,)), ((), ())), preferred_element_type=F32)


def blocks_per_expert(w_hbm, ring):
    return w_hbm.shape[2] // ring.shape[2] + 2


def weight_block(w_hbm, wd_hbm, ring, sems, dcol, e, j, rows=None):
    slots, depth, blk = ring.shape
    full, rest = w_hbm.shape[2] // blk, w_hbm.shape[2] % blk
    slot = (e * (full + 2) + j) % slots
    rows = pl.ds(0, depth) if rows is None else rows
    if isinstance(j, int) and j == full + 1:
        return pltpu.make_async_copy(wd_hbm.at[e, rows, pl.ds(0, dcol)], ring.at[slot, rows, pl.ds(0, dcol)], sems.at[slot])
    if isinstance(j, int) and j == full:
        return pltpu.make_async_copy(w_hbm.at[e, rows, pl.ds(full * blk, rest)], ring.at[slot, rows, pl.ds(0, rest)], sems.at[slot])
    off = j * blk if isinstance(j, int) else pl.multiple_of(j * blk, 128)
    return pltpu.make_async_copy(w_hbm.at[e, rows, pl.ds(off, blk)], ring.at[slot, rows], sems.at[slot])


def dispatch_kernel(n, local_exp, dcol, x_hbm, ids_hbm, g_hbm, wr_hbm, br_hbm, w_hbm, wd_hbm, hall, pos_ref, post_ref, p_ref, pre,
                    x_ref, ids_ref, g_ref, wr_ref, br_ref, isem, mall, psem, sa, ra, sb, rb, sc, rc, sd, rd, sm, rm):
    me = lax.axis_index('ep')
    chips = n // 2
    chip, core = me // 2, me % 2
    partner = chip * 2 + (1 - core)
    right_chip, left_chip = (chip + 1) % chips, (chip + chips - 1) % chips
    far_chip = (chip + 2) % chips
    right, left = right_chip * 2 + core, left_chip * 2 + core
    far = far_chip * 2 + core
    tok, _ = x_ref.shape
    top_k = ids_ref.shape[0]
    experts = wr_ref.shape[0]

    def at(dev):
        return (dev % 2) * chips + dev // 2

    half = tok // 2

    loads = [pltpu.make_async_copy(src, dst, isem.at[i]) for i, (src, dst) in enumerate(
        ((x_hbm, x_ref), (g_hbm, g_ref), (wr_hbm, wr_ref), (br_hbm, br_ref), (ids_hbm, ids_ref)))]
    for c in loads:
        c.start()
    barrier = pltpu.get_barrier_semaphore()
    for k in range(1, n):
        pl.semaphore_signal(barrier, inc=1, device_id={'ep': (me + k) % n}, device_id_type=pl.DeviceIdType.MESH)
    per_exp = blocks_per_expert(w_hbm, pre)
    ahead = [weight_block(w_hbm, wd_hbm, pre, psem, dcol, q // per_exp, q % per_exp) for q in range(pre.shape[0])]
    for c in loads:
        c.wait()
    for c in ahead:
        c.start()

    x = x_ref[...].astype(F32)
    inv = lax.rsqrt(jnp.mean(x * x, axis=-1, keepdims=True) + EPSILON)
    h = (x * inv * g_ref[...].astype(F32)[None, :]).astype(BF16)
    hall[at(me)] = h

    pl.semaphore_wait(barrier, n - 1)

    def copy(src, dst, ssem, rsem, dev):
        return pltpu.make_async_remote_copy(src_ref=src, dst_ref=dst, send_sem=ssem, recv_sem=rsem,
                                            device_id={'ep': dev}, device_id_type=pl.DeviceIdType.MESH)

    lo, hi = pl.ds(0, half), pl.ds(half, half)
    sends = []

    def start(c):
        c.start()
        sends.append(c)

    for i, (dev, parts) in enumerate(((right, (lo, hi)), (left, (hi, lo)))):
        for j, rows in enumerate(parts):
            start(copy(hall.at[at(me), rows], hall.at[at(me), rows], sb.at[i, j], rb.at[i, j], dev))
    start(copy(hall.at[at(me)], hall.at[at(me)], sa, ra, partner))
    logits = lax.dot_general(h, wr_ref[...], (((1,), (1,)), ((), ())), preferred_element_type=F32) + br_ref[...].astype(F32)[None, :]
    ids = ids_ref[...]
    expert = lax.broadcasted_iota(jnp.int32, (experts, tok), 0)
    turn = jnp.where(lax.broadcasted_iota(jnp.int32, (experts, experts), 0)
                     == lax.broadcasted_iota(jnp.int32, (experts, experts), 1), 1.0, 0.0).astype(BF16)
    hot = [dot_t(jnp.where(ids[k:k + 1, :] == expert, 1.0, 0.0).astype(BF16), turn) > 0.5 for k in range(top_k)]
    picked = [jnp.sum(jnp.where(hk, logits, 0.0), axis=1, keepdims=True) for hk in hot]
    top = functools.reduce(jnp.maximum, picked)
    ex = [jnp.exp(v - top) for v in picked]
    total = functools.reduce(jnp.add, ex)
    gates = jnp.zeros((tok, experts), F32)
    chosen = jnp.zeros((tok, experts), F32)
    for k in range(top_k):
        gates = gates + jnp.where(hot[k], ex[k] / total, 0.0)
        chosen = chosen + jnp.where(hot[k], 1.0, 0.0)
    mall[at(me), 0] = gates
    mall[at(me), 1] = chosen
    metas = []
    for k in range(1, n):
        c = copy(mall.at[at(me)], mall.at[at(me)], sm.at[k - 1], rm.at[k - 1], (me + k) % n)
        c.start()
        metas.append(c)
    order = ((0, left, right, (lo, hi)), (1, right, left, (hi, lo)))
    for i, origin, onward, parts in order:
        slot = hall.at[at(origin), parts[0]]
        copy(slot, slot, sb.at[i, 0], rb.at[i, 0], origin).wait_recv()
        start(copy(slot, slot, sc.at[i], rc.at[i], onward))
        start(copy(slot, slot, sd.at[i, 0], rd.at[i, 0], partner))
    for k in range(1, n):
        src = (me + n - k) % n
        copy(mall.at[at(src)], mall.at[at(src)], sm.at[k - 1], rm.at[k - 1], src).wait_recv()
    tokens = n * tok
    e0 = me * local_exp
    gates_all = mall[:, 0].reshape(tokens, experts)
    chosen_all = mall[:, 1].reshape(tokens, experts)
    lane_all = lax.broadcasted_iota(jnp.int32, (tokens, experts), 1)
    pick = (lax.broadcasted_iota(jnp.int32, (experts, 8), 0)
            == lax.broadcasted_iota(jnp.int32, (experts, 8), 1) + e0)
    pick = jnp.where(pick & (lax.broadcasted_iota(jnp.int32, (experts, 8), 1) < local_exp), 1.0, 0.0).astype(BF16)
    mine = dot32(chosen_all.astype(BF16), pick).astype(BF16)
    row = lax.broadcasted_iota(jnp.int32, (tokens, tokens), 0)
    col = lax.broadcasted_iota(jnp.int32, (tokens, tokens), 1)
    lower = jnp.where(col < row, 1.0, 0.0).astype(BF16)
    upper = jnp.where(row < col, 1.0, 0.0).astype(BF16)
    eye = jnp.where(row == col, 1.0, 0.0).astype(BF16)
    pos_ref[...] = jnp.where(mine.astype(F32) > 0.5, dot32(lower, mine), -1.0)
    post_ref[...] = jnp.where(dot_t(mine, eye) > 0.5, dot_t(mine, upper), -1.0)
    for e in range(local_exp):
        p_ref[:, e:e + 1] = jnp.sum(jnp.where(lane_all == e0 + e, gates_all, 0.0), axis=1, keepdims=True)
    for i, origin, onward, parts in order:
        slot = hall.at[at(origin), parts[1]]
        copy(slot, slot, sb.at[i, 1], rb.at[i, 1], origin).wait_recv()
        start(copy(slot, slot, sd.at[i, 1], rd.at[i, 1], partner))
    for i, origin, onward, parts in order:
        slot = hall.at[at(far), parts[0]]
        copy(slot, slot, sc.at[i], rc.at[i], origin).wait_recv()
        start(copy(slot, slot, sd.at[i, 2], rd.at[i, 2], partner))

    copy(hall.at[at(partner)], hall.at[at(partner)], sa, ra, partner).wait_recv()
    for i, origin_chip, parts in ((0, left_chip, (lo, hi)), (1, right_chip, (hi, lo))):
        other = origin_chip * 2 + (1 - core)
        for j in range(2):
            slot = hall.at[at(other), parts[j]]
            copy(slot, slot, sd.at[i, j], rd.at[i, j], partner).wait_recv()
        slot = hall.at[at(far_chip * 2 + (1 - core)), parts[0]]
        copy(slot, slot, sd.at[i, 2], rd.at[i, 2], partner).wait_recv()
    for c in sends:
        c.wait_send()
    for c in metas:
        c.wait_send()
    for c in ahead:
        c.wait()


def dispatch(x, ids, g, wr, br, w, wd, n, local_exp, blk, npre, dcol):
    tok, d_model = x.shape
    tokens = n * tok
    vm = pl.BlockSpec(memory_space=pltpu.VMEM)
    hbm = pl.BlockSpec(memory_space=pltpu.HBM)
    dma = pltpu.SemaphoreType.DMA
    hall, pos, post, p, pre = pl.pallas_call(
        functools.partial(dispatch_kernel, n, local_exp, dcol),
        out_shape=(vmem_out((n, tok, d_model), BF16), vmem_out((tokens, 8), F32), vmem_out((8, tokens), F32),
                   vmem_out((tokens, local_exp), F32), vmem_out((npre, d_model, blk), BF16)),
        in_specs=[hbm] * 7,
        out_specs=(vm,) * 5,
        scratch_shapes=[pltpu.VMEM(x.shape, x.dtype), pltpu.VMEM(ids.shape, ids.dtype), pltpu.VMEM(g.shape, g.dtype),
                        pltpu.VMEM(wr.shape, wr.dtype), pltpu.VMEM(br.shape, br.dtype), dma((5,)),
                        pltpu.VMEM((n, 2, tok, wr.shape[0]), F32), dma((npre,)),
                        dma, dma, dma((2, 2)), dma((2, 2)), dma((2,)), dma((2,)), dma((2, 3)), dma((2, 3)),
                        dma((n - 1,)), dma((n - 1,))],
        compiler_params=pltpu.CompilerParams(collective_id=0, has_side_effects=True, vmem_limit_bytes=DISPATCH_VMEM),
        name='dispatch',
    )(in_hbm(x), in_hbm(ids), in_hbm(g), in_hbm(wr), in_hbm(br), w, wd)
    return hall, pos, post, p, pre


def gate_up_kernel(m_blk, hall, post_ref, pos_ref, p_ref, pre, b_ref, bd_ref, w_hbm, wd_hbm, z_ref, part_ref, ring,
                   xg, ubuf, ybuf, perm, bias_ref, biasd_ref, sems):
    local_exp, d_model, width = w_hbm.shape
    slots, _, blk = ring.shape
    full, rest = width // blk, width % blk
    per_exp = full + 2
    total = local_exp * per_exp
    tokens = hall.shape[0] * hall.shape[1]
    max_rows = z_ref.shape[1]
    dcol = part_ref.shape[3]

    def block_copy(e, j):
        return weight_block(w_hbm, wd_hbm, ring, sems, dcol, e, j)

    def block_start(e, j):
        half = d_model // 2
        for i in range(2):
            weight_block(w_hbm, wd_hbm, ring, sems, dcol, e, j, pl.ds(i * half, half)).start(priority=i)

    def block_wait(e, j):
        @pl.when(e * per_exp + j >= slots)
        def _():
            block_copy(e, j).wait()

    def start(q):
        e, j = q // per_exp, q % per_exp

        @pl.when(j < full)
        def _():
            block_start(e, j)

        for last in (full, full + 1):
            @pl.when(j == last)
            def _(last=last):
                block_start(e, last)

    bias_ref[...] = b_ref[...].astype(F32)
    biasd_ref[...] = bd_ref[:, :dcol].astype(F32)
    src = lax.broadcasted_iota(jnp.int32, (256, 256), 0)
    dst = lax.broadcasted_iota(jnp.int32, (256, 256), 1)
    want = jnp.where(dst < 128, 2 * dst, 2 * (dst - 128) + 1)
    perm[...] = jnp.where(src == want, 1.0, 0.0).astype(BF16)

    def gather(e):
        where_row = post_ref[pl.ds(e, 1), :]
        count = jnp.sum(jnp.where(where_row >= 0.0, 1.0, 0.0)).astype(jnp.int32)
        chunks = (count + (m_blk - 1)) // m_blk

        def body(m, c):
            at = lax.broadcasted_iota(jnp.int32, (m_blk, tokens), 0) + m * m_blk
            onehot = jnp.where(at.astype(F32) == where_row, 1.0, 0.0).astype(BF16)
            xg[pl.ds(pl.multiple_of(m * m_blk, m_blk), m_blk), :] = dot32(onehot, hall[...].reshape(tokens, d_model)).astype(BF16)
            return c

        lax.fori_loop(0, chunks, body, 0)
        return chunks

    def glu(e, j, m, cols):
        at = pl.ds(pl.multiple_of(m * m_blk, m_blk), m_blk)
        for t in range(0, cols, 256):
            wide = min(256, cols - t)
            if wide == 256:
                pm = perm[...]
            else:
                pm = jnp.concatenate([perm[:128, :64], perm[:128, 128:192]], axis=1)
            al = dot32(ubuf[m, :, t:t + wide], pm)
            gate = jnp.minimum(al[:, :wide // 2], LIMIT)
            linear = jnp.clip(al[:, wide // 2:], -LIMIT, LIMIT)
            z = gate * jax.nn.sigmoid(ALPHA * gate) * (linear + 1.0)
            zoff = pl.multiple_of(j * (blk // 2), 128) + t // 2
            z_ref[e, at, pl.ds(zoff, wide // 2)] = z.astype(BF16)

    def compute(e, j, cols, chunks, weights):
        off = pl.multiple_of(j * blk, 128)
        bias = bias_ref[pl.ds(e, 1), pl.ds(off, cols)]
        before = j - 1 if isinstance(j, int) else jnp.maximum(j - 1, 0)

        def rows(m, c):
            at = pl.ds(pl.multiple_of(m * m_blk, m_blk), m_blk)
            glu(e, before, m, blk)
            ubuf[m, :, :cols] = (dot32(xg[at, :], weights()) + bias).astype(BF16)
            return c

        lax.fori_loop(0, chunks, rows, 0)

    def refill(q):
        @pl.when(q + slots < total)
        def _():
            start(q + slots)

    def streamed(e, j, cols, chunks):
        q = e * per_exp + j
        slot = q % slots
        block_wait(e, j)
        compute(e, j, cols, chunks, lambda: ring[slot, :, :cols])
        refill(q)

    def down_start(e, chunks, first):
        q = e * per_exp + full + 1
        slot = q % slots
        where = pos_ref[:, e:e + 1] if first else jnp.sum(
            jnp.where(lax.broadcasted_iota(jnp.int32, pos_ref.shape, 1) == e, pos_ref[...], 0.0), axis=1, keepdims=True)
        gate = p_ref[:, e:e + 1] if first else jnp.sum(
            jnp.where(lax.broadcasted_iota(jnp.int32, p_ref.shape, 1) == e, p_ref[...], 0.0), axis=1, keepdims=True)
        count = jnp.max(where) + 1.0
        ybuf[...] = jnp.zeros_like(ybuf)
        block_wait(e, full + 1)

        def rows(m, c):
            at = pl.ds(pl.multiple_of(m * m_blk, m_blk), m_blk)
            y = dot32(z_ref[e, at, :], ring[slot, :, :dcol]) + biasd_ref[pl.ds(e, 1), :]
            row_ids = (lax.broadcasted_iota(jnp.int32, (m_blk, 1), 0) + m * m_blk).astype(F32)
            ybuf[at, :] = jnp.where(row_ids < count, y, 0.0).astype(BF16)
            return c

        lax.fori_loop(0, chunks, rows, 0)
        refill(q)
        slot_ids = lax.broadcasted_iota(jnp.int32, (tokens, max_rows), 1).astype(F32)
        scat = jnp.where(where == slot_ids, 1.0, 0.0).astype(BF16)
        add = (gate * dot32(scat, ybuf[...])).reshape(part_ref.shape)
        if first:
            part_ref[...] = add
        else:
            part_ref[...] += add

    def expert(e, first):
        chunks = gather(e)

        def body(j, c):
            streamed(e, j, blk, chunks)
            return c

        lax.fori_loop(0, full, body, 0)
        streamed(e, full, rest, chunks)

        def end(m, c):
            glu(e, full, m, rest)
            return c

        lax.fori_loop(0, chunks, end, 0)
        down_start(e, chunks, first)

    expert(0, True)

    def others(e, c):
        expert(e, False)
        return c

    lax.fori_loop(1, local_exp, others, 0)


def gate_up(hall, post, pos, p, pre, w, b, wd, bd, n, max_rows, m_blk, dcol):
    local_exp, d_model, width = w.shape
    blk = pre.shape[2]
    tok = hall.shape[1]
    vm = pl.BlockSpec(memory_space=pltpu.VMEM)
    hbm = pl.BlockSpec(memory_space=pl.ANY)
    return pl.pallas_call(
        functools.partial(gate_up_kernel, m_blk),
        out_shape=(vmem_out((local_exp, max_rows, width // 2), BF16), vmem_out((2, n // 2, tok, dcol), F32),
                   vmem_out(pre.shape, pre.dtype)),
        in_specs=[vm] * 7 + [hbm] * 2,
        out_specs=(vm, vm, vm),
        input_output_aliases={4: 2},
        scratch_shapes=[pltpu.VMEM((max_rows, d_model), BF16),
                        pltpu.VMEM((max_rows // m_blk, m_blk, blk), BF16), pltpu.VMEM((max_rows, dcol), BF16),
                        pltpu.VMEM((256, 256), BF16), pltpu.VMEM((local_exp, width), F32), pltpu.VMEM((local_exp, dcol), F32),
                        pltpu.SemaphoreType.DMA((pre.shape[0],))],
        compiler_params=pltpu.CompilerParams(vmem_limit_bytes=GATE_UP_VMEM),
        name='gate_up',
    )(in_vmem(hall), in_vmem(post), in_vmem(pos), in_vmem(p), in_vmem(pre), b, bd, w, wd)[:2]


def down_kernel(n, chunks, slots, z_ref, pos_ref, p_ref, part_in, x_ref, b_ref, w_hbm, out_ref,
                wbuf, wrest, scat, part, part_r, near, near_r, ring, ring_r,
                wsem, rsem, ns, nr, fs, fr, hs, hr):
    local_exp, d_ff, width = w_hbm.shape
    tokens = pos_ref.shape[0]
    max_rows = z_ref.shape[1]
    tok = tokens // n
    half = tok // 2
    nchip = n // 2
    blk = chunks[0][1]
    total = len(chunks) * local_exp
    depth = slots - 1
    me = lax.axis_index('ep')
    chip, core = me // 2, me % 2
    partner = chip * 2 + (1 - core)
    right_chip, left_chip, far_chip = (chip + 1) % nchip, (chip + nchip - 1) % nchip, (chip + 2) % nchip
    right, left = right_chip * 2 + core, left_chip * 2 + core
    sides = ((right, right_chip, 0), (left, left_chip, 1))

    barrier = pltpu.get_barrier_semaphore()
    for dev in (partner, right, left):
        pl.semaphore_signal(barrier, inc=1, device_id={'ep': dev}, device_id_type=pl.DeviceIdType.MESH)

    def block_copy(q):
        off, cols = chunks[q // local_exp]
        src = w_hbm.at[q % local_exp, :, pl.ds(off, cols)]
        if cols == blk:
            return pltpu.make_async_copy(src, wbuf.at[q % slots], wsem.at[q % slots])
        return pltpu.make_async_copy(src, wrest.at[q % slots], rsem.at[q % slots])

    def weights(q, cols):
        return wbuf[q % slots] if cols == blk else wrest[q % slots]

    for q in range(local_exp, local_exp + depth):
        block_copy(q).start()

    def copy(src, dst, ssem, rsem_, dev):
        return pltpu.make_async_remote_copy(src_ref=src, dst_ref=dst, send_sem=ssem, recv_sem=rsem_,
                                            device_id={'ep': dev}, device_id_type=pl.DeviceIdType.MESH)

    def bufs(c):
        if chunks[c][1] == blk:
            return part.at[c], near.at[c], ring.at[c]
        return part_r, near_r, ring_r

    def near_copy(c):
        pb, nb, _ = bufs(c)
        pb = part_in if c == 0 else pb
        return copy(pb.at[1 - core], nb, ns.at[c], nr.at[c], partner)

    def far_copy(c, side):
        dev, _, i = side
        pb, _, rb = bufs(c)
        rows = pl.ds(i * half, half)
        return copy(pb.at[core, far_chip, rows], rb.at[i, 0], fs.at[c, i, 0], fr.at[c, i, 0], dev)

    def early_copy(c, side):
        dev, dchip, i = side
        pb, _, rb = bufs(c)
        rows = pl.ds((1 - i) * half, half)
        return copy(pb.at[core, dchip, rows], rb.at[i, 1], fs.at[c, i, 1], fr.at[c, i, 1], dev)

    def late_copy(c, side):
        dev, dchip, i = side
        pb, _, rb = bufs(c)
        rows = pl.ds(i * half, half)
        return copy(pb.at[core, dchip, rows], rb.at[i, 2], hs.at[c, i], hr.at[c, i], dev)

    def stage_near(c):
        near_copy(c).start()

    def stage_far(c):
        near_copy(c).wait()
        pb, nb, _ = bufs(c)
        pb[core] = (part_in if c == 0 else pb)[core] + nb[...]
        for side in sides:
            far_copy(c, side).start()
            early_copy(c, side).start()

    def stage_late(c):
        pb, _, rb = bufs(c)
        for side in sides:
            _, dchip, i = side
            far_copy(c, side).wait_recv()
            pb[core, dchip, i * half:(i + 1) * half] += rb[i, 0]
            late_copy(c, side).start()

    def stage_out(c):
        off, cols = chunks[c]
        pb, _, rb = bufs(c)
        for side in sides:
            early_copy(c, side).wait_recv()
            late_copy(c, side).wait_recv()
        for r in range(2):
            rows = slice(r * half, (r + 1) * half)
            total_ = pb[core, chip, rows] + rb[0, 2 if r == 0 else 1] + rb[1, 1 if r == 0 else 2]
            out_ref[rows, off:off + cols] = (x_ref[rows, off:off + cols].astype(F32) + total_).astype(BF16)

    pl.semaphore_wait(barrier, 3)
    stage_near(0)
    slot_ids = lax.broadcasted_iota(jnp.int32, (tokens, max_rows), 1).astype(F32)
    for e in range(local_exp):
        scat[e] = jnp.where(pos_ref[:, e:e + 1] == slot_ids, 1.0, 0.0).astype(BF16)
    row_ids = lax.broadcasted_iota(jnp.int32, (max_rows, 1), 0).astype(F32)
    counts = [jnp.max(pos_ref[:, e:e + 1]) + 1.0 for e in range(local_exp)]
    bias = b_ref[...].astype(F32)

    last = len(chunks)
    for c, (off, cols) in enumerate(chunks):
        if c == 0:
            continue
        pb = bufs(c)[0]
        for e in range(local_exp):
            q = c * local_exp + e
            if q + depth < total:
                block_copy(q + depth).start()
            block_copy(q).wait()
            y = dot32(z_ref[e], weights(q, cols)) + bias[e:e + 1, off:off + cols]
            y = jnp.where(row_ids < counts[e], y, 0.0).astype(BF16)
            add = (p_ref[:, e:e + 1] * dot32(scat[e], y)).reshape(2, nchip, tok, cols)
            if e == 0:
                pb[...] = add
            else:
                pb[...] += add
            if e == 1:
                if c >= 1:
                    stage_far(c - 1)
            if e == 2:
                if c >= 2:
                    stage_late(c - 2)
                if c >= 3:
                    stage_out(c - 3)
        stage_near(c)
    stage_late(last - 2)
    stage_far(last - 1)
    stage_out(last - 3)
    stage_out(last - 2)
    stage_late(last - 1)
    stage_out(last - 1)
    for c in range(last):
        for side in sides:
            far_copy(c, side).wait_send()
            early_copy(c, side).wait_send()
            late_copy(c, side).wait_send()


def down(z, pos, p, part, x, w, b, n, blk, slots):
    local_exp, d_ff, width = w.shape
    tokens = pos.shape[0]
    tok = tokens // n
    chunks = [(c, min(blk, width - c)) for c in range(0, width, blk)]
    full, rest, last = width // blk, width % blk, len(chunks)
    vm = pl.BlockSpec(memory_space=pltpu.VMEM)
    dma = pltpu.SemaphoreType.DMA
    return pl.pallas_call(
        functools.partial(down_kernel, n, chunks, slots),
        out_shape=vmem_out((tok, width), BF16),
        in_specs=[vm, vm, vm, vm, vm, vm, pl.BlockSpec(memory_space=pl.ANY)],
        out_specs=vm,
        scratch_shapes=[pltpu.VMEM((slots, d_ff, blk), BF16), pltpu.VMEM((slots, d_ff, rest), BF16),
                        pltpu.VMEM((local_exp, tokens, z.shape[1]), BF16),
                        pltpu.VMEM((full, 2, n // 2, tok, blk), F32), pltpu.VMEM((2, n // 2, tok, rest), F32),
                        pltpu.VMEM((full, n // 2, tok, blk), F32), pltpu.VMEM((n // 2, tok, rest), F32),
                        pltpu.VMEM((full, 2, 3, tok // 2, blk), F32), pltpu.VMEM((2, 3, tok // 2, rest), F32),
                        dma((slots,)), dma((slots,)),
                        dma((last,)), dma((last,)), dma((last, 2, 2)), dma((last, 2, 2)), dma((last, 2)), dma((last, 2))],
        compiler_params=pltpu.CompilerParams(collective_id=1, has_side_effects=True, vmem_limit_bytes=DOWN_VMEM),
        name='down',
    )(in_vmem(z), in_vmem(pos), in_vmem(p), in_vmem(part), x, b, w)


def solution(mesh):
    n = mesh.shape['ep']
    rows_spec = P(('dp', 'ep'), None)

    def local_block(x_in, expert_ids, norm_weight, router_w, router_b, w_gate_up, b_gate_up, w_down, b_down):
        tok, d_model = x_in.shape
        top_k = expert_ids.shape[1]
        local_exp = w_gate_up.shape[0]
        experts = local_exp * n
        max_rows = n * (4 * top_k * tok // experts)
        wide = w_gate_up.shape[2] >= 2048
        blk, dcol = (1024, 512) if wide else (256, 128)
        npre = 7
        hall, pos, post, p, pre = dispatch(x_in, expert_ids.T, norm_weight, router_w.T, router_b, w_gate_up, w_down, n, local_exp, blk, npre, dcol)
        z, part = gate_up(hall, post, pos, p, pre, w_gate_up, b_gate_up, w_down, b_down, n, max_rows, min(128, max_rows), dcol)
        return down(z, pos, p, part, x_in, w_down, b_down, n, dcol, 3)

    return jax.shard_map(local_block, mesh=mesh, in_specs=(rows_spec, rows_spec, P(), P(), P(), P('ep', None, None), P('ep', None), P('ep', None, None), P('ep', None)), out_specs=rows_spec, check_vma=False)
```

```python
import functools

import jax
import jax.numpy as jnp
from jax import lax
from jax.experimental import pallas as pl
from jax.experimental.pallas import tpu as pltpu
from jax.sharding import PartitionSpec as P

EPSILON = 1e-5
LIMIT = 7.0
ALPHA = 1.702
F32 = jnp.float32
BF16 = jnp.bfloat16
DISPATCH_VMEM = 10 * 1024 * 1024
GATE_UP_VMEM = 10 * 1024 * 1024
DOWN_VMEM = 30 * 1024 * 1024


def dot32(a, b):
    return jnp.dot(a, b, preferred_element_type=F32)


def in_vmem(a):
    return pltpu.with_memory_space_constraint(a, pltpu.VMEM)


def vmem_out(shape, dtype):
    return pltpu.VMEM(shape, dtype)


def in_hbm(a):
    return pltpu.with_memory_space_constraint(a, pltpu.HBM)


def dot_t(a, b):
    return lax.dot_general(a, b, (((0,), (0,)), ((), ())), preferred_element_type=F32)


def blocks_per_expert(w_hbm, ring):
    return w_hbm.shape[2] // ring.shape[2] + 2


def weight_block(w_hbm, wd_hbm, ring, sems, dcol, e, j):
    slots, _, blk = ring.shape
    full, rest = w_hbm.shape[2] // blk, w_hbm.shape[2] % blk
    slot = (e * (full + 2) + j) % slots
    if isinstance(j, int) and j == full + 1:
        return pltpu.make_async_copy(wd_hbm.at[e, :, pl.ds(0, dcol)], ring.at[slot, :, pl.ds(0, dcol)], sems.at[slot])
    if isinstance(j, int) and j == full:
        return pltpu.make_async_copy(w_hbm.at[e, :, pl.ds(full * blk, rest)], ring.at[slot, :, pl.ds(0, rest)], sems.at[slot])
    off = j * blk if isinstance(j, int) else pl.multiple_of(j * blk, 128)
    return pltpu.make_async_copy(w_hbm.at[e, :, pl.ds(off, blk)], ring.at[slot], sems.at[slot])


def dispatch_kernel(n, local_exp, dcol, x_hbm, ids_hbm, g_hbm, wr_hbm, br_hbm, w_hbm, wd_hbm, hall, pos_ref, post_ref, p_ref, pre,
                    x_ref, ids_ref, g_ref, wr_ref, br_ref, isem, mall, psem, sa, ra, sb, rb, sc, rc, sd, rd, sm, rm):
    me = lax.axis_index('ep')
    chips = n // 2
    chip, core = me // 2, me % 2
    partner = chip * 2 + (1 - core)
    right_chip, left_chip = (chip + 1) % chips, (chip + chips - 1) % chips
    far_chip = (chip + 2) % chips
    right, left = right_chip * 2 + core, left_chip * 2 + core
    far = far_chip * 2 + core
    tok, _ = x_ref.shape
    top_k = ids_ref.shape[0]
    experts = wr_ref.shape[0]

    def at(dev):
        return (dev % 2) * chips + dev // 2

    half = tok // 2

    loads = [pltpu.make_async_copy(src, dst, isem.at[i]) for i, (src, dst) in enumerate(
        ((x_hbm, x_ref), (g_hbm, g_ref), (wr_hbm, wr_ref), (br_hbm, br_ref), (ids_hbm, ids_ref)))]
    for c in loads:
        c.start()
    barrier = pltpu.get_barrier_semaphore()
    for k in range(1, n):
        pl.semaphore_signal(barrier, inc=1, device_id={'ep': (me + k) % n}, device_id_type=pl.DeviceIdType.MESH)
    per_exp = blocks_per_expert(w_hbm, pre)
    ahead = [weight_block(w_hbm, wd_hbm, pre, psem, dcol, q // per_exp, q % per_exp) for q in range(pre.shape[0])]
    for c in loads:
        c.wait()
    for c in ahead:
        c.start()

    x = x_ref[...].astype(F32)
    inv = lax.rsqrt(jnp.mean(x * x, axis=-1, keepdims=True) + EPSILON)
    h = (x * inv * g_ref[...].astype(F32)[None, :]).astype(BF16)
    hall[at(me)] = h

    pl.semaphore_wait(barrier, n - 1)

    def copy(src, dst, ssem, rsem, dev):
        return pltpu.make_async_remote_copy(src_ref=src, dst_ref=dst, send_sem=ssem, recv_sem=rsem,
                                            device_id={'ep': dev}, device_id_type=pl.DeviceIdType.MESH)

    lo, hi = pl.ds(0, half), pl.ds(half, half)
    sends = []

    def start(c):
        c.start()
        sends.append(c)

    for i, (dev, parts) in enumerate(((right, (lo, hi)), (left, (hi, lo)))):
        for j, rows in enumerate(parts):
            start(copy(hall.at[at(me), rows], hall.at[at(me), rows], sb.at[i, j], rb.at[i, j], dev))
    start(copy(hall.at[at(me)], hall.at[at(me)], sa, ra, partner))
    logits = lax.dot_general(h, wr_ref[...], (((1,), (1,)), ((), ())), preferred_element_type=F32) + br_ref[...].astype(F32)[None, :]
    ids = ids_ref[...]
    expert = lax.broadcasted_iota(jnp.int32, (experts, tok), 0)
    turn = jnp.where(lax.broadcasted_iota(jnp.int32, (experts, experts), 0)
                     == lax.broadcasted_iota(jnp.int32, (experts, experts), 1), 1.0, 0.0).astype(BF16)
    hot = [dot_t(jnp.where(ids[k:k + 1, :] == expert, 1.0, 0.0).astype(BF16), turn) > 0.5 for k in range(top_k)]
    picked = [jnp.sum(jnp.where(hk, logits, 0.0), axis=1, keepdims=True) for hk in hot]
    top = functools.reduce(jnp.maximum, picked)
    ex = [jnp.exp(v - top) for v in picked]
    total = functools.reduce(jnp.add, ex)
    gates = jnp.zeros((tok, experts), F32)
    chosen = jnp.zeros((tok, experts), F32)
    for k in range(top_k):
        gates = gates + jnp.where(hot[k], ex[k] / total, 0.0)
        chosen = chosen + jnp.where(hot[k], 1.0, 0.0)
    mall[at(me), 0] = gates
    mall[at(me), 1] = chosen
    metas = []
    for k in range(1, n):
        c = copy(mall.at[at(me)], mall.at[at(me)], sm.at[k - 1], rm.at[k - 1], (me + k) % n)
        c.start()
        metas.append(c)
    order = ((0, left, right, (lo, hi)), (1, right, left, (hi, lo)))
    for i, origin, onward, parts in order:
        slot = hall.at[at(origin), parts[0]]
        copy(slot, slot, sb.at[i, 0], rb.at[i, 0], origin).wait_recv()
        start(copy(slot, slot, sc.at[i], rc.at[i], onward))
        start(copy(slot, slot, sd.at[i, 0], rd.at[i, 0], partner))
    for k in range(1, n):
        src = (me + n - k) % n
        copy(mall.at[at(src)], mall.at[at(src)], sm.at[k - 1], rm.at[k - 1], src).wait_recv()
    tokens = n * tok
    e0 = me * local_exp
    gates_all = mall[:, 0].reshape(tokens, experts)
    chosen_all = mall[:, 1].reshape(tokens, experts)
    lane_all = lax.broadcasted_iota(jnp.int32, (tokens, experts), 1)
    pick = (lax.broadcasted_iota(jnp.int32, (experts, 8), 0)
            == lax.broadcasted_iota(jnp.int32, (experts, 8), 1) + e0)
    pick = jnp.where(pick & (lax.broadcasted_iota(jnp.int32, (experts, 8), 1) < local_exp), 1.0, 0.0).astype(BF16)
    mine = dot32(chosen_all.astype(BF16), pick).astype(BF16)
    row = lax.broadcasted_iota(jnp.int32, (tokens, tokens), 0)
    col = lax.broadcasted_iota(jnp.int32, (tokens, tokens), 1)
    lower = jnp.where(col < row, 1.0, 0.0).astype(BF16)
    upper = jnp.where(row < col, 1.0, 0.0).astype(BF16)
    eye = jnp.where(row == col, 1.0, 0.0).astype(BF16)
    pos_ref[...] = jnp.where(mine.astype(F32) > 0.5, dot32(lower, mine), -1.0)
    post_ref[...] = jnp.where(dot_t(mine, eye) > 0.5, dot_t(mine, upper), -1.0)
    for e in range(local_exp):
        p_ref[:, e:e + 1] = jnp.sum(jnp.where(lane_all == e0 + e, gates_all, 0.0), axis=1, keepdims=True)
    for i, origin, onward, parts in order:
        slot = hall.at[at(origin), parts[1]]
        copy(slot, slot, sb.at[i, 1], rb.at[i, 1], origin).wait_recv()
        start(copy(slot, slot, sd.at[i, 1], rd.at[i, 1], partner))
    for i, origin, onward, parts in order:
        slot = hall.at[at(far), parts[0]]
        copy(slot, slot, sc.at[i], rc.at[i], origin).wait_recv()
        start(copy(slot, slot, sd.at[i, 2], rd.at[i, 2], partner))

    copy(hall.at[at(partner)], hall.at[at(partner)], sa, ra, partner).wait_recv()
    for i, origin_chip, parts in ((0, left_chip, (lo, hi)), (1, right_chip, (hi, lo))):
        other = origin_chip * 2 + (1 - core)
        for j in range(2):
            slot = hall.at[at(other), parts[j]]
            copy(slot, slot, sd.at[i, j], rd.at[i, j], partner).wait_recv()
        slot = hall.at[at(far_chip * 2 + (1 - core)), parts[0]]
        copy(slot, slot, sd.at[i, 2], rd.at[i, 2], partner).wait_recv()
    for c in sends:
        c.wait_send()
    for c in metas:
        c.wait_send()
    for c in ahead:
        c.wait()


def dispatch(x, ids, g, wr, br, w, wd, n, local_exp, blk, npre, dcol):
    tok, d_model = x.shape
    tokens = n * tok
    vm = pl.BlockSpec(memory_space=pltpu.VMEM)
    hbm = pl.BlockSpec(memory_space=pltpu.HBM)
    dma = pltpu.SemaphoreType.DMA
    hall, pos, post, p, pre = pl.pallas_call(
        functools.partial(dispatch_kernel, n, local_exp, dcol),
        out_shape=(vmem_out((n, tok, d_model), BF16), vmem_out((tokens, 8), F32), vmem_out((8, tokens), F32),
                   vmem_out((tokens, local_exp), F32), vmem_out((npre, d_model, blk), BF16)),
        in_specs=[hbm] * 7,
        out_specs=(vm,) * 5,
        scratch_shapes=[pltpu.VMEM(x.shape, x.dtype), pltpu.VMEM(ids.shape, ids.dtype), pltpu.VMEM(g.shape, g.dtype),
                        pltpu.VMEM(wr.shape, wr.dtype), pltpu.VMEM(br.shape, br.dtype), dma((5,)),
                        pltpu.VMEM((n, 2, tok, wr.shape[0]), F32), dma((npre,)),
                        dma, dma, dma((2, 2)), dma((2, 2)), dma((2,)), dma((2,)), dma((2, 3)), dma((2, 3)),
                        dma((n - 1,)), dma((n - 1,))],
        compiler_params=pltpu.CompilerParams(collective_id=0, has_side_effects=True, vmem_limit_bytes=DISPATCH_VMEM),
        name='dispatch',
    )(in_hbm(x), in_hbm(ids), in_hbm(g), in_hbm(wr), in_hbm(br), w, wd)
    return hall, pos, post, p, pre


def gate_up_kernel(m_blk, hall, post_ref, pos_ref, p_ref, pre, b_ref, bd_ref, w_hbm, wd_hbm, z_ref, part_ref, ring,
                   xg, ubuf, ybuf, perm, bias_ref, biasd_ref, sems):
    local_exp, d_model, width = w_hbm.shape
    slots, _, blk = ring.shape
    full, rest = width // blk, width % blk
    per_exp = full + 2
    total = local_exp * per_exp
    tokens = hall.shape[0] * hall.shape[1]
    max_rows = z_ref.shape[1]
    dcol = part_ref.shape[3]

    def block_copy(e, j):
        return weight_block(w_hbm, wd_hbm, ring, sems, dcol, e, j)

    def block_wait(e, j):
        @pl.when(e * per_exp + j >= slots)
        def _():
            block_copy(e, j).wait()

    def start(q):
        e, j = q // per_exp, q % per_exp

        @pl.when(j < full)
        def _():
            block_copy(e, j).start()

        for last in (full, full + 1):
            @pl.when(j == last)
            def _(last=last):
                block_copy(e, last).start()

    bias_ref[...] = b_ref[...].astype(F32)
    biasd_ref[...] = bd_ref[:, :dcol].astype(F32)
    src = lax.broadcasted_iota(jnp.int32, (256, 256), 0)
    dst = lax.broadcasted_iota(jnp.int32, (256, 256), 1)
    want = jnp.where(dst < 128, 2 * dst, 2 * (dst - 128) + 1)
    perm[...] = jnp.where(src == want, 1.0, 0.0).astype(BF16)

    def gather(e):
        where_row = post_ref[pl.ds(e, 1), :]
        count = jnp.sum(jnp.where(where_row >= 0.0, 1.0, 0.0)).astype(jnp.int32)
        chunks = (count + (m_blk - 1)) // m_blk

        def body(m, c):
            at = lax.broadcasted_iota(jnp.int32, (m_blk, tokens), 0) + m * m_blk
            onehot = jnp.where(at.astype(F32) == where_row, 1.0, 0.0).astype(BF16)
            xg[pl.ds(pl.multiple_of(m * m_blk, m_blk), m_blk), :] = dot32(onehot, hall[...].reshape(tokens, d_model)).astype(BF16)
            return c

        lax.fori_loop(0, chunks, body, 0)
        return chunks

    def glu(e, j, m, cols):
        at = pl.ds(pl.multiple_of(m * m_blk, m_blk), m_blk)
        for t in range(0, cols, 256):
            wide = min(256, cols - t)
            if wide == 256:
                pm = perm[...]
            else:
                pm = jnp.concatenate([perm[:128, :64], perm[:128, 128:192]], axis=1)
            al = dot32(ubuf[m, :, t:t + wide], pm)
            gate = jnp.minimum(al[:, :wide // 2], LIMIT)
            linear = jnp.clip(al[:, wide // 2:], -LIMIT, LIMIT)
            z = gate * jax.nn.sigmoid(ALPHA * gate) * (linear + 1.0)
            zoff = pl.multiple_of(j * (blk // 2), 128) + t // 2
            z_ref[e, at, pl.ds(zoff, wide // 2)] = z.astype(BF16)

    def compute(e, j, cols, chunks, weights):
        off = pl.multiple_of(j * blk, 128)
        bias = bias_ref[pl.ds(e, 1), pl.ds(off, cols)]
        before = j - 1 if isinstance(j, int) else jnp.maximum(j - 1, 0)

        def rows(m, c):
            at = pl.ds(pl.multiple_of(m * m_blk, m_blk), m_blk)
            glu(e, before, m, blk)
            ubuf[m, :, :cols] = (dot32(xg[at, :], weights()) + bias).astype(BF16)
            return c

        lax.fori_loop(0, chunks, rows, 0)

    def refill(q):
        @pl.when(q + slots < total)
        def _():
            start(q + slots)

    def streamed(e, j, cols, chunks):
        q = e * per_exp + j
        slot = q % slots
        block_wait(e, j)
        compute(e, j, cols, chunks, lambda: ring[slot, :, :cols])
        refill(q)

    def down_start(e, chunks, first):
        q = e * per_exp + full + 1
        slot = q % slots
        where = pos_ref[:, e:e + 1] if first else jnp.sum(
            jnp.where(lax.broadcasted_iota(jnp.int32, pos_ref.shape, 1) == e, pos_ref[...], 0.0), axis=1, keepdims=True)
        gate = p_ref[:, e:e + 1] if first else jnp.sum(
            jnp.where(lax.broadcasted_iota(jnp.int32, p_ref.shape, 1) == e, p_ref[...], 0.0), axis=1, keepdims=True)
        count = jnp.max(where) + 1.0
        ybuf[...] = jnp.zeros_like(ybuf)
        block_wait(e, full + 1)

        def rows(m, c):
            at = pl.ds(pl.multiple_of(m * m_blk, m_blk), m_blk)
            y = dot32(z_ref[e, at, :], ring[slot, :, :dcol]) + biasd_ref[pl.ds(e, 1), :]
            row_ids = (lax.broadcasted_iota(jnp.int32, (m_blk, 1), 0) + m * m_blk).astype(F32)
            ybuf[at, :] = jnp.where(row_ids < count, y, 0.0).astype(BF16)
            return c

        lax.fori_loop(0, chunks, rows, 0)
        refill(q)
        slot_ids = lax.broadcasted_iota(jnp.int32, (tokens, max_rows), 1).astype(F32)
        scat = jnp.where(where == slot_ids, 1.0, 0.0).astype(BF16)
        add = (gate * dot32(scat, ybuf[...])).reshape(part_ref.shape)
        if first:
            part_ref[...] = add
        else:
            part_ref[...] += add

    def expert(e, first):
        chunks = gather(e)

        def body(j, c):
            streamed(e, j, blk, chunks)
            return c

        lax.fori_loop(0, full, body, 0)
        streamed(e, full, rest, chunks)

        def end(m, c):
            glu(e, full, m, rest)
            return c

        lax.fori_loop(0, chunks, end, 0)
        down_start(e, chunks, first)

    expert(0, True)

    def others(e, c):
        expert(e, False)
        return c

    lax.fori_loop(1, local_exp, others, 0)


def gate_up(hall, post, pos, p, pre, w, b, wd, bd, n, max_rows, m_blk, dcol):
    local_exp, d_model, width = w.shape
    blk = pre.shape[2]
    tok = hall.shape[1]
    vm = pl.BlockSpec(memory_space=pltpu.VMEM)
    hbm = pl.BlockSpec(memory_space=pl.ANY)
    return pl.pallas_call(
        functools.partial(gate_up_kernel, m_blk),
        out_shape=(vmem_out((local_exp, max_rows, width // 2), BF16), vmem_out((2, n // 2, tok, dcol), F32),
                   vmem_out(pre.shape, pre.dtype)),
        in_specs=[vm] * 7 + [hbm] * 2,
        out_specs=(vm, vm, vm),
        input_output_aliases={4: 2},
        scratch_shapes=[pltpu.VMEM((max_rows, d_model), BF16),
                        pltpu.VMEM((max_rows // m_blk, m_blk, blk), BF16), pltpu.VMEM((max_rows, dcol), BF16),
                        pltpu.VMEM((256, 256), BF16), pltpu.VMEM((local_exp, width), F32), pltpu.VMEM((local_exp, dcol), F32),
                        pltpu.SemaphoreType.DMA((pre.shape[0],))],
        compiler_params=pltpu.CompilerParams(vmem_limit_bytes=GATE_UP_VMEM),
        name='gate_up',
    )(in_vmem(hall), in_vmem(post), in_vmem(pos), in_vmem(p), in_vmem(pre), b, bd, w, wd)[:2]


def down_kernel(n, chunks, slots, z_ref, pos_ref, p_ref, part_in, x_ref, b_ref, w_hbm, out_ref,
                wbuf, wrest, scat, part, part_r, near, near_r, ring, ring_r,
                wsem, rsem, ns, nr, fs, fr, hs, hr):
    local_exp, d_ff, width = w_hbm.shape
    tokens = pos_ref.shape[0]
    max_rows = z_ref.shape[1]
    tok = tokens // n
    half = tok // 2
    nchip = n // 2
    blk = chunks[0][1]
    total = len(chunks) * local_exp
    depth = slots - 1
    me = lax.axis_index('ep')
    chip, core = me // 2, me % 2
    partner = chip * 2 + (1 - core)
    right_chip, left_chip, far_chip = (chip + 1) % nchip, (chip + nchip - 1) % nchip, (chip + 2) % nchip
    right, left = right_chip * 2 + core, left_chip * 2 + core
    sides = ((right, right_chip, 0), (left, left_chip, 1))

    barrier = pltpu.get_barrier_semaphore()
    for dev in (partner, right, left):
        pl.semaphore_signal(barrier, inc=1, device_id={'ep': dev}, device_id_type=pl.DeviceIdType.MESH)

    def block_copy(q):
        off, cols = chunks[q // local_exp]
        src = w_hbm.at[q % local_exp, :, pl.ds(off, cols)]
        if cols == blk:
            return pltpu.make_async_copy(src, wbuf.at[q % slots], wsem.at[q % slots])
        return pltpu.make_async_copy(src, wrest.at[q % slots], rsem.at[q % slots])

    def weights(q, cols):
        return wbuf[q % slots] if cols == blk else wrest[q % slots]

    for q in range(local_exp, local_exp + depth):
        block_copy(q).start()

    def copy(src, dst, ssem, rsem_, dev):
        return pltpu.make_async_remote_copy(src_ref=src, dst_ref=dst, send_sem=ssem, recv_sem=rsem_,
                                            device_id={'ep': dev}, device_id_type=pl.DeviceIdType.MESH)

    def bufs(c):
        if chunks[c][1] == blk:
            return part.at[c], near.at[c], ring.at[c]
        return part_r, near_r, ring_r

    def near_copy(c):
        pb, nb, _ = bufs(c)
        pb = part_in if c == 0 else pb
        return copy(pb.at[1 - core], nb, ns.at[c], nr.at[c], partner)

    def far_copy(c, side):
        dev, _, i = side
        pb, _, rb = bufs(c)
        rows = pl.ds(i * half, half)
        return copy(pb.at[core, far_chip, rows], rb.at[i, 0], fs.at[c, i, 0], fr.at[c, i, 0], dev)

    def early_copy(c, side):
        dev, dchip, i = side
        pb, _, rb = bufs(c)
        rows = pl.ds((1 - i) * half, half)
        return copy(pb.at[core, dchip, rows], rb.at[i, 1], fs.at[c, i, 1], fr.at[c, i, 1], dev)

    def late_copy(c, side):
        dev, dchip, i = side
        pb, _, rb = bufs(c)
        rows = pl.ds(i * half, half)
        return copy(pb.at[core, dchip, rows], rb.at[i, 2], hs.at[c, i], hr.at[c, i], dev)

    def stage_near(c):
        near_copy(c).start()

    def stage_far(c):
        near_copy(c).wait()
        pb, nb, _ = bufs(c)
        pb[core] = (part_in if c == 0 else pb)[core] + nb[...]
        for side in sides:
            far_copy(c, side).start()
            early_copy(c, side).start()

    def stage_late(c):
        pb, _, rb = bufs(c)
        for side in sides:
            _, dchip, i = side
            far_copy(c, side).wait_recv()
            pb[core, dchip, i * half:(i + 1) * half] += rb[i, 0]
            late_copy(c, side).start()

    def stage_out(c):
        off, cols = chunks[c]
        pb, _, rb = bufs(c)
        for side in sides:
            early_copy(c, side).wait_recv()
            late_copy(c, side).wait_recv()
        for r in range(2):
            rows = slice(r * half, (r + 1) * half)
            total_ = pb[core, chip, rows] + rb[0, 2 if r == 0 else 1] + rb[1, 1 if r == 0 else 2]
            out_ref[rows, off:off + cols] = (x_ref[rows, off:off + cols].astype(F32) + total_).astype(BF16)

    pl.semaphore_wait(barrier, 3)
    stage_near(0)
    slot_ids = lax.broadcasted_iota(jnp.int32, (tokens, max_rows), 1).astype(F32)
    for e in range(local_exp):
        scat[e] = jnp.where(pos_ref[:, e:e + 1] == slot_ids, 1.0, 0.0).astype(BF16)
    row_ids = lax.broadcasted_iota(jnp.int32, (max_rows, 1), 0).astype(F32)
    counts = [jnp.max(pos_ref[:, e:e + 1]) + 1.0 for e in range(local_exp)]
    bias = b_ref[...].astype(F32)

    stage_far(0)
    last = len(chunks)
    for c, (off, cols) in enumerate(chunks):
        if c == 0:
            continue
        pb = bufs(c)[0]
        for e in range(local_exp):
            q = c * local_exp + e
            if q + depth < total:
                block_copy(q + depth).start()
            block_copy(q).wait()
            y = dot32(z_ref[e], weights(q, cols)) + bias[e:e + 1, off:off + cols]
            y = jnp.where(row_ids < counts[e], y, 0.0).astype(BF16)
            add = (p_ref[:, e:e + 1] * dot32(scat[e], y)).reshape(2, nchip, tok, cols)
            if e == 0:
                pb[...] = add
            else:
                pb[...] += add
            if e == 0:
                if c >= 2:
                    stage_far(c - 1)
            if e == 2:
                if c >= 2:
                    stage_late(c - 2)
                if c >= 3:
                    stage_out(c - 3)
        stage_near(c)
    stage_late(last - 2)
    stage_far(last - 1)
    stage_out(last - 3)
    stage_out(last - 2)
    stage_late(last - 1)
    stage_out(last - 1)
    for c in range(last):
        for side in sides:
            far_copy(c, side).wait_send()
            early_copy(c, side).wait_send()
            late_copy(c, side).wait_send()


def down(z, pos, p, part, x, w, b, n, blk, slots):
    local_exp, d_ff, width = w.shape
    tokens = pos.shape[0]
    tok = tokens // n
    chunks = [(c, min(blk, width - c)) for c in range(0, width, blk)]
    full, rest, last = width // blk, width % blk, len(chunks)
    vm = pl.BlockSpec(memory_space=pltpu.VMEM)
    dma = pltpu.SemaphoreType.DMA
    return pl.pallas_call(
        functools.partial(down_kernel, n, chunks, slots),
        out_shape=vmem_out((tok, width), BF16),
        in_specs=[vm, vm, vm, vm, vm, vm, pl.BlockSpec(memory_space=pl.ANY)],
        out_specs=vm,
        scratch_shapes=[pltpu.VMEM((slots, d_ff, blk), BF16), pltpu.VMEM((slots, d_ff, rest), BF16),
                        pltpu.VMEM((local_exp, tokens, z.shape[1]), BF16),
                        pltpu.VMEM((full, 2, n // 2, tok, blk), F32), pltpu.VMEM((2, n // 2, tok, rest), F32),
                        pltpu.VMEM((full, n // 2, tok, blk), F32), pltpu.VMEM((n // 2, tok, rest), F32),
                        pltpu.VMEM((full, 2, 3, tok // 2, blk), F32), pltpu.VMEM((2, 3, tok // 2, rest), F32),
                        dma((slots,)), dma((slots,)),
                        dma((last,)), dma((last,)), dma((last, 2, 2)), dma((last, 2, 2)), dma((last, 2)), dma((last, 2))],
        compiler_params=pltpu.CompilerParams(collective_id=1, has_side_effects=True, vmem_limit_bytes=DOWN_VMEM),
        name='down',
    )(in_vmem(z), in_vmem(pos), in_vmem(p), in_vmem(part), x, b, w)


def solution(mesh):
    n = mesh.shape['ep']
    rows_spec = P(('dp', 'ep'), None)

    def local_block(x_in, expert_ids, norm_weight, router_w, router_b, w_gate_up, b_gate_up, w_down, b_down):
        tok, d_model = x_in.shape
        top_k = expert_ids.shape[1]
        local_exp = w_gate_up.shape[0]
        experts = local_exp * n
        max_rows = n * (4 * top_k * tok // experts)
        wide = w_gate_up.shape[2] >= 2048
        blk, dcol = (1024, 512) if wide else (256, 128)
        npre = 7
        hall, pos, post, p, pre = dispatch(x_in, expert_ids.T, norm_weight, router_w.T, router_b, w_gate_up, w_down, n, local_exp, blk, npre, dcol)
        z, part = gate_up(hall, post, pos, p, pre, w_gate_up, b_gate_up, w_down, b_down, n, max_rows, min(128, max_rows), dcol)
        return down(z, pos, p, part, x_in, w_down, b_down, n, dcol, 3)

    return jax.shard_map(local_block, mesh=mesh, in_specs=(rows_spec, rows_spec, P(), P(), P(), P('ep', None, None), P('ep', None), P('ep', None, None), P('ep', None)), out_specs=rows_spec, check_vma=False)
```
